128 devices in a mesh: gx: 16 (over x, z), gy: 8 (over y, core).
Axes of the slice: x: 4, y: 4, z: 4, core: 2. Of those that a mesh axis runs over, the one named last changes fastest.
Arguments:
- velocity: float32 [3, 256, 256, 256], P(None, 'gx', 'gy'), may hold values from -6 to 6
- owner_block: int32 [262144, 1], P(('gx', 'gy')), may hold values from 0 to 127, as said below
- base_x: int32 [262144], P(('gx', 'gy')), may hold values from 0 to 16
- base_y: int32 [262144], P(('gx', 'gy')), may hold values from 0 to 32
- base_z: int32 [262144], P(('gx', 'gy')), may hold values from 0 to 255
- delta_weights: float32 [12, 262144], P(None, ('gx', 'gy')), may hold values from 0.1 to 1
- marker_offset: float32 [3, 262144], P(None, ('gx', 'gy')), may hold values from -4 to 4
- sphere_motion: float32 [6, 256], P(None, ('gx', 'gy')), may hold values from -6 to 6
- contact_sphere: int32 [512], P(('gx', 'gy')), may hold values from 0 to 255, as said below
- contact_partner: int32 [512], P(('gx', 'gy')), may hold values from 0 to 255
Outputs:
- velocity_star: float32 [3, 256, 256, 256], P(None, 'gx', 'gy')
- new_motion: float32 [6, 256], P(None, ('gx', 'gy'))
The draws below stay inside these ranges and needn't reach their ends.
Inputs may be any that keep to these rules, and one draw needn't show every extreme that they name: `owner_block`: block b stands at gx index b // 8 and gy index b % 8. Each marker's owner block is the block of the device that holds the marker or one of the eight blocks beside it (periodic along gx, none beyond the walls along gy). Among the markers of one device, at most 256 have any one owner block other than that device's own, and in every device exactly 256 have one such block. `contact_sphere`: entry k names one of the 2 spheres k // 4 * 2 and after, those of the device that holds entry k.
All inputs are finite; a program needn't handle non-finite values.
Results may differ from the reference program's by a relative error of at most 0.0003.
Values sent between devices are 32-bit elements; how exact they have to be, the bound alone decides.
A program may use at most 64 MiB of HBM per device.

```python
import math
import jax
import jax.numpy as jnp
from jax import lax

CX = 16
CY = 32
NZ = 256
MK = 1024
S_DEV = 2
CT_DEV = 4
ITERS = 4
NX = 256
NY = 256
SPHERES = 256
MARKERS = 262144
CAP = 256
CONTACTS = 512
N_GX = 16
N_GY = 8


def draw_contact_sphere(key, part):
    entries = jnp.arange(CONTACTS, dtype=jnp.int32)
    picked = jax.random.randint(key, (CONTACTS,), 0, S_DEV, dtype=jnp.int32)
    return entries // CT_DEV * S_DEV + picked


def draw_owner_block(key, part):
    per_device = S_DEV * MK
    devices = N_GX * N_GY
    device = jnp.arange(devices, dtype=jnp.int32)
    column = device // N_GY
    row = device % N_GY
    shift_x = jnp.array([-1, -1, -1, 0, 0, 1, 1, 1], dtype=jnp.int32)
    shift_y = jnp.array([-1, 0, 1, -1, 1, -1, 0, 1], dtype=jnp.int32)
    counts = jax.random.randint(jax.random.fold_in(key, 11), (devices, 8), 1, CAP + 1, dtype=jnp.int32)
    coin = jax.random.randint(jax.random.fold_in(key, 12), (devices,), 0, 2, dtype=jnp.int32)
    full_lane = jnp.where(coin == 0, 1, 6).astype(jnp.int32)
    counts = jnp.where(jnp.arange(8, dtype=jnp.int32)[None, :] == full_lane[:, None], CAP, counts)
    device_keys = jax.random.split(jax.random.fold_in(key, 13), devices)
    position = jax.vmap(lambda one_key: jax.random.permutation(one_key, per_device))(device_keys).astype(jnp.int32)
    lane = jnp.minimum(position // CAP, 7)
    within = position % CAP
    count_here = jnp.take_along_axis(counts, lane, axis=1)
    away = within < count_here
    towards_x = (column[:, None] + shift_x[lane]) % N_GX
    towards_y = row[:, None] + shift_y[lane]
    inside = jnp.logical_and(towards_y >= 0, towards_y < N_GY)
    chosen = jnp.where(jnp.logical_and(away, inside), towards_x * N_GY + towards_y, device[:, None])
    return chosen.reshape(MARKERS, 1).astype(jnp.int32)


def plant(values, stream_key, low, largest):
    shape = values.shape
    index_at = [jax.random.randint(jax.random.fold_in(stream_key, axis), (), 0, shape[axis]) for axis in range(len(shape))]
    values = values.at[tuple(index_at)].set(low)
    longest = shape.index(max(shape))
    index_at[longest] = (index_at[longest] + 1) % shape[longest]
    return values.at[tuple(index_at)].set(largest)


def block_levels(key, extent, shards, smallest, high):
    gain = 1.0
    for axis_at, shards_of in shards:
        heights = jax.random.uniform(jax.random.fold_in(jax.random.fold_in(key, 6), axis_at), (shards_of,), jnp.float32, smallest / len(shards), high / len(shards))
        gain = gain * jnp.repeat(jnp.exp(heights), extent[axis_at] // shards_of).reshape((-1,) + (1,) * (len(extent) - 1 - axis_at))
    return gain


def noise(rng, dims, scale, limit, cuts=(), held_as=jnp.bfloat16):
    level = block_levels(rng, dims, cuts, -0.22, 0.18) if cuts else 1.0
    result = jax.random.normal(rng, dims, jnp.float32) * scale * level
    return jnp.minimum(jnp.maximum(result, -limit), limit).astype(held_as)


def setup_inputs(seed: int = 0) -> dict:
    seeds = jax.random.split(jax.random.key(seed), 11)
    return {
        "velocity": noise(seeds[0], (3, NX, NY, NZ), 1.0, 6.0, ((1, 16), (2, 8)), jnp.float32),
        "owner_block": draw_owner_block(jax.random.fold_in(seeds[10], 71), 0),
        "base_x": plant(jax.random.randint(seeds[2], (MARKERS,), 0, CX + 1), jax.random.fold_in(seeds[2], 1), 0, CX).astype(jnp.int32),
        "base_y": plant(jax.random.randint(seeds[3], (MARKERS,), 0, CY + 1), jax.random.fold_in(seeds[3], 1), 0, CY).astype(jnp.int32),
        "base_z": plant(jax.random.randint(seeds[4], (MARKERS,), 0, NZ), jax.random.fold_in(seeds[4], 1), 0, NZ - 1).astype(jnp.int32),
        "delta_weights": jnp.clip(jnp.exp(math.log(1.0) - 2.3025851 * jax.random.uniform(seeds[5], (12, MARKERS), jnp.float32) ** block_levels(seeds[5], (12, MARKERS), ((1, 128),), -0.2, 0.2)), 0.1, 1.0),
        "marker_offset": noise(seeds[6], (3, MARKERS), 1.0, 4.0, ((1, 128),), jnp.float32),
        "sphere_motion": noise(seeds[7], (6, SPHERES), 1.0, 6.0, ((1, 128),), jnp.float32),
        "contact_sphere": draw_contact_sphere(jax.random.fold_in(seeds[10], 71), 0),
        "contact_partner": plant(jax.random.randint(seeds[9], (CONTACTS,), 0, SPHERES), jax.random.fold_in(seeds[9], 1), 0, SPHERES - 1).astype(jnp.int32),
    }


DIFFUSION = 1.0
RESPONSE = 0.5
DASHPOT = 0.1


def support(start_x, start_y, start_z, weights, stride_y, extent_z):
    offsets = jnp.arange(4, dtype=jnp.int32)
    cells_x = start_x[None, :] + offsets[:, None]
    cells_y = start_y[None, :] + offsets[:, None]
    cells_z = (start_z[None, :] + offsets[:, None]) % extent_z
    where = ((cells_x[:, None, None, :] * stride_y + cells_y[None, :, None, :]) * extent_z + cells_z[None, None, :, :]).reshape(64, -1)
    product = (weights[0:4][:, None, None, :] * weights[4:8][None, :, None, :] * weights[8:12][None, None, :, :]).reshape(64, -1)
    return where, product


def reference(velocity, owner_block, base_x, base_y, base_z, delta_weights, marker_offset, sphere_motion, contact_sphere, contact_partner):
    padded = jnp.pad(velocity, ((0, 0), (2, 2), (0, 0), (0, 0)), mode="wrap")
    padded = jnp.pad(padded, ((0, 0), (0, 0), (2, 2), (0, 0)))
    flat_field = padded.reshape(3, -1)
    owner = owner_block[:, 0]
    start_x = (owner // N_GY) * CX + base_x
    start_y = (owner % N_GY) * CY + base_y
    linear = sphere_motion[0:3]
    angular = sphere_motion[3:6]
    marker_linear = jnp.repeat(linear, MK, axis=1)
    marker_angular = jnp.repeat(angular, MK, axis=1)
    target = marker_linear + jnp.cross(marker_angular, marker_offset, axis=0)
    block_x = start_x.reshape(SPHERES, MK)
    block_y = start_y.reshape(SPHERES, MK)
    block_z = base_z.reshape(SPHERES, MK)
    block_w = delta_weights.reshape(12, SPHERES, MK).transpose(1, 0, 2)
    block_t = target.reshape(3, SPHERES, MK).transpose(1, 0, 2)

    def sample(item):
        where, product = support(item[0], item[1], item[2], item[3], NY + 4, NZ)
        picked = flat_field[:, where]
        return jnp.sum(picked * product[None], axis=1)

    sampled = lax.map(sample, (block_x, block_y, block_z, block_w))
    block_force = block_t - sampled
    force = block_force.transpose(1, 0, 2).reshape(3, MARKERS)
    push = jnp.sum(block_force, axis=-1).T / MK
    twist = jnp.sum(jnp.cross(marker_offset, force, axis=0).reshape(3, SPHERES, MK), axis=-1) / MK
    moved = linear - RESPONSE * push
    turned = angular - RESPONSE * twist
    spring = moved[:, contact_partner] - moved[:, contact_sphere]
    settled = moved + DASHPOT * jax.ops.segment_sum(spring.T, contact_sphere, SPHERES).T
    new_motion = jnp.concatenate([settled, turned], axis=0)

    def deposit(field, item):
        where, product = support(item[0], item[1], item[2], item[3], NY + 4, NZ)
        return field.at[:, where.reshape(-1)].add((product[None] * item[4][:, None, :]).reshape(3, -1)), None

    spread, unused = lax.scan(deposit, jnp.zeros_like(flat_field), (block_x, block_y, block_z, block_w, block_force))
    spread = spread.reshape(padded.shape)
    folded = spread[:, 2:NX + 2]
    folded = folded.at[:, 0:2].add(spread[:, NX + 2:NX + 4])
    folded = folded.at[:, NX - 2:NX].add(spread[:, 0:2])
    source = folded[:, :, 2:NY + 2]
    rhs = velocity + source
    state = rhs
    for sweep in range(ITERS):
        walled = jnp.pad(state, ((0, 0), (0, 0), (1, 1), (0, 0)))
        beside_all = jnp.roll(state, -1, 1) + jnp.roll(state, 1, 1) + walled[:, :, 2:] + walled[:, :, :-2]
        beside_all = beside_all + jnp.roll(state, -1, 3) + jnp.roll(state, 1, 3)
        state = (rhs + DIFFUSION * beside_all) / (1.0 + 6.0 * DIFFUSION)
    return state, new_motion
```

```python
import functools

import jax
import jax.numpy as jnp
from jax import lax
from jax.experimental import pallas as pl
from jax.experimental.pallas import tpu as pltpu
from jax.sharding import PartitionSpec as P

F32 = jnp.float32
BF16 = jnp.bfloat16
I32 = jnp.int32
MESH = pl.DeviceIdType.MESH

ITERS = 4
DIFFUSION = 1.0
RESPONSE = 0.5
DASHPOT = 0.1

TILE = 256
ROWS = 40
HALO = 4
LANES = [(dx, dy) for dx in (-1, 0, 1) for dy in (-1, 0, 1) if (dx, dy) != (0, 0)]
GROUPS = [(0, 1, 2, 17, 18, 19), (3, 4, 5, 14, 15, 16), (6, 7, 8, 9, 10, 11, 12, 13)]
RUNS = [((0, 3), (17, 3)), ((3, 3), (14, 3)), ((6, 8),)]


def split(values):
    high = values.astype(BF16)
    low = (values - high.astype(F32)).astype(BF16)
    return high, low


def pick(distance, weights):
    result = jnp.where(distance == 3, weights[3], 0.0)
    for k in (2, 1, 0):
        result = jnp.where(distance == k, weights[k], result)
    return result


def cross(a, b):
    return (
        a[1] * b[2] - a[2] * b[1],
        a[2] * b[0] - a[0] * b[2],
        a[0] * b[1] - a[1] * b[0],
    )


def kernel(
    n_gx,
    n_gy,
    v_ref,
    int_ref,
    dw_ref,
    off_ref,
    mot_ref,
    cs_ref,
    cp_ref,
    out_ref,
    nm_ref,
    hx,
    hy,
    hc,
    pay,
    pay3,
    own_sq,
    slot_b,
    snd,
    mk,
    frame,
    fhl,
    tz,
    ty_s,
    tx_s,
    sums,
    ret,
    agx,
    agy,
    ag1,
    moved_s,
    rhs,
    state_a,
    state_b,
    ybuf,
    xbuf,
    halo_send,
    halo_recv,
    pay_send,
    pay_recv,
    ret_send,
    ret_recv,
    agx_send,
    agx_recv,
    agy_send,
    agy_recv,
    y_send,
    y_recv,
    x_send,
    x_recv,
):
    gx = lax.axis_index("gx")
    gy = lax.axis_index("gy")
    here = gx * n_gy + gy
    markers = dw_ref.shape[1]
    home_tiles = markers // TILE
    tiles = home_tiles + 8
    span_x = v_ref.shape[1]
    span_y = v_ref.shape[2]
    extent_z = v_ref.shape[3]
    planes = span_x + 4

    def at(dx, dy):
        return (lax.rem(gx + (dx + n_gx), n_gx), lax.rem(gy + (dy + n_gy), n_gy))

    barrier = pltpu.get_barrier_semaphore()
    peers = (
        [at(k, 0) for k in range(1, n_gx)]
        + [at(0, k) for k in range(1, n_gy)]
        + [at(dx, dy) for dx in (-1, 1) for dy in (-1, 1)]
    )
    for peer in peers:
        pl.semaphore_signal(barrier, inc=1, device_id=peer, device_id_type=MESH)

    def remote(src, dst, send, recv, peer):
        return pltpu.make_async_remote_copy(
            src_ref=src,
            dst_ref=dst,
            send_sem=send,
            recv_sem=recv,
            device_id=peer,
            device_id_type=MESH,
        )

    pay[0:12, :] = dw_ref[...]
    pay[12:15, :] = int_ref[1:4, :].astype(F32)
    per_sphere = markers // 2
    second = (lax.broadcasted_iota(I32, (1, markers), 1) >= per_sphere).astype(F32)
    pay[15:16, :] = second
    motion = [mot_ref[c, 0] * (1.0 - second) + mot_ref[c, 1] * second for c in range(6)]
    offset = [off_ref[c : c + 1, :] for c in range(3)]
    swing = cross(motion[3:6], offset)
    for c in range(3):
        pay[16 + c : 17 + c, :] = motion[c] + swing[c]
        pay[19 + c : 20 + c, :] = offset[c]
    pay[22:32, :] = jnp.zeros((10, markers), F32)
    whole = pay[...]
    rest = whole
    for term in range(3):
        part = rest.astype(BF16)
        pay3[32 * term : 32 * term + 32, :] = part
        rest = rest - part.astype(F32)
    at_home = (int_ref[0:1, :] == here).astype(F32)
    for t in range(home_tiles):
        cols = slice(t * TILE, (t + 1) * TILE)
        here_t = at_home[:, cols]
        mk[t, 0:4, :] = pay[0:4, cols] * here_t
        mk[t, 4:16, :] = pay[4:16, cols]
        mk[t, 16:19, :] = pay[16:19, cols] * here_t
        mk[t, 19:24, :] = pay[19:24, cols]

    pl.semaphore_wait(barrier, len(peers))
    last = span_x - 2
    top = span_y - 8
    halo = []
    halo.append(remote(v_ref.at[:, 0:2], hx.at[1], halo_send.at[0], halo_recv.at[0], at(-1, 0)))
    halo.append(
        remote(v_ref.at[:, last:span_x], hx.at[0], halo_send.at[1], halo_recv.at[1], at(1, 0))
    )
    halo.append(
        remote(v_ref.at[:, :, 0:8], hy.at[1], halo_send.at[2], halo_recv.at[2], at(0, -1))
    )
    halo.append(
        remote(v_ref.at[:, :, top:span_y], hy.at[0], halo_send.at[3], halo_recv.at[3], at(0, 1))
    )
    k = 4
    for dx in (-1, 1):
        for dy in (-1, 1):
            x0 = 0 if dx < 0 else last
            y0 = 0 if dy < 0 else top
            slot = (1 if dx < 0 else 0) * 2 + (1 if dy < 0 else 0)
            halo.append(
                remote(
                    v_ref.at[:, x0 : x0 + 2, y0 : y0 + 8],
                    hc.at[slot],
                    halo_send.at[k],
                    halo_recv.at[k],
                    at(dx, dy),
                )
            )
            k += 1
    for copy in halo:
        copy.start()

    own_sq[...] = jnp.zeros_like(own_sq)
    for q in range(markers // 128):
        own_sq[q : q + 1, :] = int_ref[0:1, q * 128 : (q + 1) * 128].astype(F32)
    columns = own_sq[...].T.astype(I32)
    lane_id = lax.broadcasted_iota(I32, (TILE, 128), 1)
    lower = (
        lax.broadcasted_iota(I32, (TILE, TILE), 0) > lax.broadcasted_iota(I32, (TILE, TILE), 1)
    ).astype(BF16)
    carry = jnp.zeros((1, 128), F32)
    for q in range(home_tiles):
        owner = jnp.concatenate(
            [columns[:, 2 * q : 2 * q + 1], columns[:, 2 * q + 1 : 2 * q + 2]], axis=0
        )
        owner_x = lax.shift_right_logical(owner, n_gy.bit_length() - 1)
        owner_y = owner & (n_gy - 1)
        step_x = (owner_x - gx + 1) & (n_gx - 1)
        lane = step_x * 3 + (owner_y - gy + 1)
        lane = jnp.where(owner == here, -1, jnp.where(lane > 4, lane - 1, lane))
        hit = lane_id == lane
        hits = hit.astype(F32)
        ranked = jnp.dot(lower, hits.astype(BF16), preferred_element_type=F32) + carry
        carry = carry + jnp.sum(hits, axis=0, keepdims=True)
        wanted = jnp.sum(
            jnp.where(hit, ranked + (lane_id * TILE).astype(F32), 0.0), axis=1, keepdims=True
        )
        slot = jnp.where(lane < 0, -1, wanted.astype(I32))
        slot_b[q * TILE : (q + 1) * TILE, :] = jnp.broadcast_to(slot, (TILE, 128))

    def compact(n, _):
        slots = slot_b[...] - n * TILE
        low = (slots == lax.broadcasted_iota(I32, (markers, 128), 1)).astype(F32)
        high = (slots == lax.broadcasted_iota(I32, (markers, 128), 1) + 128).astype(F32)
        chosen = jnp.concatenate([low.astype(BF16), high.astype(BF16)], axis=1)
        moved = jnp.dot(pay3[...], chosen, preferred_element_type=F32)
        moved = moved[0:32] + moved[32:64] + moved[64:96]
        snd[n] = moved[0:24]
        return 0

    lax.fori_loop(0, 8, compact, 0)

    requests = [
        remote(snd.at[n], mk.at[home_tiles + n], pay_send.at[n], pay_recv.at[n], at(dx, dy))
        for n, (dx, dy) in enumerate(LANES)
    ]
    for copy in requests:
        copy.start()

    inner_low = jnp.where(gy > 0, 1.0, 0.0).astype(F32)
    inner_high = jnp.where(gy < n_gy - 1, 1.0, 0.0).astype(F32)

    def clear(p, _):
        frame[p] = jnp.zeros((3, ROWS, extent_z), F32)
        rhs[p] = jnp.zeros((3, ROWS, extent_z), F32)
        return 0

    lax.fori_loop(0, planes + 4, clear, 0)

    def place(x, _):
        for c in range(3):
            plane = v_ref[c, x]
            frame[x + 2, c, 4 : 4 + span_y, :] = plane
            rhs[x + 4, c, 4 : 4 + span_y, :] = plane
        return 0

    lax.fori_loop(0, span_x, place, 0)
    for copy in halo:
        copy.wait()

    def rims(x, _):
        for c in range(3):
            frame[x + 2, c, 2:4, :] = hy[0, c, x, 6:8, :] * inner_low
            frame[x + 2, c, 36:38, :] = hy[1, c, x, 0:2, :] * inner_high
        return 0

    lax.fori_loop(0, span_x, rims, 0)
    for side in range(2):
        for i in range(2):
            p = (0 if side == 0 else planes - 2) + i
            for c in range(3):
                frame[p, c, 4 : 4 + span_y, :] = hx[side, c, i]
                frame[p, c, 2:4, :] = hc[side * 2, c, i, 6:8, :] * inner_low
                frame[p, c, 36:38, :] = hc[side * 2 + 1, c, i, 0:2, :] * inner_high

    def halve(p, _):
        high, low = split(frame[p].reshape(3 * ROWS, extent_z))
        fhl[p, :, 0:extent_z] = high
        fhl[p, :, extent_z : 2 * extent_z] = low
        return 0

    lax.fori_loop(0, planes, halve, 0)

    def sample(t, _):
        @pl.when(t == home_tiles)
        def _arrivals():
            for copy in requests:
                copy.wait()

        m = mk[t]
        cell_x = m[12:13].astype(I32)
        cell_y = m[13:14].astype(I32)
        cell_z = m[14:15].astype(I32)
        z = lax.broadcasted_iota(I32, (extent_z, TILE), 0)
        table = pick((z - cell_z) & (extent_z - 1), [m[8 + i : 9 + i] for i in range(4)])
        high, low = split(table)
        tz[t, 0] = high
        tz[t, 1] = low
        y = lax.broadcasted_iota(I32, (ROWS, TILE), 0) - 2
        table_y = pick(y - cell_y, [m[4 + i : 5 + i] for i in range(4)])
        ty_s[t] = table_y
        x = lax.broadcasted_iota(I32, (24, TILE), 0)
        table_x = pick(x - cell_x, [m[i : i + 1] for i in range(4)])
        tx_s[t] = table_x
        both = fhl[...].reshape(planes * 3 * ROWS, 2 * extent_z)
        left = jnp.concatenate([both, both[:, 0:extent_z]], axis=1)
        right = jnp.concatenate([high, high, low], axis=0)
        part = jnp.dot(left, right, preferred_element_type=F32)
        part = part.reshape(planes, 3, ROWS // 8, 8, TILE)
        folded_y = table_y.reshape(ROWS // 8, 8, TILE)
        totals = []
        for c in range(3):
            total = jnp.zeros((8, TILE), F32)
            for p in range(planes):
                total = total + jnp.sum(part[p, c] * folded_y, axis=0) * table_x[p : p + 1]
            totals.append(jnp.sum(total, axis=0, keepdims=True))
        force = [m[16 + c : 17 + c] - totals[c] for c in range(3)]
        torque = cross([m[19 + c : 20 + c] for c in range(3)], force)
        for c in range(3):
            mk[t, 16 + c : 17 + c, :] = force[c]
        acting = jnp.concatenate(force + list(torque) + [jnp.zeros((2, TILE), F32)], axis=0)
        on_second = m[15:16]
        first_sum = jnp.sum(acting * (1.0 - on_second), axis=1, keepdims=True)
        second_sum = jnp.sum(acting * on_second, axis=1, keepdims=True)
        lanes = lax.broadcasted_iota(I32, (8, 128), 1)
        sums[t] = jnp.where(lanes == 0, first_sum, jnp.where(lanes == 1, second_sum, 0.0))
        return 0

    lax.fori_loop(0, tiles, sample, 0)

    replies = [
        remote(sums.at[home_tiles + n], ret.at[n], ret_send.at[n], ret_recv.at[n], at(-dx, -dy))
        for n, (dx, dy) in enumerate(LANES)
    ]
    for copy in replies:
        copy.start()

    lanes = lax.broadcasted_iota(I32, (8, 128), 1)
    row_id = lax.broadcasted_iota(I32, (8, 128), 0)

    def along_x(k):
        return remote(ag1.at[0], agx.at[k], agx_send.at[k], agx_recv.at[k], at(k, 0))

    def along_y(k):
        return remote(ag1.at[1], agy.at[k], agy_send.at[k], agy_recv.at[k], at(0, k))

    def sphere_step_one():
        for copy in replies:
            copy.wait()
        total = jnp.zeros((8, 128), F32)
        for t in range(home_tiles):
            total = total + sums[t]
        for n in range(8):
            total = total + ret[n]
        start = jnp.zeros((8, 128), F32)
        for c in range(6):
            for s in range(2):
                start = jnp.where((row_id == c) & (lanes == s), mot_ref[c, s], start)
        moved = start - total * (RESPONSE / per_sphere)
        moved_s[...] = moved
        first = jnp.broadcast_to(moved[:, 0:1], (8, 128))
        other = pltpu.roll(jnp.broadcast_to(moved[:, 1:2], (8, 128)), 3, 0)
        ag1[0] = jnp.where(lanes == here, jnp.where(row_id < 3, first, other), 0.0)
        for k in range(1, n_gx):
            along_x(k).start()

    def sphere_step_two():
        for k in range(1, n_gx):
            along_x(k).wait()
        total = ag1[0]
        for k in range(1, n_gx):
            total = total + agx[k]
        ag1[1] = total
        for k in range(1, n_gy):
            along_y(k).start()

    def sphere_step_three():
        for k in range(1, n_gy):
            along_y(k).wait()
        total = ag1[1]
        for k in range(1, n_gy):
            total = total + agy[k]
        moved = moved_s[...]
        pull = jnp.zeros((8, 128), F32)
        for k in range(cs_ref.shape[0]):
            partner = cp_ref[k]
            own = cs_ref[k] - 2 * here
            chosen = jnp.sum(
                jnp.where(lanes == lax.shift_right_logical(partner, 1), total, 0.0),
                axis=1,
                keepdims=True,
            )
            chosen = jnp.broadcast_to(chosen, (8, 128))
            odd = jnp.broadcast_to(partner & 1, (8, 128)) == 1
            chosen = jnp.where(odd, pltpu.roll(chosen, 5, 0), chosen)
            pull = pull + jnp.where((lanes == own) & (row_id < 3), chosen - moved, 0.0)
        nm_ref[...] = (moved + DASHPOT * pull)[0:6, 0:2]

    def y_copies(g):
        copies = []
        for r, (first, count) in enumerate(RUNS[g]):
            lo = first + 2
            base = 4 * g + 2 * r
            copies.append(
                remote(
                    rhs.at[pl.ds(lo, count), :, pl.ds(0, 8)],
                    ybuf.at[1, pl.ds(first, count)],
                    y_send.at[base],
                    y_recv.at[base],
                    at(0, -1),
                )
            )
            copies.append(
                remote(
                    rhs.at[pl.ds(lo, count), :, pl.ds(ROWS - 8, 8)],
                    ybuf.at[0, pl.ds(first, count)],
                    y_send.at[base + 1],
                    y_recv.at[base + 1],
                    at(0, 1),
                )
            )
        return copies

    def x_copies(g):
        low = 3 * g
        high = planes - 3 - 3 * g
        return [
            remote(
                rhs.at[pl.ds(low + 2, 3)],
                xbuf.at[1, pl.ds(low, 3)],
                x_send.at[2 * g],
                x_recv.at[2 * g],
                at(-1, 0),
            ),
            remote(
                rhs.at[pl.ds(high + 2, 3)],
                xbuf.at[0, pl.ds(3 - low, 3)],
                x_send.at[2 * g + 1],
                x_recv.at[2 * g + 1],
                at(1, 0),
            ),
        ]

    def finish_y(g):
        for copy in y_copies(g):
            copy.wait()
        for p in GROUPS[g]:
            rhs[p + 2, :, 0:8, :] = rhs[p + 2, :, 0:8, :] + ybuf[0, p] * inner_low
            rhs[p + 2, :, ROWS - 8 : ROWS, :] = (
                rhs[p + 2, :, ROWS - 8 : ROWS, :] + ybuf[1, p] * inner_high
            )

    def deposit(g, t):
        m = mk[t]
        table_y = ty_s[t]
        table_x = tx_s[t]
        rows = []
        for p in GROUPS[g]:
            strength = m[16:19] * table_x[p : p + 1]
            for c in range(3):
                rows.append(strength[c : c + 1] * table_y)
        high, low = split(jnp.concatenate(rows, axis=0))
        left = jnp.concatenate([high, low, high], axis=1)
        right = jnp.concatenate([tz[t, 0], tz[t, 0], tz[t, 1]], axis=1)
        added = lax.dot_general(
            left, right, (((1,), (1,)), ((), ())), preferred_element_type=F32
        ).reshape(len(GROUPS[g]), 3, ROWS, extent_z)
        for i, p in enumerate(GROUPS[g]):
            rhs[p + 2] = rhs[p + 2] + added[i]

    def group_zero(t, _):
        deposit(0, t)
        return 0

    lax.fori_loop(0, tiles, group_zero, 0)
    for copy in y_copies(0):
        copy.start()
    sphere_step_one()

    def group_one(t, _):
        deposit(1, t)

        @pl.when(t == 5)
        def _send():
            finish_y(0)
            for copy in x_copies(0):
                copy.start()

        return 0

    lax.fori_loop(0, tiles, group_one, 0)
    for copy in y_copies(1):
        copy.start()
    sphere_step_two()

    def group_two(t, _):
        deposit(2, t)

        @pl.when(t == 4)
        def _send():
            finish_y(1)
            for copy in x_copies(1):
                copy.start()

        return 0

    lax.fori_loop(0, tiles, group_two, 0)
    for copy in y_copies(2):
        copy.start()
    sphere_step_three()
    finish_y(2)
    for g in range(2):
        for copy in x_copies(g):
            copy.wait()

    y = lax.broadcasted_iota(I32, (ROWS, extent_z), 0)
    low_edge = jnp.where(gy > 0, 0, HALO)
    high_edge = jnp.where(gy < n_gy - 1, ROWS, HALO + span_y)
    inside = jnp.where((y >= low_edge) & (y < high_edge), 1.0, 0.0).astype(F32)
    inside = jnp.concatenate([inside] * 3, axis=0)
    scale = inside * (1.0 / (1.0 + 6.0 * DIFFUSION))
    flat = (3 * ROWS, extent_z)

    for i in range(6):
        rhs[i] = rhs[i] + xbuf[0, i]
        rhs[planes - 2 + i] = rhs[planes - 2 + i] + xbuf[1, i]

    def begin(x, _):
        state_a[x] = (rhs[x].reshape(flat) * inside).reshape(3, ROWS, extent_z)
        return 0

    lax.fori_loop(0, planes + 4, begin, 0)

    def sweep(source, x):
        centre = source[x].reshape(flat)
        total = rhs[x].reshape(flat) + source[x - 1].reshape(flat) + source[x + 1].reshape(flat)
        total = total + pltpu.roll(centre, 1, 0) + pltpu.roll(centre, 3 * ROWS - 1, 0)
        total = total + pltpu.roll(centre, 1, 1) + pltpu.roll(centre, extent_z - 1, 1)
        return total * scale

    buffers = (state_a, state_b)
    for k in range(ITERS - 1):
        source, target = buffers[k % 2], buffers[(k + 1) % 2]

        def step(x, _, source=source, target=target):
            target[x] = sweep(source, x).reshape(3, ROWS, extent_z)
            return 0

        lax.fori_loop(k + 1, planes + 3 - k, step, 0)
    source = buffers[(ITERS - 1) % 2]

    def final(x, _):
        result = sweep(source, x + HALO).reshape(3, ROWS, extent_z)
        for c in range(3):
            out_ref[c, x] = result[c, HALO : HALO + span_y, :]
        return 0

    lax.fori_loop(0, span_x, final, 0)


def on_device(n_gx, n_gy, velocity, owner_block, base_x, base_y, base_z, delta_weights, marker_offset, sphere_motion, contact_sphere, contact_partner):
    span_x, span_y, extent_z = velocity.shape[1:]
    markers = base_x.shape[0]
    ints = jnp.stack([owner_block[:, 0], base_x, base_y, base_z])
    tiles = markers // TILE + 8
    planes = span_x + 4
    vmem = pl.BlockSpec(memory_space=pltpu.VMEM)
    smem = pl.BlockSpec(memory_space=pltpu.SMEM)
    dma = pltpu.SemaphoreType.DMA
    return pl.pallas_call(
        functools.partial(kernel, n_gx, n_gy),
        out_shape=(
            jax.ShapeDtypeStruct(velocity.shape, F32),
            jax.ShapeDtypeStruct(sphere_motion.shape, F32),
        ),
        in_specs=[vmem, vmem, vmem, vmem, smem, smem, smem],
        out_specs=(vmem, vmem),
        scratch_shapes=[
            pltpu.VMEM((2, 3, 2, span_y, extent_z), F32),
            pltpu.VMEM((2, 3, span_x, 8, extent_z), F32),
            pltpu.VMEM((4, 3, 2, 8, extent_z), F32),
            pltpu.VMEM((32, markers), F32),
            pltpu.VMEM((96, markers), BF16),
            pltpu.VMEM((128, 128), F32),
            pltpu.VMEM((markers, 128), I32),
            pltpu.VMEM((8, 24, TILE), F32),
            pltpu.VMEM((tiles, 24, TILE), F32),
            pltpu.VMEM((planes + 4, 3, ROWS, extent_z), F32),
            pltpu.VMEM((planes, 3 * ROWS, 2 * extent_z), BF16),
            pltpu.VMEM((tiles, 2, extent_z, TILE), BF16),
            pltpu.VMEM((tiles, ROWS, TILE), F32),
            pltpu.VMEM((tiles, 24, TILE), F32),
            pltpu.VMEM((tiles, 8, 128), F32),
            pltpu.VMEM((8, 8, 128), F32),
            pltpu.VMEM((n_gx, 8, 128), F32),
            pltpu.VMEM((n_gy, 8, 128), F32),
            pltpu.VMEM((2, 8, 128), F32),
            pltpu.VMEM((8, 128), F32),
            pltpu.VMEM((planes + 4, 3, ROWS, extent_z), F32),
            pltpu.VMEM((planes + 4, 3, ROWS, extent_z), F32),
            pltpu.VMEM((planes + 4, 3, ROWS, extent_z), F32),
            pltpu.VMEM((2, planes, 3, 8, extent_z), F32),
            pltpu.VMEM((2, 6, 3, ROWS, extent_z), F32),
            dma((8,)),
            dma((8,)),
            dma((8,)),
            dma((8,)),
            dma((8,)),
            dma((8,)),
            dma((n_gx,)),
            dma((n_gx,)),
            dma((n_gy,)),
            dma((n_gy,)),
            dma((12,)),
            dma((12,)),
            dma((4,)),
            dma((4,)),
        ],
        compiler_params=pltpu.CompilerParams(
            collective_id=0, has_side_effects=True, vmem_limit_bytes=62 << 20
        ),
        name="substep",
    )(velocity, ints, delta_weights, marker_offset, sphere_motion, contact_sphere, contact_partner)


def solution(mesh):
    placed = (
        P(None, "gx", "gy", None),
        P(("gx", "gy"), None),
        P(("gx", "gy")),
        P(("gx", "gy")),
        P(("gx", "gy")),
        P(None, ("gx", "gy")),
        P(None, ("gx", "gy")),
        P(None, ("gx", "gy")),
        P(("gx", "gy")),
        P(("gx", "gy")),
    )
    return jax.shard_map(
        functools.partial(on_device, mesh.shape["gx"], mesh.shape["gy"]),
        mesh=mesh,
        in_specs=placed,
        out_specs=(P(None, "gx", "gy", None), P(None, ("gx", "gy"))),
        check_vma=False,
    )
```

```python
import functools

import jax
import jax.numpy as jnp
from jax import lax
from jax.experimental import pallas as pl
from jax.experimental.pallas import tpu as pltpu
from jax.sharding import PartitionSpec as P

F32 = jnp.float32
BF16 = jnp.bfloat16
I32 = jnp.int32
MESH = pl.DeviceIdType.MESH

ITERS = 4
DIFFUSION = 1.0
RESPONSE = 0.5
DASHPOT = 0.1

TILE = 256
UNROLL = 4
ROWS = 40
HALO = 4
LANES = [(dx, dy) for dx in (-1, 0, 1) for dy in (-1, 0, 1) if (dx, dy) != (0, 0)]
GROUPS = [(0, 1, 2, 17, 18, 19), (3, 4, 5, 14, 15, 16), (6, 7, 8, 9, 10, 11, 12, 13)]
RUNS = [((0, 3), (17, 3)), ((3, 3), (14, 3)), ((6, 8),)]


def split(values):
    high = values.astype(BF16)
    low = (values - high.astype(F32)).astype(BF16)
    return high, low


def pick(distance, weights):
    result = jnp.where(distance == 3, weights[3], 0.0)
    for k in (2, 1, 0):
        result = jnp.where(distance == k, weights[k], result)
    return result


def cross(a, b):
    return (
        a[1] * b[2] - a[2] * b[1],
        a[2] * b[0] - a[0] * b[2],
        a[0] * b[1] - a[1] * b[0],
    )


def kernel(
    n_gx,
    n_gy,
    v_ref,
    own_ref,
    bx_ref,
    by_ref,
    bz_ref,
    dw_ref,
    off_ref,
    mot_ref,
    cs_ref,
    cp_ref,
    rhs,
    nm_ref,
    hx,
    hy,
    hc,
    pay,
    pay3,
    own_sq,
    slot_b,
    snd,
    mk,
    frame,
    fhl,
    tz,
    ty_s,
    tx_s,
    sums,
    ret,
    agx,
    agy,
    ag1,
    moved_s,
    ybuf,
    xbuf,
    halo_send,
    halo_recv,
    pay_send,
    pay_recv,
    ret_send,
    ret_recv,
    agx_send,
    agx_recv,
    agy_send,
    agy_recv,
    y_send,
    y_recv,
    x_send,
    x_recv,
):
    gx = lax.axis_index("gx")
    gy = lax.axis_index("gy")
    here = gx * n_gy + gy
    markers = dw_ref.shape[1]
    home_tiles = markers // TILE
    tiles = home_tiles + 8
    span_x = v_ref.shape[1]
    span_y = v_ref.shape[2]
    extent_z = v_ref.shape[3]
    planes = span_x + 4

    def at(dx, dy):
        return (lax.rem(gx + (dx + n_gx), n_gx), lax.rem(gy + (dy + n_gy), n_gy))

    barrier = pltpu.get_barrier_semaphore()
    peers = (
        [at(k, 0) for k in range(1, n_gx)]
        + [at(0, k) for k in range(1, n_gy)]
        + [at(dx, dy) for dx in (-1, 1) for dy in (-1, 1)]
    )
    for peer in peers:
        pl.semaphore_signal(barrier, inc=1, device_id=peer, device_id_type=MESH)

    def remote(src, dst, send, recv, peer):
        return pltpu.make_async_remote_copy(
            src_ref=src,
            dst_ref=dst,
            send_sem=send,
            recv_sem=recv,
            device_id=peer,
            device_id_type=MESH,
        )

    pay[0:12, :] = dw_ref[...]
    pay[12:13, :] = bx_ref[...].astype(F32)
    pay[13:14, :] = by_ref[...].astype(F32)
    pay[14:15, :] = bz_ref[...].astype(F32)
    per_sphere = markers // 2
    second = (lax.broadcasted_iota(I32, (1, markers), 1) >= per_sphere).astype(F32)
    pay[15:16, :] = second
    motion = [mot_ref[0, c] * (1.0 - second) + mot_ref[1, c] * second for c in range(6)]
    offset = [off_ref[c : c + 1, :] for c in range(3)]
    swing = cross(motion[3:6], offset)
    for c in range(3):
        pay[16 + c : 17 + c, :] = motion[c] + swing[c]
        pay[19 + c : 20 + c, :] = offset[c]
    pay[22:32, :] = jnp.zeros((10, markers), F32)
    whole = pay[...]
    rest = whole
    for term in range(3):
        part = rest.astype(BF16)
        pay3[32 * term : 32 * term + 32, :] = part
        rest = rest - part.astype(F32)
    at_home = (own_ref[...] == here).astype(F32)
    for t in range(home_tiles):
        cols = slice(t * TILE, (t + 1) * TILE)
        here_t = at_home[:, cols]
        mk[t, 0:4, :] = pay[0:4, cols] * here_t
        mk[t, 4:16, :] = pay[4:16, cols]
        mk[t, 16:19, :] = pay[16:19, cols] * here_t
        mk[t, 19:24, :] = pay[19:24, cols]

    pl.semaphore_wait(barrier, len(peers))
    last = span_x - 2
    top = span_y - 8
    halo = []
    halo.append(remote(v_ref.at[:, 0:2], hx.at[1], halo_send.at[0], halo_recv.at[0], at(-1, 0)))
    halo.append(
        remote(v_ref.at[:, last:span_x], hx.at[0], halo_send.at[1], halo_recv.at[1], at(1, 0))
    )
    halo.append(
        remote(v_ref.at[:, :, 0:8], hy.at[1], halo_send.at[2], halo_recv.at[2], at(0, -1))
    )
    halo.append(
        remote(v_ref.at[:, :, top:span_y], hy.at[0], halo_send.at[3], halo_recv.at[3], at(0, 1))
    )
    k = 4
    for dx in (-1, 1):
        for dy in (-1, 1):
            x0 = 0 if dx < 0 else last
            y0 = 0 if dy < 0 else top
            slot = (1 if dx < 0 else 0) * 2 + (1 if dy < 0 else 0)
            halo.append(
                remote(
                    v_ref.at[:, x0 : x0 + 2, y0 : y0 + 8],
                    hc.at[slot],
                    halo_send.at[k],
                    halo_recv.at[k],
                    at(dx, dy),
                )
            )
            k += 1
    for copy in halo:
        copy.start()

    own_sq[...] = jnp.zeros_like(own_sq)
    for q in range(markers // 128):
        own_sq[q : q + 1, :] = own_ref[:, q * 128 : (q + 1) * 128].astype(F32)
    columns = own_sq[...].T.astype(I32)
    lane_id = lax.broadcasted_iota(I32, (TILE, 128), 1)
    lower = (
        lax.broadcasted_iota(I32, (TILE, TILE), 0) > lax.broadcasted_iota(I32, (TILE, TILE), 1)
    ).astype(BF16)
    carry = jnp.zeros((1, 128), F32)
    for q in range(home_tiles):
        owner = jnp.concatenate(
            [columns[:, 2 * q : 2 * q + 1], columns[:, 2 * q + 1 : 2 * q + 2]], axis=0
        )
        owner_x = lax.shift_right_logical(owner, n_gy.bit_length() - 1)
        owner_y = owner & (n_gy - 1)
        step_x = (owner_x - gx + 1) & (n_gx - 1)
        lane = step_x * 3 + (owner_y - gy + 1)
        lane = jnp.where(owner == here, -1, jnp.where(lane > 4, lane - 1, lane))
        hit = lane_id == lane
        hits = hit.astype(F32)
        ranked = jnp.dot(lower, hits.astype(BF16), preferred_element_type=F32) + carry
        carry = carry + jnp.sum(hits, axis=0, keepdims=True)
        wanted = jnp.sum(
            jnp.where(hit, ranked + (lane_id * TILE).astype(F32), 0.0), axis=1, keepdims=True
        )
        slot = jnp.where(lane < 0, -1, wanted.astype(I32))
        slot_b[q * TILE : (q + 1) * TILE, :] = jnp.broadcast_to(slot, (TILE, 128))

    def compact(n, _):
        slots = slot_b[...] - n * TILE
        low = (slots == lax.broadcasted_iota(I32, (markers, 128), 1)).astype(F32)
        high = (slots == lax.broadcasted_iota(I32, (markers, 128), 1) + 128).astype(F32)
        chosen = jnp.concatenate([low.astype(BF16), high.astype(BF16)], axis=1)
        moved = jnp.dot(pay3[...], chosen, preferred_element_type=F32)
        moved = moved[0:32] + moved[32:64] + moved[64:96]
        snd[n] = moved[0:24]
        return 0

    lax.fori_loop(0, 8, compact, 0)

    requests = [
        remote(snd.at[n], mk.at[home_tiles + n], pay_send.at[n], pay_recv.at[n], at(dx, dy))
        for n, (dx, dy) in enumerate(LANES)
    ]
    for copy in requests:
        copy.start()

    inner_low = jnp.where(gy > 0, 1.0, 0.0).astype(F32)
    inner_high = jnp.where(gy < n_gy - 1, 1.0, 0.0).astype(F32)

    def clear(p, _):
        frame[p] = jnp.zeros((3, ROWS, extent_z), F32)
        rhs[p] = jnp.zeros((3, ROWS, extent_z), F32)
        return 0

    lax.fori_loop(0, planes + 4, clear, 0)

    def place(x, _):
        for c in range(3):
            plane = v_ref[c, x]
            frame[x + 2, c, 4 : 4 + span_y, :] = plane
            rhs[x + 4, c, 4 : 4 + span_y, :] = plane
        return 0

    lax.fori_loop(0, span_x, place, 0)
    for copy in halo:
        copy.wait()

    def rims(x, _):
        for c in range(3):
            frame[x + 2, c, 2:4, :] = hy[0, c, x, 6:8, :] * inner_low
            frame[x + 2, c, 36:38, :] = hy[1, c, x, 0:2, :] * inner_high
        return 0

    lax.fori_loop(0, span_x, rims, 0)
    for side in range(2):
        for i in range(2):
            p = (0 if side == 0 else planes - 2) + i
            for c in range(3):
                frame[p, c, 4 : 4 + span_y, :] = hx[side, c, i]
                frame[p, c, 2:4, :] = hc[side * 2, c, i, 6:8, :] * inner_low
                frame[p, c, 36:38, :] = hc[side * 2 + 1, c, i, 0:2, :] * inner_high

    def halve(p, _):
        high, low = split(frame[p].reshape(3 * ROWS, extent_z))
        fhl[p, :, 0:extent_z] = high
        fhl[p, :, extent_z : 2 * extent_z] = low
        return 0

    lax.fori_loop(0, planes, halve, 0)

    def sample(t):
        m = mk[t]
        cell_x = m[12:13].astype(I32)
        cell_y = m[13:14].astype(I32)
        cell_z = m[14:15].astype(I32)
        z = lax.broadcasted_iota(I32, (extent_z, TILE), 0)
        table = pick((z - cell_z) & (extent_z - 1), [m[8 + i : 9 + i] for i in range(4)])
        high, low = split(table)
        tz[t, 0] = high
        tz[t, 1] = low
        y = lax.broadcasted_iota(I32, (ROWS, TILE), 0) - 2
        table_y = pick(y - cell_y, [m[4 + i : 5 + i] for i in range(4)])
        ty_s[t] = table_y
        x = lax.broadcasted_iota(I32, (24, TILE), 0)
        table_x = pick(x - cell_x, [m[i : i + 1] for i in range(4)])
        tx_s[t] = table_x
        both = fhl[...].reshape(planes * 3 * ROWS, 2 * extent_z)
        left = jnp.concatenate([both, both[:, 0:extent_z]], axis=1)
        right = jnp.concatenate([high, high, low], axis=0)
        part = jnp.dot(left, right, preferred_element_type=F32)
        part = part.reshape(planes, 3, ROWS // 8, 8, TILE)
        folded_y = table_y.reshape(ROWS // 8, 8, TILE)
        totals = []
        for c in range(3):
            total = jnp.zeros((8, TILE), F32)
            for p in range(planes):
                total = total + jnp.sum(part[p, c] * folded_y, axis=0) * table_x[p : p + 1]
            totals.append(jnp.sum(total, axis=0, keepdims=True))
        force = [m[16 + c : 17 + c] - totals[c] for c in range(3)]
        torque = cross([m[19 + c : 20 + c] for c in range(3)], force)
        for c in range(3):
            mk[t, 16 + c : 17 + c, :] = force[c]
        acting = jnp.concatenate(force + list(torque) + [jnp.zeros((2, TILE), F32)], axis=0)
        on_second = m[15:16]
        first_sum = jnp.sum(acting * (1.0 - on_second), axis=1, keepdims=True)
        second_sum = jnp.sum(acting * on_second, axis=1, keepdims=True)
        lanes = lax.broadcasted_iota(I32, (8, 128), 1)
        sums[t] = jnp.where(lanes == 0, first_sum, jnp.where(lanes == 1, second_sum, 0.0))

    def sample_some(step, _):
        @pl.when(step == home_tiles // UNROLL)
        def _arrivals():
            for copy in requests:
                copy.wait()

        for u in range(UNROLL):
            sample(step * UNROLL + u)
        return 0

    lax.fori_loop(0, tiles // UNROLL, sample_some, 0)

    replies = [
        remote(sums.at[home_tiles + n], ret.at[n], ret_send.at[n], ret_recv.at[n], at(-dx, -dy))
        for n, (dx, dy) in enumerate(LANES)
    ]
    for copy in replies:
        copy.start()

    lanes = lax.broadcasted_iota(I32, (8, 128), 1)
    row_id = lax.broadcasted_iota(I32, (8, 128), 0)

    def along_x(k):
        return remote(ag1.at[0], agx.at[k], agx_send.at[k], agx_recv.at[k], at(k, 0))

    def along_y(k):
        return remote(ag1.at[1], agy.at[k], agy_send.at[k], agy_recv.at[k], at(0, k))

    def sphere_step_one():
        for copy in replies:
            copy.wait()
        total = jnp.zeros((8, 128), F32)
        for t in range(home_tiles):
            total = total + sums[t]
        for n in range(8):
            total = total + ret[n]
        start = jnp.zeros((8, 128), F32)
        for c in range(6):
            for s in range(2):
                start = jnp.where((row_id == c) & (lanes == s), mot_ref[s, c], start)
        moved = start - total * (RESPONSE / per_sphere)
        moved_s[...] = moved
        first = jnp.broadcast_to(moved[:, 0:1], (8, 128))
        other = pltpu.roll(jnp.broadcast_to(moved[:, 1:2], (8, 128)), 3, 0)
        ag1[0] = jnp.where(lanes == here, jnp.where(row_id < 3, first, other), 0.0)
        for k in range(1, n_gx):
            along_x(k).start()

    def sphere_step_two():
        for k in range(1, n_gx):
            along_x(k).wait()
        total = ag1[0]
        for k in range(1, n_gx):
            total = total + agx[k]
        ag1[1] = total
        for k in range(1, n_gy):
            along_y(k).start()

    def sphere_step_three():
        for k in range(1, n_gy):
            along_y(k).wait()
        total = ag1[1]
        for k in range(1, n_gy):
            total = total + agy[k]
        moved = moved_s[...]
        pull = jnp.zeros((8, 128), F32)
        for k in range(cs_ref.shape[0]):
            partner = cp_ref[k]
            own = cs_ref[k] - 2 * here
            chosen = jnp.sum(
                jnp.where(lanes == lax.shift_right_logical(partner, 1), total, 0.0),
                axis=1,
                keepdims=True,
            )
            chosen = jnp.broadcast_to(chosen, (8, 128))
            odd = jnp.broadcast_to(partner & 1, (8, 128)) == 1
            chosen = jnp.where(odd, pltpu.roll(chosen, 5, 0), chosen)
            pull = pull + jnp.where((lanes == own) & (row_id < 3), chosen - moved, 0.0)
        settled = jnp.concatenate(
            [moved + DASHPOT * pull, jnp.zeros((120, 128), F32)], axis=0
        )
        nm_ref[...] = settled.T[0:2, 0:6]

    def y_copies(g):
        copies = []
        for r, (first, count) in enumerate(RUNS[g]):
            lo = first + 2
            base = 4 * g + 2 * r
            copies.append(
                remote(
                    rhs.at[pl.ds(lo, count), :, pl.ds(0, 8)],
                    ybuf.at[1, pl.ds(first, count)],
                    y_send.at[base],
                    y_recv.at[base],
                    at(0, -1),
                )
            )
            copies.append(
                remote(
                    rhs.at[pl.ds(lo, count), :, pl.ds(ROWS - 8, 8)],
                    ybuf.at[0, pl.ds(first, count)],
                    y_send.at[base + 1],
                    y_recv.at[base + 1],
                    at(0, 1),
                )
            )
        return copies

    def x_copies(g):
        low = 3 * g
        high = planes - 3 - 3 * g
        return [
            remote(
                rhs.at[pl.ds(low + 2, 3)],
                xbuf.at[1, pl.ds(low, 3)],
                x_send.at[2 * g],
                x_recv.at[2 * g],
                at(-1, 0),
            ),
            remote(
                rhs.at[pl.ds(high + 2, 3)],
                xbuf.at[0, pl.ds(3 - low, 3)],
                x_send.at[2 * g + 1],
                x_recv.at[2 * g + 1],
                at(1, 0),
            ),
        ]

    def finish_y(g):
        for copy in y_copies(g):
            copy.wait()
        for p in GROUPS[g]:
            rhs[p + 2, :, 0:8, :] = rhs[p + 2, :, 0:8, :] + ybuf[0, p] * inner_low
            rhs[p + 2, :, ROWS - 8 : ROWS, :] = (
                rhs[p + 2, :, ROWS - 8 : ROWS, :] + ybuf[1, p] * inner_high
            )

    def deposit(g, step):
        added = None
        for u in range(UNROLL):
            t = step * UNROLL + u
            m = mk[t]
            table_y = ty_s[t]
            table_x = tx_s[t]
            rows = []
            for p in GROUPS[g]:
                strength = m[16:19] * table_x[p : p + 1]
                for c in range(3):
                    rows.append(strength[c : c + 1] * table_y)
            high, low = split(jnp.concatenate(rows, axis=0))
            left = jnp.concatenate([high, low, high], axis=1)
            right = jnp.concatenate([tz[t, 0], tz[t, 0], tz[t, 1]], axis=1)
            part = lax.dot_general(
                left, right, (((1,), (1,)), ((), ())), preferred_element_type=F32
            )
            added = part if added is None else added + part
        added = added.reshape(len(GROUPS[g]), 3, ROWS, extent_z)
        for i, p in enumerate(GROUPS[g]):
            rhs[p + 2] = rhs[p + 2] + added[i]

    def group_zero(t, _):
        deposit(0, t)
        return 0

    lax.fori_loop(0, tiles // UNROLL, group_zero, 0)
    for copy in y_copies(0):
        copy.start()
    sphere_step_one()

    def group_one(t, _):
        deposit(1, t)

        @pl.when(t == 1)
        def _send():
            finish_y(0)
            for copy in x_copies(0):
                copy.start()

        return 0

    lax.fori_loop(0, tiles // UNROLL, group_one, 0)
    for copy in y_copies(1):
        copy.start()
    sphere_step_two()

    def group_two(t, _):
        deposit(2, t)

        @pl.when(t == 1)
        def _send():
            finish_y(1)
            for copy in x_copies(1):
                copy.start()

        return 0

    lax.fori_loop(0, tiles // UNROLL, group_two, 0)
    for copy in y_copies(2):
        copy.start()
    sphere_step_three()
    finish_y(2)
    for g in range(2):
        for copy in x_copies(g):
            copy.wait()

    for i in range(6):
        rhs[i] = rhs[i] + xbuf[0, i]
        rhs[planes - 2 + i] = rhs[planes - 2 + i] + xbuf[1, i]


def relax_kernel(n_gy, rhs, out_ref, state_a, state_b, staged, sems):
    gy = lax.axis_index("gy")
    extent_z = rhs.shape[3]
    planes = rhs.shape[0] - 4
    span_x = planes - 4
    span_y = out_ref.shape[2]
    y = lax.broadcasted_iota(I32, (ROWS, extent_z), 0)
    low_edge = jnp.where(gy > 0, 0, HALO)
    high_edge = jnp.where(gy < n_gy - 1, ROWS, HALO + span_y)
    inside = jnp.where((y >= low_edge) & (y < high_edge), 1.0, 0.0).astype(F32)
    inside = jnp.concatenate([inside] * 3, axis=0)
    scale = inside * (1.0 / (1.0 + 6.0 * DIFFUSION))
    flat = (3 * ROWS, extent_z)

    def begin(x, _):
        state_a[x] = (rhs[x].reshape(flat) * inside).reshape(3, ROWS, extent_z)
        return 0

    lax.fori_loop(0, planes + 4, begin, 0)

    def sweep(source, x):
        centre = source[x].reshape(flat)
        total = rhs[x].reshape(flat) + source[x - 1].reshape(flat) + source[x + 1].reshape(flat)
        total = total + pltpu.roll(centre, 1, 0) + pltpu.roll(centre, 3 * ROWS - 1, 0)
        total = total + pltpu.roll(centre, 1, 1) + pltpu.roll(centre, extent_z - 1, 1)
        return total * scale

    buffers = (state_a, state_b)
    for k in range(ITERS - 1):
        source, target = buffers[k % 2], buffers[(k + 1) % 2]

        def step(s, _, source=source, target=target, first=k + 1):
            for u in range(2):
                x = first + 2 * s + u
                target[x] = sweep(source, x).reshape(3, ROWS, extent_z)
            return 0

        lax.fori_loop(0, (planes + 2 - 2 * k) // 2, step, 0)
    source = buffers[(ITERS - 1) % 2]

    def store(s):
        return pltpu.make_async_copy(
            staged.at[:, pl.ds(2 * s, 2)], out_ref.at[:, pl.ds(2 * s, 2)], sems.at[s]
        )

    def final(s, _):
        for u in range(2):
            x = 2 * s + u
            result = sweep(source, x + HALO).reshape(3, ROWS, extent_z)
            for c in range(3):
                staged[c, x] = result[c, HALO : HALO + span_y, :]
        store(s).start()
        return 0

    lax.fori_loop(0, span_x // 2, final, 0)
    for s in range(span_x // 2):
        store(s).wait()


def on_device(n_gx, n_gy, velocity, owner_block, base_x, base_y, base_z, delta_weights, marker_offset, sphere_motion, contact_sphere, contact_partner):
    span_x, span_y, extent_z = velocity.shape[1:]
    markers = base_x.shape[0]
    tiles = markers // TILE + 8
    planes = span_x + 4
    vmem = pl.BlockSpec(memory_space=pltpu.VMEM)
    smem = pl.BlockSpec(memory_space=pltpu.SMEM)
    dma = pltpu.SemaphoreType.DMA
    rhs, new_motion = pl.pallas_call(
        functools.partial(kernel, n_gx, n_gy),
        out_shape=(
            jax.ShapeDtypeStruct((planes + 4, 3, ROWS, extent_z), F32),
            jax.ShapeDtypeStruct(sphere_motion.shape[::-1], F32),
        ),
        in_specs=[vmem] * 7 + [smem] * 3,
        out_specs=(vmem, vmem),
        scratch_shapes=[
            pltpu.VMEM((2, 3, 2, span_y, extent_z), F32),
            pltpu.VMEM((2, 3, span_x, 8, extent_z), F32),
            pltpu.VMEM((4, 3, 2, 8, extent_z), F32),
            pltpu.VMEM((32, markers), F32),
            pltpu.VMEM((96, markers), BF16),
            pltpu.VMEM((128, 128), F32),
            pltpu.VMEM((markers, 128), I32),
            pltpu.VMEM((8, 24, TILE), F32),
            pltpu.VMEM((tiles, 24, TILE), F32),
            pltpu.VMEM((planes + 4, 3, ROWS, extent_z), F32),
            pltpu.VMEM((planes, 3 * ROWS, 2 * extent_z), BF16),
            pltpu.VMEM((tiles, 2, extent_z, TILE), BF16),
            pltpu.VMEM((tiles, ROWS, TILE), F32),
            pltpu.VMEM((tiles, 24, TILE), F32),
            pltpu.VMEM((tiles, 8, 128), F32),
            pltpu.VMEM((8, 8, 128), F32),
            pltpu.VMEM((n_gx, 8, 128), F32),
            pltpu.VMEM((n_gy, 8, 128), F32),
            pltpu.VMEM((2, 8, 128), F32),
            pltpu.VMEM((8, 128), F32),
            pltpu.VMEM((2, planes, 3, 8, extent_z), F32),
            pltpu.VMEM((2, 6, 3, ROWS, extent_z), F32),
            dma((8,)),
            dma((8,)),
            dma((8,)),
            dma((8,)),
            dma((8,)),
            dma((8,)),
            dma((n_gx,)),
            dma((n_gx,)),
            dma((n_gy,)),
            dma((n_gy,)),
            dma((12,)),
            dma((12,)),
            dma((4,)),
            dma((4,)),
        ],
        compiler_params=pltpu.CompilerParams(
            collective_id=0, has_side_effects=True, vmem_limit_bytes=44 << 20
        ),
        name="substep",
    )(
        velocity,
        owner_block.reshape(1, markers),
        base_x.reshape(1, markers),
        base_y.reshape(1, markers),
        base_z.reshape(1, markers),
        delta_weights,
        marker_offset,
        sphere_motion.T,
        contact_sphere,
        contact_partner,
    )
    relaxed = pl.pallas_call(
        functools.partial(relax_kernel, n_gy),
        out_shape=jax.ShapeDtypeStruct(velocity.shape, F32),
        in_specs=[vmem],
        out_specs=pl.BlockSpec(memory_space=pl.ANY),
        scratch_shapes=[
            pltpu.VMEM((planes + 4, 3, ROWS, extent_z), F32),
            pltpu.VMEM((planes + 4, 3, ROWS, extent_z), F32),
            pltpu.VMEM(velocity.shape, F32),
            dma((span_x // 2,)),
        ],
        compiler_params=pltpu.CompilerParams(vmem_limit_bytes=20 << 20),
        name="relax",
    )(rhs)
    return relaxed, new_motion.T


def solution(mesh):
    placed = (
        P(None, "gx", "gy", None),
        P(("gx", "gy"), None),
        P(("gx", "gy")),
        P(("gx", "gy")),
        P(("gx", "gy")),
        P(None, ("gx", "gy")),
        P(None, ("gx", "gy")),
        P(None, ("gx", "gy")),
        P(("gx", "gy")),
        P(("gx", "gy")),
    )
    return jax.shard_map(
        functools.partial(on_device, mesh.shape["gx"], mesh.shape["gy"]),
        mesh=mesh,
        in_specs=placed,
        out_specs=(P(None, "gx", "gy", None), P(None, ("gx", "gy"))),
        check_vma=False,
    )
```

```python
import functools

import jax
import jax.numpy as jnp
from jax import lax
from jax.experimental import pallas as pl
from jax.experimental.pallas import tpu as pltpu
from jax.sharding import PartitionSpec as P

F32 = jnp.float32
BF16 = jnp.bfloat16
I32 = jnp.int32
MESH = pl.DeviceIdType.MESH

ITERS = 4
DIFFUSION = 1.0
RESPONSE = 0.5
DASHPOT = 0.1

TILE = 256
BINS = 32
WINDOW = 6
ROWS = 40
HALO = 4
LANES = [(dx, dy) for dx in (-1, 0, 1) for dy in (-1, 0, 1) if (dx, dy) != (0, 0)]
RUNS = [((0, 3), (17, 3)), ((3, 3), (14, 3)), ((6, 8),)]


def split(values):
    high = values.astype(BF16)
    low = (values - high.astype(F32)).astype(BF16)
    return high, low


def pick(distance, weights):
    result = jnp.where(distance == 3, weights[3], 0.0)
    for k in (2, 1, 0):
        result = jnp.where(distance == k, weights[k], result)
    return result


def cross(a, b):
    return (
        a[1] * b[2] - a[2] * b[1],
        a[2] * b[0] - a[0] * b[2],
        a[0] * b[1] - a[1] * b[0],
    )


def remote(src, dst, send, recv, peer):
    return pltpu.make_async_remote_copy(
        src_ref=src,
        dst_ref=dst,
        send_sem=send,
        recv_sem=recv,
        device_id=peer,
        device_id_type=MESH,
    )


def greet(peers):
    barrier = pltpu.get_barrier_semaphore()
    for peer in peers:
        pl.semaphore_signal(barrier, inc=1, device_id=peer, device_id_type=MESH)
    return barrier


def neighbours(n_gx, n_gy):
    gx = lax.axis_index("gx")
    gy = lax.axis_index("gy")

    def at(dx, dy):
        return (lax.rem(gx + (dx + n_gx), n_gx), lax.rem(gy + (dy + n_gy), n_gy))

    return gx, gy, at


def terms(values):
    parts = []
    rest = values
    for _ in range(3):
        part = rest.astype(BF16)
        parts.append(part)
        rest = rest - part.astype(F32)
    return jnp.concatenate(parts, axis=0)


def chosen_columns(parts, slots, first):
    wanted = lax.broadcasted_iota(I32, (TILE, TILE), 0).astype(F32) + first
    hit = jnp.where(wanted == slots, 1.0, 0.0).astype(BF16)
    return lax.dot_general(parts, hit, (((1,), (1,)), ((), ())), preferred_element_type=F32)


def ranks(hits, above):
    return jnp.dot(hits.astype(BF16), above, preferred_element_type=F32)


def strictly_above(size):
    return (
        lax.broadcasted_iota(I32, (size, size), 0) < lax.broadcasted_iota(I32, (size, size), 1)
    ).astype(BF16)


def request_kernel(
    n_gx,
    n_gy,
    v_hbm,
    own_hbm,
    bx_hbm,
    by_hbm,
    bz_hbm,
    dw_hbm,
    off_hbm,
    mot_hbm,
    fhl,
    rhs,
    home,
    arrived,
    v_ref,
    own_ref,
    bx_ref,
    by_ref,
    bz_ref,
    dw_ref,
    off_ref,
    mot_ref,
    hx,
    hy,
    hc,
    pay,
    pay3,
    slot_s,
    snd,
    inbox,
    frame,
    in_sem,
    halo_send,
    halo_recv,
    pay_send,
    pay_recv,
):
    gx, gy, at = neighbours(n_gx, n_gy)
    here = gx * n_gy + gy
    barrier = greet([at(dx, dy) for dx, dy in LANES])
    loads = [
        pltpu.make_async_copy(src, dst, in_sem.at[i])
        for i, (src, dst) in enumerate(
            (
                (v_hbm, v_ref),
                (own_hbm, own_ref),
                (bx_hbm, bx_ref),
                (by_hbm, by_ref),
                (bz_hbm, bz_ref),
                (dw_hbm, dw_ref),
                (off_hbm, off_ref),
                (mot_hbm, mot_ref),
            )
        )
    ]
    for copy in loads:
        copy.start()
    markers = dw_ref.shape[1]
    chunks = markers // TILE
    span_x = v_ref.shape[1]
    span_y = v_ref.shape[2]
    extent_z = v_ref.shape[3]
    planes = span_x + 4
    for copy in loads:
        copy.wait()

    pl.semaphore_wait(barrier, len(LANES))
    last = span_x - 2
    top = span_y - 8
    halo = []
    halo.append(remote(v_ref.at[:, 0:2], hx.at[1], halo_send.at[0], halo_recv.at[0], at(-1, 0)))
    halo.append(
        remote(v_ref.at[:, last:span_x], hx.at[0], halo_send.at[1], halo_recv.at[1], at(1, 0))
    )
    halo.append(
        remote(v_ref.at[:, :, 0:8], hy.at[1], halo_send.at[2], halo_recv.at[2], at(0, -1))
    )
    halo.append(
        remote(v_ref.at[:, :, top:span_y], hy.at[0], halo_send.at[3], halo_recv.at[3], at(0, 1))
    )
    k = 4
    for dx in (-1, 1):
        for dy in (-1, 1):
            x0 = 0 if dx < 0 else last
            y0 = 0 if dy < 0 else top
            slot = (1 if dx < 0 else 0) * 2 + (1 if dy < 0 else 0)
            halo.append(
                remote(
                    v_ref.at[:, x0 : x0 + 2, y0 : y0 + 8],
                    hc.at[slot],
                    halo_send.at[k],
                    halo_recv.at[k],
                    at(dx, dy),
                )
            )
            k += 1
    for copy in halo:
        copy.start()

    pay[0:12, :] = dw_ref[...]
    pay[12:13, :] = bx_ref[...].astype(F32)
    pay[13:14, :] = by_ref[...].astype(F32)
    pay[14:15, :] = bz_ref[...].astype(F32)
    per_sphere = markers // 2
    second = (lax.broadcasted_iota(I32, (1, markers), 1) >= per_sphere).astype(F32)
    pay[15:16, :] = second
    motion = [mot_ref[0, c] * (1.0 - second) + mot_ref[1, c] * second for c in range(6)]
    offset = [off_ref[c : c + 1, :] for c in range(3)]
    swing = cross(motion[3:6], offset)
    for c in range(3):
        pay[16 + c : 17 + c, :] = motion[c] + swing[c]
        pay[19 + c : 20 + c, :] = offset[c]
    pay[22:23, :] = jnp.ones((1, markers), F32)
    pay[23:32, :] = jnp.zeros((9, markers), F32)
    whole = pay[...]
    pay3[...] = terms(whole)
    home[...] = whole
    home[22:23, :] = (own_ref[...] == here).astype(F32)

    above = strictly_above(TILE)
    bins = lax.broadcasted_iota(I32, (8, TILE), 0)
    carry = jnp.zeros((8, 1), F32)
    for q in range(chunks):
        owner = own_ref[:, q * TILE : (q + 1) * TILE]
        owner_x = lax.shift_right_logical(owner, n_gy.bit_length() - 1)
        owner_y = owner & (n_gy - 1)
        step_x = (owner_x - gx + 1) & (n_gx - 1)
        lane = step_x * 3 + (owner_y - gy + 1)
        lane = jnp.where(owner == here, -1, jnp.where(lane > 4, lane - 1, lane))
        hits = jnp.where(bins == lane, 1.0, 0.0)
        ranked = ranks(hits, above) + carry + bins.astype(F32) * TILE
        carry = carry + jnp.sum(hits, axis=1, keepdims=True)
        slot = jnp.sum(hits * ranked, axis=0, keepdims=True)
        slot_s[q : q + 1, :] = jnp.where(lane < 0, -1.0, slot)

    def compact(n, _):
        first = (n * TILE).astype(F32)
        moved = None
        for q in range(chunks):
            part = chosen_columns(
                pay3[:, q * TILE : (q + 1) * TILE], slot_s[q : q + 1, :], first
            )
            moved = part if moved is None else moved + part
        snd[n] = moved[0:24] + moved[32:56] + moved[64:88]
        return 0

    lax.fori_loop(0, 8, compact, 0)

    requests = [
        remote(snd.at[n], inbox.at[n], pay_send.at[n], pay_recv.at[n], at(dx, dy))
        for n, (dx, dy) in enumerate(LANES)
    ]
    for copy in requests:
        copy.start()

    inner_low = jnp.where(gy > 0, 1.0, 0.0).astype(F32)
    inner_high = jnp.where(gy < n_gy - 1, 1.0, 0.0).astype(F32)

    def clear(p, _):
        rhs[p] = jnp.zeros((3, ROWS, extent_z), F32)
        return 0

    lax.fori_loop(0, rhs.shape[0], clear, 0)

    def clear_frame(p, _):
        frame[p] = jnp.zeros((3, ROWS, extent_z), F32)
        return 0

    lax.fori_loop(0, planes, clear_frame, 0)

    def clear_beyond(p, _):
        fhl[p] = jnp.zeros((3 * ROWS, 2 * extent_z), BF16)
        return 0

    lax.fori_loop(planes, fhl.shape[0], clear_beyond, 0)

    def place(x, _):
        for c in range(3):
            plane = v_ref[c, x]
            frame[x + 2, c, 4 : 4 + span_y, :] = plane
            rhs[x + 4, c, 4 : 4 + span_y, :] = plane
        return 0

    lax.fori_loop(0, span_x, place, 0)
    for copy in halo:
        copy.wait()

    def rims(x, _):
        for c in range(3):
            frame[x + 2, c, 2:4, :] = hy[0, c, x, 6:8, :] * inner_low
            frame[x + 2, c, 36:38, :] = hy[1, c, x, 0:2, :] * inner_high
        return 0

    lax.fori_loop(0, span_x, rims, 0)
    for side in range(2):
        for i in range(2):
            p = (0 if side == 0 else planes - 2) + i
            for c in range(3):
                frame[p, c, 4 : 4 + span_y, :] = hx[side, c, i]
                frame[p, c, 2:4, :] = hc[side * 2, c, i, 6:8, :] * inner_low
                frame[p, c, 36:38, :] = hc[side * 2 + 1, c, i, 0:2, :] * inner_high

    def halve(p, _):
        high, low = split(frame[p].reshape(3 * ROWS, extent_z))
        fhl[p, :, 0:extent_z] = high
        fhl[p, :, extent_z : 2 * extent_z] = low
        return 0

    lax.fori_loop(0, planes, halve, 0)
    for copy in requests:
        copy.wait()
    arrived[...] = inbox[...]


def marker_kernel(
    fhl, rhs_in, home, arrived, rhs, acted, pay3, hit_s, rank_s, slot_s, tz
):
    chunks = home.shape[1] // TILE
    every = chunks + 8
    extent_z = rhs.shape[3]
    bins = lax.broadcasted_iota(I32, (BINS, TILE), 0).astype(F32)

    def chunk(q):
        return home[0:24, q * TILE : (q + 1) * TILE] if q < chunks else arrived[q - chunks]

    totals = []
    for q in range(every):
        m = chunk(q)
        if q < chunks:
            source = jnp.zeros((1, TILE), F32)
        else:
            source = jnp.full((1, TILE), float(q - chunks + 1), F32)
        filled = jnp.concatenate([m[0:23], source, jnp.zeros((8, TILE), F32)], axis=0)
        pay3[q] = terms(filled)
        hits = jnp.where((bins == m[12:13]) & (m[22:23] > 0.5), 1.0, 0.0)
        hit_s[q * BINS : (q + 1) * BINS, :] = hits
        totals.append(jnp.sum(hits, axis=1, keepdims=True))
    rank_s[...] = ranks(hit_s[...], strictly_above(TILE))
    carries = []
    count = jnp.zeros((BINS, 1), F32)
    for q in range(every):
        carries.append(count)
        count = count + totals[q]
    high, low = split(jnp.broadcast_to(count, (BINS, 128)))
    below = (
        lax.broadcasted_iota(I32, (BINS, BINS), 0) > lax.broadcasted_iota(I32, (BINS, BINS), 1)
    ).astype(BF16)
    start = jnp.dot(below, high, preferred_element_type=F32)
    start = (start + jnp.dot(below, low, preferred_element_type=F32))[:, 0:1]
    for q in range(every):
        hits = hit_s[q * BINS : (q + 1) * BINS, :]
        ranked = rank_s[q * BINS : (q + 1) * BINS, :] + (carries[q] + start)
        slot = jnp.sum(hits * ranked, axis=0, keepdims=True)
        there = jnp.sum(hits, axis=0, keepdims=True)
        slot_s[q : q + 1, :] = jnp.where(there > 0.5, slot, -1.0)
    present = jnp.sum(count).astype(I32)
    tiles = lax.shift_right_logical(present + (TILE - 1), TILE.bit_length() - 1)
    acted[...] = jnp.zeros_like(acted)

    def start_from(p, _):
        rhs[p] = rhs_in[p]
        return 0

    lax.fori_loop(0, rhs.shape[0], start_from, 0)

    def work(n, _):
        first = (n * TILE).astype(F32)
        moved = None
        for q in range(every):
            part = chosen_columns(pay3[q], slot_s[q : q + 1, :], first)
            moved = part if moved is None else moved + part
        m = moved[0:32] + moved[32:64] + moved[64:96]
        cell_x = m[12:13]
        there = m[22:23] > 0.5
        low_plane = jnp.min(jnp.where(there, cell_x, 16.0)).astype(I32)
        high_plane = jnp.max(jnp.where(there, cell_x, 0.0)).astype(I32) + 3
        spans = (high_plane - low_plane + WINDOW) // WINDOW
        cell_x = cell_x.astype(I32)
        cell_y = m[13:14].astype(I32)
        cell_z = m[14:15].astype(I32)
        z = lax.broadcasted_iota(I32, (extent_z, TILE), 0)
        table = pick((z - cell_z) & (extent_z - 1), [m[8 + i : 9 + i] for i in range(4)])
        high, low = split(table)
        tz[0] = high
        tz[1] = low
        y = lax.broadcasted_iota(I32, (ROWS, TILE), 0) - 2
        table_y = pick(y - cell_y, [m[4 + i : 5 + i] for i in range(4)])
        folded_y = table_y.reshape(ROWS // 8, 8, TILE)
        x = lax.broadcasted_iota(I32, (WINDOW, TILE), 0)
        x_weights = [m[i : i + 1] for i in range(4)]

        def sample(j, totals):
            plane = low_plane + j * WINDOW
            table_x = pick(x + plane - cell_x, x_weights)
            both = fhl[pl.ds(plane, WINDOW)].reshape(WINDOW * 3 * ROWS, 2 * extent_z)
            left = jnp.concatenate([both, both[:, 0:extent_z]], axis=1)
            right = jnp.concatenate([tz[0], tz[0], tz[1]], axis=0)
            part = jnp.dot(left, right, preferred_element_type=F32)
            part = part.reshape(WINDOW, 3, ROWS // 8, 8, TILE)
            result = []
            for c in range(3):
                total = totals[c]
                for p in range(WINDOW):
                    total = total + jnp.sum(part[p, c] * folded_y, axis=0) * table_x[p : p + 1]
                result.append(total)
            return tuple(result)

        totals = lax.fori_loop(0, spans, sample, (jnp.zeros((8, TILE), F32),) * 3)
        totals = [jnp.sum(total, axis=0, keepdims=True) for total in totals]
        force = [m[16 + c : 17 + c] - totals[c] for c in range(3)]
        torque = cross([m[19 + c : 20 + c] for c in range(3)], force)
        acting = jnp.concatenate(force + list(torque) + [jnp.zeros((2, TILE), F32)], axis=0)
        group = m[23:24] * 2.0 + m[15:16]
        member = (
            (lax.broadcasted_iota(I32, (128, TILE), 0).astype(F32) == group) & there
        ).astype(F32)
        summed = lax.dot_general(
            terms(acting),
            member.astype(BF16),
            (((1,), (1,)), ((), ())),
            preferred_element_type=F32,
        )
        acted[...] += summed[0:8] + summed[8:16] + summed[16:24]

        def deposit(j, _):
            plane = low_plane + j * WINDOW
            table_x = pick(x + plane - cell_x, x_weights)
            rows = []
            for p in range(WINDOW):
                for c in range(3):
                    rows.append((force[c] * table_x[p : p + 1]) * table_y)
            high, low = split(jnp.concatenate(rows, axis=0))
            left = jnp.concatenate([high, low, high], axis=1)
            right = jnp.concatenate([tz[0], tz[0], tz[1]], axis=1)
            added = lax.dot_general(
                left, right, (((1,), (1,)), ((), ())), preferred_element_type=F32
            )
            rhs[pl.ds(plane + 2, WINDOW)] += added.reshape(WINDOW, 3, ROWS, extent_z)
            return 0

        lax.fori_loop(0, spans, deposit, 0)
        return 0

    lax.fori_loop(0, tiles, work, 0)


def strip_kernel(
    n_gx,
    n_gy,
    per_sphere,
    rhs,
    acted,
    mot_ref,
    cs_ref,
    cp_ref,
    nm_ref,
    ybuf,
    xbuf,
    sums,
    ret,
    agx,
    agy,
    ag1,
    moved_s,
    staged,
    ret_send,
    ret_recv,
    agx_send,
    agx_recv,
    agy_send,
    agy_recv,
    y_send,
    y_recv,
    x_send,
    x_recv,
):
    gx, gy, at = neighbours(n_gx, n_gy)
    here = gx * n_gy + gy
    planes = ybuf.shape[1]
    peers = (
        [at(k, 0) for k in range(1, n_gx)]
        + [at(0, k) for k in range(1, n_gy)]
        + [at(dx, dy) for dx in (-1, 1) for dy in (-1, 1)]
    )
    barrier = greet(peers)
    inner_low = jnp.where(gy > 0, 1.0, 0.0).astype(F32)
    inner_high = jnp.where(gy < n_gy - 1, 1.0, 0.0).astype(F32)
    for n in range(8):
        sums[n] = pltpu.roll(acted[...], 128 - 2 * (n + 1), 1)
    replies = [
        remote(sums.at[n], ret.at[n], ret_send.at[n], ret_recv.at[n], at(-dx, -dy))
        for n, (dx, dy) in enumerate(LANES)
    ]
    lanes = lax.broadcasted_iota(I32, (8, 128), 1)
    row_id = lax.broadcasted_iota(I32, (8, 128), 0)
    pl.semaphore_wait(barrier, len(peers))

    def along_x(k):
        return remote(ag1.at[0], agx.at[k], agx_send.at[k], agx_recv.at[k], at(k, 0))

    def along_y(k):
        return remote(ag1.at[1], agy.at[k], agy_send.at[k], agy_recv.at[k], at(0, k))

    def sphere_step_one():
        for copy in replies:
            copy.wait()
        total = acted[...]
        for n in range(8):
            total = total + ret[n]
        start = jnp.zeros((8, 128), F32)
        for c in range(6):
            for s in range(2):
                start = jnp.where((row_id == c) & (lanes == s), mot_ref[s, c], start)
        moved = start - total * (RESPONSE / per_sphere)
        moved_s[...] = moved
        first = jnp.broadcast_to(moved[:, 0:1], (8, 128))
        other = pltpu.roll(jnp.broadcast_to(moved[:, 1:2], (8, 128)), 3, 0)
        ag1[0] = jnp.where(lanes == here, jnp.where(row_id < 3, first, other), 0.0)
        for k in range(1, n_gx):
            along_x(k).start()

    def sphere_step_two():
        for k in range(1, n_gx):
            along_x(k).wait()
        total = ag1[0]
        for k in range(1, n_gx):
            total = total + agx[k]
        ag1[1] = total
        for k in range(1, n_gy):
            along_y(k).start()

    def sphere_step_three():
        for k in range(1, n_gy):
            along_y(k).wait()
        total = ag1[1]
        for k in range(1, n_gy):
            total = total + agy[k]
        moved = moved_s[...]
        pull = jnp.zeros((8, 128), F32)
        for k in range(cs_ref.shape[0]):
            partner = cp_ref[k]
            own = cs_ref[k] - 2 * here
            chosen = jnp.sum(
                jnp.where(lanes == lax.shift_right_logical(partner, 1), total, 0.0),
                axis=1,
                keepdims=True,
            )
            chosen = jnp.broadcast_to(chosen, (8, 128))
            odd = jnp.broadcast_to(partner & 1, (8, 128)) == 1
            chosen = jnp.where(odd, pltpu.roll(chosen, 5, 0), chosen)
            pull = pull + jnp.where((lanes == own) & (row_id < 3), chosen - moved, 0.0)
        settled = jnp.concatenate(
            [moved + DASHPOT * pull, jnp.zeros((120, 128), F32)], axis=0
        )
        nm_ref[...] = settled.T[0:2, 0:6]

    def y_copies(g):
        copies = []
        for r, (first, count) in enumerate(RUNS[g]):
            lo = first + 2
            base = 4 * g + 2 * r
            copies.append(
                remote(
                    rhs.at[pl.ds(lo, count), :, pl.ds(0, 8)],
                    ybuf.at[1, pl.ds(first, count)],
                    y_send.at[base],
                    y_recv.at[base],
                    at(0, -1),
                )
            )
            copies.append(
                remote(
                    rhs.at[pl.ds(lo, count), :, pl.ds(ROWS - 8, 8)],
                    ybuf.at[0, pl.ds(first, count)],
                    y_send.at[base + 1],
                    y_recv.at[base + 1],
                    at(0, 1),
                )
            )
        return copies

    def x_copies(g):
        low = 3 * g
        return [
            remote(
                staged.at[1, pl.ds(low, 3)],
                xbuf.at[1, pl.ds(low, 3)],
                x_send.at[2 * g],
                x_recv.at[2 * g],
                at(-1, 0),
            ),
            remote(
                staged.at[0, pl.ds(3 - low, 3)],
                xbuf.at[0, pl.ds(3 - low, 3)],
                x_send.at[2 * g + 1],
                x_recv.at[2 * g + 1],
                at(1, 0),
            ),
        ]

    def stage(g):
        for side, first, base in ((1, RUNS[g][0][0], 0), (0, RUNS[g][1][0], planes - 6)):
            for i in range(3):
                p = first + i
                whole = rhs[p + 2]
                staged[side, p - base, :, 0:8, :] = whole[:, 0:8] + ybuf[0, p] * inner_low
                staged[side, p - base, :, 8 : ROWS - 8, :] = whole[:, 8 : ROWS - 8]
                staged[side, p - base, :, ROWS - 8 : ROWS, :] = (
                    whole[:, ROWS - 8 : ROWS] + ybuf[1, p] * inner_high
                )

    for g in range(2):
        for copy in y_copies(g):
            copy.start()
    for copy in replies:
        copy.start()
    for copy in y_copies(2):
        copy.start()
    for copy in y_copies(0):
        copy.wait()
    stage(0)
    for copy in x_copies(0):
        copy.start()
    sphere_step_one()
    for copy in y_copies(1):
        copy.wait()
    stage(1)
    for copy in x_copies(1):
        copy.start()
    sphere_step_two()
    sphere_step_three()
    for copy in y_copies(2):
        copy.wait()
    for g in range(2):
        for copy in x_copies(g):
            copy.wait()


def relax_kernel(n_gy, rhs_in, ybuf, xbuf, out_ref, rhs, state_a, state_b, staged, sems):
    gy = lax.axis_index("gy")
    extent_z = rhs.shape[3]
    planes = ybuf.shape[1]
    span_x = planes - 4
    span_y = out_ref.shape[2]
    y = lax.broadcasted_iota(I32, (ROWS, extent_z), 0)
    low_edge = jnp.where(gy > 0, 0, HALO)
    high_edge = jnp.where(gy < n_gy - 1, ROWS, HALO + span_y)
    inside = jnp.where((y >= low_edge) & (y < high_edge), 1.0, 0.0).astype(F32)
    inside = jnp.concatenate([inside] * 3, axis=0)
    scale = inside * (1.0 / (1.0 + 6.0 * DIFFUSION))
    flat = (3 * ROWS, extent_z)

    inner_low = jnp.where(gy > 0, 1.0, 0.0).astype(F32)
    inner_high = jnp.where(gy < n_gy - 1, 1.0, 0.0).astype(F32)

    def begin(x, beside):
        whole = rhs_in[x]
        if beside is None:
            whole = whole + xbuf[0 if x < planes // 2 else 1, x % (planes - 2)]
        if not isinstance(x, int) or 2 <= x < planes + 2:
            low = ybuf[0, x - 2] * inner_low
            high = ybuf[1, x - 2] * inner_high
            middle = jnp.zeros((3, ROWS - 16, extent_z), F32)
            whole = whole + jnp.concatenate([low, middle, high], axis=1)
        rhs[x] = whole
        state_a[x] = (whole.reshape(flat) * inside).reshape(3, ROWS, extent_z)
        return 0

    for x in list(range(6)) + list(range(planes - 2, planes + 4)):
        begin(x, None)
    lax.fori_loop(6, planes - 2, begin, 0)

    def sweep(source, x):
        centre = source[x].reshape(flat)
        total = rhs[x].reshape(flat) + source[x - 1].reshape(flat) + source[x + 1].reshape(flat)
        total = total + pltpu.roll(centre, 1, 0) + pltpu.roll(centre, 3 * ROWS - 1, 0)
        total = total + pltpu.roll(centre, 1, 1) + pltpu.roll(centre, extent_z - 1, 1)
        return total * scale

    buffers = (state_a, state_b)
    for k in range(ITERS - 1):
        source, target = buffers[k % 2], buffers[(k + 1) % 2]

        def step(s, _, source=source, target=target, first=k + 1):
            for u in range(2):
                x = first + 2 * s + u
                target[x] = sweep(source, x).reshape(3, ROWS, extent_z)
            return 0

        lax.fori_loop(0, (planes + 2 - 2 * k) // 2, step, 0)
    source = buffers[(ITERS - 1) % 2]

    def store(s):
        return pltpu.make_async_copy(
            staged.at[:, pl.ds(2 * s, 2)], out_ref.at[:, pl.ds(2 * s, 2)], sems.at[s]
        )

    def final(s, _):
        for u in range(2):
            x = 2 * s + u
            result = sweep(source, x + HALO).reshape(3, ROWS, extent_z)
            for c in range(3):
                staged[c, x] = result[c, HALO : HALO + span_y, :]
        store(s).start()
        return 0

    lax.fori_loop(0, span_x // 2, final, 0)
    for s in range(span_x // 2):
        store(s).wait()


def on_device(
    n_gx,
    n_gy,
    velocity,
    owner_block,
    base_x,
    base_y,
    base_z,
    delta_weights,
    marker_offset,
    sphere_motion,
    contact_sphere,
    contact_partner,
):
    span_x, span_y, extent_z = velocity.shape[1:]
    markers = base_x.shape[0]
    planes = span_x + 4
    every = markers // TILE + 8
    padded = planes + WINDOW - 1
    grown = (padded + 2, 3, ROWS, extent_z)
    vmem = pl.BlockSpec(memory_space=pltpu.VMEM)
    smem = pl.BlockSpec(memory_space=pltpu.SMEM)
    hbm = pl.BlockSpec(memory_space=pltpu.HBM)
    dma = pltpu.SemaphoreType.DMA
    motion = sphere_motion.T
    fhl, started, home, arrived = pl.pallas_call(
        functools.partial(request_kernel, n_gx, n_gy),
        out_shape=(
            jax.ShapeDtypeStruct((padded, 3 * ROWS, 2 * extent_z), BF16),
            jax.ShapeDtypeStruct(grown, F32),
            jax.ShapeDtypeStruct((32, markers), F32),
            jax.ShapeDtypeStruct((8, 24, TILE), F32),
        ),
        in_specs=[hbm] * 8,
        out_specs=(vmem,) * 4,
        scratch_shapes=[
            pltpu.VMEM(velocity.shape, F32),
            pltpu.VMEM((1, markers), I32),
            pltpu.VMEM((1, markers), I32),
            pltpu.VMEM((1, markers), I32),
            pltpu.VMEM((1, markers), I32),
            pltpu.VMEM((12, markers), F32),
            pltpu.VMEM((3, markers), F32),
            pltpu.SMEM((2, 6), F32),
            pltpu.VMEM((2, 3, 2, span_y, extent_z), F32),
            pltpu.VMEM((2, 3, span_x, 8, extent_z), F32),
            pltpu.VMEM((4, 3, 2, 8, extent_z), F32),
            pltpu.VMEM((32, markers), F32),
            pltpu.VMEM((96, markers), BF16),
            pltpu.VMEM((8, TILE), F32),
            pltpu.VMEM((8, 24, TILE), F32),
            pltpu.VMEM((8, 24, TILE), F32),
            pltpu.VMEM((planes, 3, ROWS, extent_z), F32),
            dma((8,)),
            dma((8,)),
            dma((8,)),
            dma((8,)),
            dma((8,)),
        ],
        compiler_params=pltpu.CompilerParams(
            collective_id=0, has_side_effects=True, vmem_limit_bytes=24 << 20
        ),
        name="requests",
    )(
        *(
            pltpu.with_memory_space_constraint(array, pltpu.HBM)
            for array in (
                velocity,
                owner_block.reshape(1, markers),
                base_x.reshape(1, markers),
                base_y.reshape(1, markers),
                base_z.reshape(1, markers),
                delta_weights,
                marker_offset,
                motion,
            )
        )
    )
    rhs, acted = pl.pallas_call(
        marker_kernel,
        out_shape=(
            jax.ShapeDtypeStruct(grown, F32),
            jax.ShapeDtypeStruct((8, 128), F32),
        ),
        in_specs=[vmem] * 4,
        out_specs=(vmem,) * 2,
        scratch_shapes=[
            pltpu.VMEM((every, 96, TILE), BF16),
            pltpu.VMEM((every * BINS, TILE), F32),
            pltpu.VMEM((every * BINS, TILE), F32),
            pltpu.VMEM((every, TILE), F32),
            pltpu.VMEM((2, extent_z, TILE), BF16),
        ],
        compiler_params=pltpu.CompilerParams(vmem_limit_bytes=24 << 20),
        name="markers",
    )(fhl, started, home, arrived)
    new_motion, ybuf, xbuf = pl.pallas_call(
        functools.partial(strip_kernel, n_gx, n_gy, markers // 2),
        out_shape=(
            jax.ShapeDtypeStruct(motion.shape, F32),
            jax.ShapeDtypeStruct((2, planes, 3, 8, extent_z), F32),
            jax.ShapeDtypeStruct((2, 6, 3, ROWS, extent_z), F32),
        ),
        in_specs=[vmem] * 2 + [smem] * 3,
        out_specs=(vmem,) * 3,
        scratch_shapes=[
            pltpu.VMEM((8, 8, 128), F32),
            pltpu.VMEM((8, 8, 128), F32),
            pltpu.VMEM((n_gx, 8, 128), F32),
            pltpu.VMEM((n_gy, 8, 128), F32),
            pltpu.VMEM((2, 8, 128), F32),
            pltpu.VMEM((8, 128), F32),
            pltpu.VMEM((2, 6, 3, ROWS, extent_z), F32),
            dma((8,)),
            dma((8,)),
            dma((n_gx,)),
            dma((n_gx,)),
            dma((n_gy,)),
            dma((n_gy,)),
            dma((12,)),
            dma((12,)),
            dma((4,)),
            dma((4,)),
        ],
        compiler_params=pltpu.CompilerParams(
            collective_id=1, has_side_effects=True, vmem_limit_bytes=24 << 20
        ),
        name="strips",
    )(rhs, acted, motion, contact_sphere, contact_partner)
    relaxed = pl.pallas_call(
        functools.partial(relax_kernel, n_gy),
        out_shape=jax.ShapeDtypeStruct(velocity.shape, F32),
        in_specs=[vmem] * 3,
        out_specs=pl.BlockSpec(memory_space=pltpu.HBM),
        scratch_shapes=[
            pltpu.VMEM((planes + 4, 3, ROWS, extent_z), F32),
            pltpu.VMEM((planes + 4, 3, ROWS, extent_z), F32),
            pltpu.VMEM((planes + 4, 3, ROWS, extent_z), F32),
            pltpu.VMEM(velocity.shape, F32),
            dma((span_x // 2,)),
        ],
        compiler_params=pltpu.CompilerParams(vmem_limit_bytes=24 << 20),
        name="relax",
    )(rhs, ybuf, xbuf)
    return relaxed, new_motion.T


def solution(mesh):
    placed = (
        P(None, "gx", "gy", None),
        P(("gx", "gy"), None),
        P(("gx", "gy")),
        P(("gx", "gy")),
        P(("gx", "gy")),
        P(None, ("gx", "gy")),
        P(None, ("gx", "gy")),
        P(None, ("gx", "gy")),
        P(("gx", "gy")),
        P(("gx", "gy")),
    )
    return jax.shard_map(
        functools.partial(on_device, mesh.shape["gx"], mesh.shape["gy"]),
        mesh=mesh,
        in_specs=placed,
        out_specs=(P(None, "gx", "gy", None), P(None, ("gx", "gy"))),
        check_vma=False,
    )
```

```python
import functools

import jax
import jax.numpy as jnp
from jax import lax
from jax.experimental import pallas as pl
from jax.experimental.pallas import tpu as pltpu
from jax.sharding import PartitionSpec as P

F32 = jnp.float32
BF16 = jnp.bfloat16
I32 = jnp.int32
MESH = pl.DeviceIdType.MESH

ITERS = 4
DIFFUSION = 1.0
RESPONSE = 0.5
DASHPOT = 0.1

TILE = 256
BINS = 32
WINDOW = 6
ROWS = 40
HALO = 4
LANES = [(dx, dy) for dx in (-1, 0, 1) for dy in (-1, 0, 1) if (dx, dy) != (0, 0)]
DIAGONALS = [(dx, dy) for dx, dy in LANES if dx * dy != 0]
RUNS = [((0, 1), (19, 1)), ((1, 2), (17, 2)), ((3, 3), (14, 3)), ((6, 8),)]


def split(values):
    high = values.astype(BF16)
    low = (values - high.astype(F32)).astype(BF16)
    return high, low


def pick(distance, weights):
    result = jnp.where(distance == 3, weights[3], 0.0)
    for k in (2, 1, 0):
        result = jnp.where(distance == k, weights[k], result)
    return result


def cross(a, b):
    return (
        a[1] * b[2] - a[2] * b[1],
        a[2] * b[0] - a[0] * b[2],
        a[0] * b[1] - a[1] * b[0],
    )


def remote(src, dst, send, recv, peer):
    return pltpu.make_async_remote_copy(
        src_ref=src,
        dst_ref=dst,
        send_sem=send,
        recv_sem=recv,
        device_id=peer,
        device_id_type=MESH,
    )


def greet(peers):
    barrier = pltpu.get_barrier_semaphore()
    for peer in peers:
        pl.semaphore_signal(barrier, inc=1, device_id=peer, device_id_type=MESH)
    return barrier


def neighbours(n_gx, n_gy):
    gx = lax.axis_index("gx")
    gy = lax.axis_index("gy")

    def at(dx, dy):
        return (lax.rem(gx + (dx + n_gx), n_gx), lax.rem(gy + (dy + n_gy), n_gy))

    return gx, gy, at


def terms(values):
    parts = []
    rest = values
    for _ in range(3):
        part = rest.astype(BF16)
        parts.append(part)
        rest = rest - part.astype(F32)
    return jnp.concatenate(parts, axis=0)


def chosen_columns(parts, slots, first):
    wanted = lax.broadcasted_iota(I32, (TILE, TILE), 0).astype(F32) + first
    hit = jnp.where(wanted == slots, 1.0, 0.0).astype(BF16)
    return lax.dot_general(parts, hit, (((1,), (1,)), ((), ())), preferred_element_type=F32)


def ranks(hits, above):
    return jnp.dot(hits.astype(BF16), above, preferred_element_type=F32)


def strictly_above(size):
    return (
        lax.broadcasted_iota(I32, (size, size), 0) < lax.broadcasted_iota(I32, (size, size), 1)
    ).astype(BF16)


def request_kernel(
    n_gx,
    n_gy,
    v_hbm,
    own_hbm,
    bx_hbm,
    by_hbm,
    bz_hbm,
    dw_hbm,
    off_hbm,
    mot_hbm,
    fhl,
    rhs,
    home,
    arrived,
    v_ref,
    own_ref,
    bx_ref,
    by_ref,
    bz_ref,
    dw_ref,
    off_ref,
    mot_ref,
    hx,
    hy,
    hc,
    corner,
    pay,
    pay3,
    slot_s,
    snd,
    inbox,
    frame,
    in_sem,
    halo_send,
    halo_recv,
    pay_send,
    pay_recv,
):
    gx, gy, at = neighbours(n_gx, n_gy)
    here = gx * n_gy + gy
    barrier = greet([at(dx, dy) for dx, dy in LANES])
    loads = [
        pltpu.make_async_copy(src, dst, in_sem.at[i])
        for i, (src, dst) in enumerate(
            (
                (v_hbm, v_ref),
                (own_hbm, own_ref),
                (bx_hbm, bx_ref),
                (by_hbm, by_ref),
                (bz_hbm, bz_ref),
                (dw_hbm, dw_ref),
                (off_hbm, off_ref),
                (mot_hbm, mot_ref),
            )
        )
    ]
    for copy in loads:
        copy.start()
    markers = dw_ref.shape[1]
    chunks = markers // TILE
    span_x = v_ref.shape[1]
    span_y = v_ref.shape[2]
    extent_z = v_ref.shape[3]
    planes = span_x + 4
    for copy in loads:
        copy.wait()

    last = span_x - 2
    top = span_y - 8
    corner[...] = jnp.zeros_like(corner)
    for k, (dx, dy) in enumerate(DIAGONALS):
        x0 = 0 if dx < 0 else last
        y0 = 0 if dy < 0 else span_y - 2
        for c in range(3):
            for i in range(2):
                row = 4 * c + 2 * i
                corner[k, row : row + 2, :] = v_ref[c, x0 + i, y0 : y0 + 2, :]
    pl.semaphore_wait(barrier, len(LANES))
    halo = []
    halo.append(remote(v_ref.at[:, 0:2], hx.at[1], halo_send.at[0], halo_recv.at[0], at(-1, 0)))
    halo.append(
        remote(v_ref.at[:, last:span_x], hx.at[0], halo_send.at[1], halo_recv.at[1], at(1, 0))
    )
    halo.append(
        remote(v_ref.at[:, :, 0:8], hy.at[1], halo_send.at[2], halo_recv.at[2], at(0, -1))
    )
    halo.append(
        remote(v_ref.at[:, :, top:span_y], hy.at[0], halo_send.at[3], halo_recv.at[3], at(0, 1))
    )
    for k, (dx, dy) in enumerate(DIAGONALS):
        slot = (1 if dx < 0 else 0) * 2 + (1 if dy < 0 else 0)
        halo.append(
            remote(
                corner.at[k], hc.at[slot], halo_send.at[4 + k], halo_recv.at[4 + k], at(dx, dy)
            )
        )
    for copy in halo:
        copy.start()

    pay[0:12, :] = dw_ref[...]
    pay[12:13, :] = bx_ref[...].astype(F32)
    pay[13:14, :] = by_ref[...].astype(F32)
    pay[14:15, :] = bz_ref[...].astype(F32)
    per_sphere = markers // 2
    second = (lax.broadcasted_iota(I32, (1, markers), 1) >= per_sphere).astype(F32)
    pay[15:16, :] = second
    motion = [mot_ref[0, c] * (1.0 - second) + mot_ref[1, c] * second for c in range(6)]
    offset = [off_ref[c : c + 1, :] for c in range(3)]
    swing = cross(motion[3:6], offset)
    for c in range(3):
        pay[16 + c : 17 + c, :] = motion[c] + swing[c]
        pay[19 + c : 20 + c, :] = offset[c]
    pay[22:23, :] = jnp.ones((1, markers), F32)
    pay[23:32, :] = jnp.zeros((9, markers), F32)
    whole = pay[...]
    pay3[...] = terms(whole)
    home[...] = whole
    home[22:23, :] = (own_ref[...] == here).astype(F32)

    above = strictly_above(TILE)
    bins = lax.broadcasted_iota(I32, (8, TILE), 0)
    carry = jnp.zeros((8, 1), F32)
    for q in range(chunks):
        owner = own_ref[:, q * TILE : (q + 1) * TILE]
        owner_x = lax.shift_right_logical(owner, n_gy.bit_length() - 1)
        owner_y = owner & (n_gy - 1)
        step_x = (owner_x - gx + 1) & (n_gx - 1)
        lane = step_x * 3 + (owner_y - gy + 1)
        lane = jnp.where(owner == here, -1, jnp.where(lane > 4, lane - 1, lane))
        hits = jnp.where(bins == lane, 1.0, 0.0)
        ranked = ranks(hits, above) + carry + bins.astype(F32) * TILE
        carry = carry + jnp.sum(hits, axis=1, keepdims=True)
        slot = jnp.sum(hits * ranked, axis=0, keepdims=True)
        slot_s[q : q + 1, :] = jnp.where(lane < 0, -1.0, slot)

    def compact(n, _):
        first = (n * TILE).astype(F32)
        moved = None
        for q in range(chunks):
            part = chosen_columns(
                pay3[:, q * TILE : (q + 1) * TILE], slot_s[q : q + 1, :], first
            )
            moved = part if moved is None else moved + part
        snd[n] = moved[0:24] + moved[32:56] + moved[64:88]
        return 0

    lax.fori_loop(0, 8, compact, 0)

    requests = [
        remote(snd.at[n], inbox.at[n], pay_send.at[n], pay_recv.at[n], at(dx, dy))
        for n, (dx, dy) in enumerate(LANES)
    ]
    for copy in requests:
        copy.start()

    inner_low = jnp.where(gy > 0, 1.0, 0.0).astype(F32)
    inner_high = jnp.where(gy < n_gy - 1, 1.0, 0.0).astype(F32)

    def clear(p, _):
        rhs[p] = jnp.zeros((3, ROWS, extent_z), F32)
        return 0

    lax.fori_loop(0, rhs.shape[0], clear, 0)

    def clear_frame(p, _):
        frame[p] = jnp.zeros((3, ROWS, extent_z), F32)
        return 0

    lax.fori_loop(0, planes, clear_frame, 0)

    def clear_beyond(p, _):
        fhl[p] = jnp.zeros((3 * ROWS, 2 * extent_z), BF16)
        return 0

    lax.fori_loop(planes, fhl.shape[0], clear_beyond, 0)

    def place(x, _):
        for c in range(3):
            plane = v_ref[c, x]
            frame[x + 2, c, 4 : 4 + span_y, :] = plane
            rhs[x + 4, c, 4 : 4 + span_y, :] = plane
        return 0

    lax.fori_loop(0, span_x, place, 0)
    for copy in halo:
        copy.wait()

    def rims(x, _):
        for c in range(3):
            frame[x + 2, c, 2:4, :] = hy[0, c, x, 6:8, :] * inner_low
            frame[x + 2, c, 36:38, :] = hy[1, c, x, 0:2, :] * inner_high
        return 0

    lax.fori_loop(0, span_x, rims, 0)
    for side in range(2):
        for i in range(2):
            p = (0 if side == 0 else planes - 2) + i
            for c in range(3):
                frame[p, c, 4 : 4 + span_y, :] = hx[side, c, i]
                frame[p, c, 2:4, :] = hc[side * 2, 4 * c + 2 * i : 4 * c + 2 * i + 2, :] * inner_low
                frame[p, c, 36:38, :] = (
                    hc[side * 2 + 1, 4 * c + 2 * i : 4 * c + 2 * i + 2, :] * inner_high
                )

    def halve(p, _):
        high, low = split(frame[p].reshape(3 * ROWS, extent_z))
        fhl[p, :, 0:extent_z] = high
        fhl[p, :, extent_z : 2 * extent_z] = low
        return 0

    lax.fori_loop(0, planes, halve, 0)
    for copy in requests:
        copy.wait()
    arrived[...] = inbox[...]


def marker_kernel(
    fhl,
    rhs_in,
    home,
    arrived,
    rhs,
    acted,
    pay3,
    hit_s,
    rank_s,
    slot_s,
    tz,
    held,
    edge_v,
    edge,
    edge_sem,
):
    chunks = home.shape[1] // TILE
    every = chunks + 8
    extent_z = rhs.shape[3]
    bins = lax.broadcasted_iota(I32, (BINS, TILE), 0).astype(F32)

    def chunk(q):
        return home[0:24, q * TILE : (q + 1) * TILE] if q < chunks else arrived[q - chunks]

    totals = []
    for q in range(every):
        m = chunk(q)
        hits = jnp.where((bins == m[12:13]) & (m[22:23] > 0.5), 1.0, 0.0)
        hit_s[q * BINS : (q + 1) * BINS, :] = hits
        totals.append(jnp.sum(hits, axis=1, keepdims=True))
    rank_s[...] = ranks(hit_s[...], strictly_above(TILE))
    carries = []
    count = jnp.zeros((BINS, 1), F32)
    for q in range(every):
        carries.append(count)
        count = count + totals[q]
    count = jnp.broadcast_to(count, (BINS, 128))
    high, low = split(count)
    below = (
        lax.broadcasted_iota(I32, (BINS, BINS), 0) > lax.broadcasted_iota(I32, (BINS, BINS), 1)
    ).astype(BF16)
    start = jnp.dot(below, high, preferred_element_type=F32)
    start = start + jnp.dot(below, low, preferred_element_type=F32)
    opening = lax.broadcasted_iota(I32, (BINS, 128), 1).astype(F32) * TILE
    present = jnp.sum(count, axis=0, keepdims=True)
    closing = jnp.minimum(opening + TILE, present)
    first_bin = jnp.sum(jnp.where(start + count <= opening, 1.0, 0.0), axis=0, keepdims=True)
    last_bin = jnp.sum(jnp.where(start < closing, 1.0, 0.0), axis=0, keepdims=True) - 1.0
    edge_v[...] = jnp.concatenate(
        [first_bin, last_bin, present, jnp.zeros((5, 128), F32)], axis=0
    ).astype(I32)
    to_scalars = pltpu.make_async_copy(edge_v, edge, edge_sem)
    to_scalars.start()
    start = start[:, 0:1]
    for q in range(every):
        hits = hit_s[q * BINS : (q + 1) * BINS, :]
        ranked = rank_s[q * BINS : (q + 1) * BINS, :] + (carries[q] + start)
        slot = jnp.sum(hits * ranked, axis=0, keepdims=True)
        there = jnp.sum(hits, axis=0, keepdims=True)
        slot_s[q : q + 1, :] = jnp.where(there > 0.5, slot, -1.0)
        m = chunk(q)
        if q < chunks:
            source = jnp.zeros((1, TILE), F32)
        else:
            source = jnp.full((1, TILE), float(q - chunks + 1), F32)
        filled = jnp.concatenate([m[0:23], source, jnp.zeros((8, TILE), F32)], axis=0)
        pay3[q] = terms(filled)
    acted[...] = jnp.zeros_like(acted)

    def start_from(p, _):
        rhs[p] = rhs_in[p]
        return 0

    lax.fori_loop(0, rhs.shape[0], start_from, 0)
    slot_id = lax.broadcasted_iota(I32, (TILE, TILE), 0).astype(F32)

    def gather(n):
        wanted = slot_id + (n * TILE).astype(F32)
        moved = None
        for q in range(every):
            hit = jnp.where(wanted == slot_s[q : q + 1, :], 1.0, 0.0).astype(BF16)
            part = lax.dot_general(
                hit, pay3[q], (((1,), (1,)), ((), ())), preferred_element_type=F32
            )
            moved = part if moved is None else moved + part
        moved = jnp.concatenate([moved, jnp.zeros((TILE, 32), F32)], axis=1).T
        return moved[0:32] + moved[32:64] + moved[64:96]

    def prepare(m):
        cell_y = m[13:14].astype(I32)
        cell_z = m[14:15].astype(I32)
        z = lax.broadcasted_iota(I32, (extent_z, TILE), 0)
        table = pick((z - cell_z) & (extent_z - 1), [m[8 + i : 9 + i] for i in range(4)])
        high, low = split(table)
        y = lax.broadcasted_iota(I32, (ROWS, TILE), 0) - 2
        table_y = pick(y - cell_y, [m[4 + i : 5 + i] for i in range(4)])
        return high, low, table_y

    def x_table(m, plane):
        x = lax.broadcasted_iota(I32, (8, TILE), 0)
        return pick(x + plane - m[12:13].astype(I32), [m[i : i + 1] for i in range(4)])

    def sample(m, plane, high, low, table_y, totals):
        table_x = x_table(m, plane)
        folded_y = table_y.reshape(ROWS // 8, 8, TILE)
        both = fhl[pl.ds(plane, WINDOW)].reshape(WINDOW * 3 * ROWS, 2 * extent_z)
        left = jnp.concatenate([both, both[:, 0:extent_z]], axis=1)
        right = jnp.concatenate([high, high, low], axis=0)
        part = jnp.dot(left, right, preferred_element_type=F32)
        part = part.reshape(WINDOW, 3, ROWS // 8, 8, TILE)
        result = []
        for c in range(3):
            total = totals[c]
            for p in range(WINDOW):
                total = total + jnp.sum(part[p, c] * folded_y, axis=0) * table_x[p : p + 1]
            result.append(total)
        return tuple(result)

    def act(m, totals):
        totals = [jnp.sum(total, axis=0, keepdims=True) for total in totals]
        force = [m[16 + c : 17 + c] - totals[c] for c in range(3)]
        torque = cross([m[19 + c : 20 + c] for c in range(3)], force)
        acting = jnp.concatenate(force + list(torque) + [jnp.zeros((2, TILE), F32)], axis=0)
        group = m[23:24] * 2.0 + m[15:16]
        member = (
            (lax.broadcasted_iota(I32, (128, TILE), 0).astype(F32) == group)
            & (m[22:23] > 0.5)
        ).astype(F32)
        summed = lax.dot_general(
            terms(acting),
            member.astype(BF16),
            (((1,), (1,)), ((), ())),
            preferred_element_type=F32,
        )
        acted[...] += summed[0:8] + summed[8:16] + summed[16:24]
        return force

    def deposit(m, plane, force, z_high, z_low, table_y):
        table_x = x_table(m, plane)
        rows = []
        for p in range(WINDOW):
            for c in range(3):
                rows.append((force[c] * table_x[p : p + 1]) * table_y)
        high, low = split(jnp.concatenate(rows, axis=0))
        left = jnp.concatenate([high, low, high], axis=1)
        right = jnp.concatenate([z_high, z_high, z_low], axis=1)
        added = lax.dot_general(
            left, right, (((1,), (1,)), ((), ())), preferred_element_type=F32
        )
        rhs[pl.ds(plane + 2, WINDOW)] += added.reshape(WINDOW, 3, ROWS, extent_z)

    held[0] = gather(jnp.int32(0))
    to_scalars.wait()
    tiles = lax.shift_right_logical(edge[2, 0] + (TILE - 1), TILE.bit_length() - 1)
    nothing = (jnp.zeros((8, TILE), F32),) * 3

    def work(n, _):
        low_plane = edge[0, n]
        spans = (edge[1, n] + 3 - low_plane + WINDOW) // WINDOW
        slot = n & 1

        @pl.when(spans <= 1)
        def _narrow():
            m = held[slot]
            high, low, table_y = prepare(m)
            totals = sample(m, low_plane, high, low, table_y, nothing)
            following = gather(n + 1)
            force = act(m, totals)
            deposit(m, low_plane, force, high, low, table_y)
            held[1 - slot] = following

        @pl.when(spans > 1)
        def _wide():
            m = held[slot]
            high, low, table_y = prepare(m)
            tz[0] = high
            tz[1] = low

            def sample_span(j, totals):
                plane = low_plane + j * WINDOW
                return sample(held[slot], plane, tz[0], tz[1], table_y, totals)

            force = act(m, lax.fori_loop(0, spans, sample_span, nothing))

            def deposit_span(j, _):
                plane = low_plane + j * WINDOW
                deposit(held[slot], plane, force, tz[0], tz[1], table_y)
                return 0

            lax.fori_loop(0, spans, deposit_span, 0)
            held[1 - slot] = gather(n + 1)

        return 0

    lax.fori_loop(0, tiles, work, 0)


def wall_masks(gy, n_gy, span_y, extent_z):
    y = lax.broadcasted_iota(I32, (ROWS, extent_z), 0)
    low_edge = jnp.where(gy > 0, 0, HALO)
    high_edge = jnp.where(gy < n_gy - 1, ROWS, HALO + span_y)
    inside = jnp.where((y >= low_edge) & (y < high_edge), 1.0, 0.0).astype(F32)
    inside = jnp.concatenate([inside] * 3, axis=0)
    return inside, inside * (1.0 / (1.0 + 6.0 * DIFFUSION))


def relaxed(rhs, before, centre, after, scale):
    shape = rhs.shape
    flat = scale.shape
    centre = centre.reshape(flat)
    total = rhs.reshape(flat) + before.reshape(flat) + after.reshape(flat)
    total = total + pltpu.roll(centre, 1, 0) + pltpu.roll(centre, flat[0] - 1, 0)
    total = total + pltpu.roll(centre, 1, 1) + pltpu.roll(centre, flat[1] - 1, 1)
    return (total * scale).reshape(shape)


def strip_kernel(
    n_gx,
    n_gy,
    per_sphere,
    rhs,
    acted,
    mot_ref,
    cs_ref,
    cp_ref,
    nm_ref,
    ybuf,
    xbuf,
    mid_0,
    mid_1,
    mid_2,
    mid_3,
    done,
    sums,
    ret,
    agx,
    agy,
    ag1,
    moved_s,
    staged,
    ret_send,
    ret_recv,
    agx_send,
    agx_recv,
    agy_send,
    agy_recv,
    y_send,
    y_recv,
    x_send,
    x_recv,
):
    gx, gy, at = neighbours(n_gx, n_gy)
    here = gx * n_gy + gy
    planes = ybuf.shape[1]
    span_y = done.shape[2]
    peers = (
        [at(k, 0) for k in range(1, n_gx)]
        + [at(0, k) for k in range(1, n_gy)]
        + [at(dx, dy) for dx in (-1, 1) for dy in (-1, 1)]
    )
    barrier = greet(peers)
    inner_low = jnp.where(gy > 0, 1.0, 0.0).astype(F32)
    inner_high = jnp.where(gy < n_gy - 1, 1.0, 0.0).astype(F32)
    for n in range(8):
        sums[n] = pltpu.roll(acted[...], 128 - 2 * (n + 1), 1)
    replies = [
        remote(sums.at[n], ret.at[n], ret_send.at[n], ret_recv.at[n], at(-dx, -dy))
        for n, (dx, dy) in enumerate(LANES)
    ]
    lanes = lax.broadcasted_iota(I32, (8, 128), 1)
    row_id = lax.broadcasted_iota(I32, (8, 128), 0)
    pl.semaphore_wait(barrier, len(peers))

    def along_x(k):
        return remote(ag1.at[0], agx.at[k], agx_send.at[k], agx_recv.at[k], at(k, 0))

    def along_y(k):
        return remote(ag1.at[1], agy.at[k], agy_send.at[k], agy_recv.at[k], at(0, k))

    def sphere_step_one():
        for copy in replies:
            copy.wait()
        total = acted[...]
        for n in range(8):
            total = total + ret[n]
        start = jnp.zeros((8, 128), F32)
        for c in range(6):
            for s in range(2):
                start = jnp.where((row_id == c) & (lanes == s), mot_ref[s, c], start)
        moved = start - total * (RESPONSE / per_sphere)
        moved_s[...] = moved
        first = jnp.broadcast_to(moved[:, 0:1], (8, 128))
        other = pltpu.roll(jnp.broadcast_to(moved[:, 1:2], (8, 128)), 3, 0)
        ag1[0] = jnp.where(lanes == here, jnp.where(row_id < 3, first, other), 0.0)
        for k in range(1, n_gx):
            along_x(k).start()

    def sphere_step_two():
        for k in range(1, n_gx):
            along_x(k).wait()
        total = ag1[0]
        for k in range(1, n_gx):
            total = total + agx[k]
        ag1[1] = total
        for k in range(1, n_gy):
            along_y(k).start()

    def sphere_step_three():
        for k in range(1, n_gy):
            along_y(k).wait()
        total = ag1[1]
        for k in range(1, n_gy):
            total = total + agy[k]
        moved = moved_s[...]
        pull = jnp.zeros((8, 128), F32)
        for k in range(cs_ref.shape[0]):
            partner = cp_ref[k]
            own = cs_ref[k] - 2 * here
            chosen = jnp.sum(
                jnp.where(lanes == lax.shift_right_logical(partner, 1), total, 0.0),
                axis=1,
                keepdims=True,
            )
            chosen = jnp.broadcast_to(chosen, (8, 128))
            odd = jnp.broadcast_to(partner & 1, (8, 128)) == 1
            chosen = jnp.where(odd, pltpu.roll(chosen, 5, 0), chosen)
            pull = pull + jnp.where((lanes == own) & (row_id < 3), chosen - moved, 0.0)
        settled = jnp.concatenate(
            [moved + DASHPOT * pull, jnp.zeros((120, 128), F32)], axis=0
        )
        nm_ref[...] = settled.T[0:2, 0:6]

    def y_copies(g):
        copies = []
        for r, (first, count) in enumerate(RUNS[g]):
            lo = first + 2
            base = 4 * g + 2 * r
            copies.append(
                remote(
                    rhs.at[pl.ds(lo, count), :, pl.ds(0, 8)],
                    ybuf.at[1, pl.ds(first, count)],
                    y_send.at[base],
                    y_recv.at[base],
                    at(0, -1),
                )
            )
            copies.append(
                remote(
                    rhs.at[pl.ds(lo, count), :, pl.ds(ROWS - 8, 8)],
                    ybuf.at[0, pl.ds(first, count)],
                    y_send.at[base + 1],
                    y_recv.at[base + 1],
                    at(0, 1),
                )
            )
        return copies

    def x_copies(g):
        (low, count), (high, _) = RUNS[g]
        high = high - (planes - 6)
        return [
            remote(
                staged.at[1, pl.ds(low, count)],
                xbuf.at[1, pl.ds(low, count)],
                x_send.at[2 * g],
                x_recv.at[2 * g],
                at(-1, 0),
            ),
            remote(
                staged.at[0, pl.ds(high, count)],
                xbuf.at[0, pl.ds(high, count)],
                x_send.at[2 * g + 1],
                x_recv.at[2 * g + 1],
                at(1, 0),
            ),
        ]

    def with_strips(p):
        whole = rhs[p + 2]
        low = whole[:, 0:8] + ybuf[0, p] * inner_low
        high = whole[:, ROWS - 8 : ROWS] + ybuf[1, p] * inner_high
        return jnp.concatenate([low, whole[:, 8 : ROWS - 8], high], axis=1)

    def stage(g):
        for side, base in ((1, 0), (0, planes - 6)):
            first, count = RUNS[g][1 - side]
            for p in range(first, first + count):
                staged[side, p - base] = with_strips(p)

    for g in range(2):
        for copy in y_copies(g):
            copy.start()
    for copy in replies:
        copy.start()
    for g in range(2, 4):
        for copy in y_copies(g):
            copy.start()
    for g in range(2):
        for copy in y_copies(g):
            copy.wait()
        stage(g)
        for copy in x_copies(g):
            copy.start()
    sphere_step_one()
    for copy in y_copies(2):
        copy.wait()
    stage(2)
    for copy in x_copies(2):
        copy.start()
    for copy in y_copies(3):
        copy.wait()
    inside, scale = wall_masks(gy, n_gy, span_y, rhs.shape[3])
    span_mid = mid_0.shape[0]

    def begin(i, _):
        mid_0[i] = (with_strips(i + 4).reshape(inside.shape) * inside).reshape(mid_0.shape[1:])
        return 0

    lax.fori_loop(0, span_mid, begin, 0)
    sphere_step_two()
    stages = (mid_0, mid_1, mid_2, mid_3)
    for k in range(1, ITERS):
        source, target = stages[k - 1], stages[k]

        def step(s, _, source=source, target=target, k=k):
            for u in range(2):
                i = 2 * s + u
                target[i] = relaxed(
                    mid_0[i + k], source[i], source[i + 1], source[i + 2], scale
                )
            return 0

        lax.fori_loop(0, (span_mid - 2 * k) // 2, step, 0)
    for i in range(span_mid - 2 * ITERS):
        result = relaxed(mid_0[i + ITERS], mid_3[i], mid_3[i + 1], mid_3[i + 2], scale)
        for c in range(3):
            done[c, i] = result[c, HALO : HALO + span_y, :]
    sphere_step_three()
    for g in range(3):
        for copy in x_copies(g):
            copy.wait()


def relax_kernel(
    n_gy,
    rhs_in,
    ybuf,
    xbuf,
    mid_0,
    mid_1,
    mid_2,
    mid_3,
    done,
    out_ref,
    rhs,
    one,
    two,
    three,
    staged,
    sems,
    done_sem,
):
    gy = lax.axis_index("gy")
    planes = ybuf.shape[1]
    span_x = planes - 4
    span_y = out_ref.shape[2]
    whole_span = planes + 4
    middle = pltpu.make_async_copy(done, out_ref.at[:, 6 : span_x - 6], done_sem)
    middle.start()
    inside, scale = wall_masks(gy, n_gy, span_y, rhs.shape[3])
    inner_low = jnp.where(gy > 0, 1.0, 0.0).astype(F32)
    inner_high = jnp.where(gy < n_gy - 1, 1.0, 0.0).astype(F32)
    for i in range(6):
        for x, beside in ((i, xbuf[0, i]), (planes - 2 + i, xbuf[1, i])):
            whole = rhs_in[x] + beside
            if 2 <= x < planes + 2:
                low = whole[:, 0:8] + ybuf[0, x - 2] * inner_low
                high = whole[:, ROWS - 8 : ROWS] + ybuf[1, x - 2] * inner_high
                whole = jnp.concatenate([low, whole[:, 8 : ROWS - 8], high], axis=1)
            rhs[x] = (whole.reshape(inside.shape) * inside).reshape(whole.shape)
    stages = (rhs, one, two, three)
    for k, (mid, count) in enumerate(((mid_0, 4), (mid_1, 2), (mid_2, 2), (mid_3, 2))):
        for i in range(count):
            stages[k][6 + k + i] = mid[i]
            stages[k][whole_span - 7 - k - i] = mid[mid.shape[0] - 1 - i]

    def swept(k, x):
        source = stages[k - 1]
        return relaxed(rhs[x], source[x - 1], source[x], source[x + 1], scale)

    for k in range(1, ITERS):

        def step(s, _, k=k):
            for u in range(2):
                low = k + 2 * s + u
                high = whole_span - 6 - k + 2 * s + u
                stages[k][low] = swept(k, low)
                stages[k][high] = swept(k, high)
            return 0

        lax.fori_loop(0, 3, step, 0)

    def stores(s):
        return [
            pltpu.make_async_copy(
                staged.at[:, pl.ds(first + 2 * s, 2)],
                out_ref.at[:, pl.ds(first + 2 * s, 2)],
                sems.at[2 * s + side],
            )
            for side, first in enumerate((0, span_x - 6))
        ]

    def final(s, _):
        for u in range(2):
            for first in (0, span_x - 6):
                x = first + 2 * s + u
                result = swept(ITERS, x + HALO)
                for c in range(3):
                    staged[c, x] = result[c, HALO : HALO + span_y, :]
        for copy in stores(s):
            copy.start()
        return 0

    lax.fori_loop(0, 3, final, 0)
    for s in range(3):
        for copy in stores(s):
            copy.wait()
    middle.wait()


def on_device(
    n_gx,
    n_gy,
    velocity,
    owner_block,
    base_x,
    base_y,
    base_z,
    delta_weights,
    marker_offset,
    sphere_motion,
    contact_sphere,
    contact_partner,
):
    span_x, span_y, extent_z = velocity.shape[1:]
    markers = base_x.shape[0]
    planes = span_x + 4
    every = markers // TILE + 8
    padded = planes + WINDOW - 1
    grown = (padded + 2, 3, ROWS, extent_z)
    vmem = pl.BlockSpec(memory_space=pltpu.VMEM)
    smem = pl.BlockSpec(memory_space=pltpu.SMEM)
    hbm = pl.BlockSpec(memory_space=pltpu.HBM)
    dma = pltpu.SemaphoreType.DMA
    motion = sphere_motion.T
    fhl, started, home, arrived = pl.pallas_call(
        functools.partial(request_kernel, n_gx, n_gy),
        out_shape=(
            jax.ShapeDtypeStruct((padded, 3 * ROWS, 2 * extent_z), BF16),
            jax.ShapeDtypeStruct(grown, F32),
            jax.ShapeDtypeStruct((32, markers), F32),
            jax.ShapeDtypeStruct((8, 24, TILE), F32),
        ),
        in_specs=[hbm] * 8,
        out_specs=(vmem,) * 4,
        scratch_shapes=[
            pltpu.VMEM(velocity.shape, F32),
            pltpu.VMEM((1, markers), I32),
            pltpu.VMEM((1, markers), I32),
            pltpu.VMEM((1, markers), I32),
            pltpu.VMEM((1, markers), I32),
            pltpu.VMEM((12, markers), F32),
            pltpu.VMEM((3, markers), F32),
            pltpu.SMEM((2, 6), F32),
            pltpu.VMEM((2, 3, 2, span_y, extent_z), F32),
            pltpu.VMEM((2, 3, span_x, 8, extent_z), F32),
            pltpu.VMEM((4, 16, extent_z), F32),
            pltpu.VMEM((4, 16, extent_z), F32),
            pltpu.VMEM((32, markers), F32),
            pltpu.VMEM((96, markers), BF16),
            pltpu.VMEM((8, TILE), F32),
            pltpu.VMEM((8, 24, TILE), F32),
            pltpu.VMEM((8, 24, TILE), F32),
            pltpu.VMEM((planes, 3, ROWS, extent_z), F32),
            dma((8,)),
            dma((8,)),
            dma((8,)),
            dma((8,)),
            dma((8,)),
        ],
        compiler_params=pltpu.CompilerParams(
            collective_id=0, has_side_effects=True, vmem_limit_bytes=24 << 20
        ),
        name="requests",
    )(
        *(
            pltpu.with_memory_space_constraint(array, pltpu.HBM)
            for array in (
                velocity,
                owner_block.reshape(1, markers),
                base_x.reshape(1, markers),
                base_y.reshape(1, markers),
                base_z.reshape(1, markers),
                delta_weights,
                marker_offset,
                motion,
            )
        )
    )
    rhs, acted = pl.pallas_call(
        marker_kernel,
        out_shape=(
            jax.ShapeDtypeStruct(grown, F32),
            jax.ShapeDtypeStruct((8, 128), F32),
        ),
        in_specs=[vmem] * 4,
        out_specs=(vmem,) * 2,
        scratch_shapes=[
            pltpu.VMEM((every, 96, TILE), BF16),
            pltpu.VMEM((every * BINS, TILE), F32),
            pltpu.VMEM((every * BINS, TILE), F32),
            pltpu.VMEM((every, TILE), F32),
            pltpu.VMEM((2, extent_z, TILE), BF16),
            pltpu.VMEM((2, 32, TILE), F32),
            pltpu.VMEM((8, 128), I32),
            pltpu.SMEM((8, 128), I32),
            dma,
        ],
        compiler_params=pltpu.CompilerParams(vmem_limit_bytes=24 << 20),
        name="markers",
    )(fhl, started, home, arrived)
    plane = (3, ROWS, extent_z)
    middle = planes - 8
    new_motion, *strips = pl.pallas_call(
        functools.partial(strip_kernel, n_gx, n_gy, markers // 2),
        out_shape=(
            jax.ShapeDtypeStruct(motion.shape, F32),
            jax.ShapeDtypeStruct((2, planes, 3, 8, extent_z), F32),
            jax.ShapeDtypeStruct((2, 6, 3, ROWS, extent_z), F32),
            jax.ShapeDtypeStruct((middle,) + plane, F32),
            jax.ShapeDtypeStruct((middle - 2,) + plane, F32),
            jax.ShapeDtypeStruct((middle - 4,) + plane, F32),
            jax.ShapeDtypeStruct((middle - 6,) + plane, F32),
            jax.ShapeDtypeStruct((3, middle - 8, span_y, extent_z), F32),
        ),
        in_specs=[vmem] * 2 + [smem] * 3,
        out_specs=(vmem,) * 8,
        scratch_shapes=[
            pltpu.VMEM((8, 8, 128), F32),
            pltpu.VMEM((8, 8, 128), F32),
            pltpu.VMEM((n_gx, 8, 128), F32),
            pltpu.VMEM((n_gy, 8, 128), F32),
            pltpu.VMEM((2, 8, 128), F32),
            pltpu.VMEM((8, 128), F32),
            pltpu.VMEM((2, 6, 3, ROWS, extent_z), F32),
            dma((8,)),
            dma((8,)),
            dma((n_gx,)),
            dma((n_gx,)),
            dma((n_gy,)),
            dma((n_gy,)),
            dma((16,)),
            dma((16,)),
            dma((6,)),
            dma((6,)),
        ],
        compiler_params=pltpu.CompilerParams(
            collective_id=1, has_side_effects=True, vmem_limit_bytes=24 << 20
        ),
        name="strips",
    )(rhs, acted, motion, contact_sphere, contact_partner)
    velocity_star = pl.pallas_call(
        functools.partial(relax_kernel, n_gy),
        out_shape=jax.ShapeDtypeStruct(velocity.shape, F32),
        in_specs=[vmem] * 8,
        out_specs=pl.BlockSpec(memory_space=pltpu.HBM),
        scratch_shapes=[pltpu.VMEM((planes + 4,) + plane, F32)] * 4
        + [
            pltpu.VMEM(velocity.shape, F32),
            dma((6,)),
            dma,
        ],
        compiler_params=pltpu.CompilerParams(vmem_limit_bytes=24 << 20),
        name="relax",
    )(rhs, *strips)
    return velocity_star, new_motion.T


def solution(mesh):
    placed = (
        P(None, "gx", "gy", None),
        P(("gx", "gy"), None),
        P(("gx", "gy")),
        P(("gx", "gy")),
        P(("gx", "gy")),
        P(None, ("gx", "gy")),
        P(None, ("gx", "gy")),
        P(None, ("gx", "gy")),
        P(("gx", "gy")),
        P(("gx", "gy")),
    )
    return jax.shard_map(
        functools.partial(on_device, mesh.shape["gx"], mesh.shape["gy"]),
        mesh=mesh,
        in_specs=placed,
        out_specs=(P(None, "gx", "gy", None), P(None, ("gx", "gy"))),
        check_vma=False,
    )
```

```python
import functools

import jax
import jax.numpy as jnp
from jax import lax
from jax.experimental import pallas as pl
from jax.experimental.pallas import tpu as pltpu
from jax.sharding import PartitionSpec as P

F32 = jnp.float32
BF16 = jnp.bfloat16
I32 = jnp.int32
MESH = pl.DeviceIdType.MESH

ITERS = 4
DIFFUSION = 1.0
RESPONSE = 0.5
DASHPOT = 0.1

TILE = 256
BINS = 32
WINDOW = 6
ROWS = 40
HALO = 4
LANES = [(dx, dy) for dx in (-1, 0, 1) for dy in (-1, 0, 1) if (dx, dy) != (0, 0)]
DIAGONALS = [(dx, dy) for dx, dy in LANES if dx * dy != 0]
RUNS = [((0, 1), (19, 1)), ((1, 2), (17, 2)), ((3, 3), (14, 3)), ((6, 8),)]


def split(values):
    high = values.astype(BF16)
    low = (values - high.astype(F32)).astype(BF16)
    return high, low


def pick(distance, weights):
    result = jnp.where(distance == 3, weights[3], 0.0)
    for k in (2, 1, 0):
        result = jnp.where(distance == k, weights[k], result)
    return result


def cross(a, b):
    return (
        a[1] * b[2] - a[2] * b[1],
        a[2] * b[0] - a[0] * b[2],
        a[0] * b[1] - a[1] * b[0],
    )


def remote(src, dst, send, recv, peer):
    return pltpu.make_async_remote_copy(
        src_ref=src,
        dst_ref=dst,
        send_sem=send,
        recv_sem=recv,
        device_id=peer,
        device_id_type=MESH,
    )


def greet(peers):
    barrier = pltpu.get_barrier_semaphore()
    for peer in peers:
        pl.semaphore_signal(barrier, inc=1, device_id=peer, device_id_type=MESH)
    return barrier


def neighbours(n_gx, n_gy):
    gx = lax.axis_index("gx")
    gy = lax.axis_index("gy")

    def at(dx, dy):
        return (lax.rem(gx + (dx + n_gx), n_gx), lax.rem(gy + (dy + n_gy), n_gy))

    return gx, gy, at


def terms(values):
    parts = []
    rest = values
    for _ in range(3):
        part = rest.astype(BF16)
        parts.append(part)
        rest = rest - part.astype(F32)
    return jnp.concatenate(parts, axis=0)


def chosen_columns(parts, slots, first):
    wanted = lax.broadcasted_iota(I32, (TILE, TILE), 0).astype(F32) + first
    hit = jnp.where(wanted == slots, 1.0, 0.0).astype(BF16)
    return lax.dot_general(parts, hit, (((1,), (1,)), ((), ())), preferred_element_type=F32)


def ranks(hits, above):
    return jnp.dot(hits.astype(BF16), above, preferred_element_type=F32)


def strictly_above(size):
    return (
        lax.broadcasted_iota(I32, (size, size), 0) < lax.broadcasted_iota(I32, (size, size), 1)
    ).astype(BF16)


def request_kernel(
    n_gx,
    n_gy,
    v_hbm,
    own_hbm,
    bx_hbm,
    by_hbm,
    bz_hbm,
    dw_hbm,
    off_hbm,
    mot_hbm,
    fhl,
    rhs,
    home,
    arrived,
    v_ref,
    own_ref,
    bx_ref,
    by_ref,
    bz_ref,
    dw_ref,
    off_ref,
    mot_ref,
    hx,
    hy,
    hc,
    corner,
    edges,
    pay,
    pay3,
    slot_s,
    snd,
    inbox,
    frame,
    in_sem,
    halo_send,
    halo_recv,
    pay_send,
    pay_recv,
):
    gx, gy, at = neighbours(n_gx, n_gy)
    here = gx * n_gy + gy
    barrier = greet([at(dx, dy) for dx, dy in LANES])
    loads = [
        pltpu.make_async_copy(src, dst, in_sem.at[i])
        for i, (src, dst) in enumerate(
            (
                (v_hbm, v_ref),
                (own_hbm, own_ref),
                (bx_hbm, bx_ref),
                (by_hbm, by_ref),
                (bz_hbm, bz_ref),
                (dw_hbm, dw_ref),
                (off_hbm, off_ref),
                (mot_hbm, mot_ref),
            )
        )
    ]
    for copy in loads:
        copy.start()
    markers = dw_ref.shape[1]
    chunks = markers // TILE
    span_x = v_ref.shape[1]
    span_y = v_ref.shape[2]
    extent_z = v_ref.shape[3]
    planes = span_x + 4
    for copy in loads:
        copy.wait()

    last = span_x - 2
    pl.semaphore_wait(barrier, len(LANES))
    halo = []
    halo.append(remote(v_ref.at[:, 0:2], hx.at[1], halo_send.at[0], halo_recv.at[0], at(-1, 0)))
    halo.append(
        remote(v_ref.at[:, last:span_x], hx.at[0], halo_send.at[1], halo_recv.at[1], at(1, 0))
    )
    halo.append(remote(edges.at[0], hy.at[1], halo_send.at[2], halo_recv.at[2], at(0, -1)))
    halo.append(remote(edges.at[1], hy.at[0], halo_send.at[3], halo_recv.at[3], at(0, 1)))
    for k, (dx, dy) in enumerate(DIAGONALS):
        slot = (1 if dx < 0 else 0) * 2 + (1 if dy < 0 else 0)
        halo.append(
            remote(
                corner.at[k], hc.at[slot], halo_send.at[4 + k], halo_recv.at[4 + k], at(dx, dy)
            )
        )
    for copy in halo[0:2]:
        copy.start()
    corner[...] = jnp.zeros_like(corner)
    for k, (dx, dy) in enumerate(DIAGONALS):
        x0 = 0 if dx < 0 else last
        y0 = 0 if dy < 0 else span_y - 2
        for c in range(3):
            for i in range(2):
                row = 4 * c + 2 * i
                corner[k, row : row + 2, :] = v_ref[c, x0 + i, y0 : y0 + 2, :]
    for side, y0 in enumerate((0, span_y - 2)):
        for c in range(3):
            for x in range(span_x):
                edges[side, c, 2 * x : 2 * x + 2, :] = v_ref[c, x, y0 : y0 + 2, :]
    for copy in halo[2:]:
        copy.start()

    pay[0:12, :] = dw_ref[...]
    pay[12:13, :] = bx_ref[...].astype(F32)
    pay[13:14, :] = by_ref[...].astype(F32)
    pay[14:15, :] = bz_ref[...].astype(F32)
    per_sphere = markers // 2
    second = (lax.broadcasted_iota(I32, (1, markers), 1) >= per_sphere).astype(F32)
    pay[15:16, :] = second
    motion = [mot_ref[0, c] * (1.0 - second) + mot_ref[1, c] * second for c in range(6)]
    offset = [off_ref[c : c + 1, :] for c in range(3)]
    swing = cross(motion[3:6], offset)
    for c in range(3):
        pay[16 + c : 17 + c, :] = motion[c] + swing[c]
        pay[19 + c : 20 + c, :] = offset[c]
    pay[22:23, :] = jnp.ones((1, markers), F32)
    pay[23:32, :] = jnp.zeros((9, markers), F32)
    whole = pay[...]
    pay3[...] = terms(whole)
    home[...] = whole
    home[22:23, :] = (own_ref[...] == here).astype(F32)

    above = strictly_above(TILE)
    bins = lax.broadcasted_iota(I32, (8, TILE), 0)
    carry = jnp.zeros((8, 1), F32)
    for q in range(chunks):
        owner = own_ref[:, q * TILE : (q + 1) * TILE]
        owner_x = lax.shift_right_logical(owner, n_gy.bit_length() - 1)
        owner_y = owner & (n_gy - 1)
        step_x = (owner_x - gx + 1) & (n_gx - 1)
        lane = step_x * 3 + (owner_y - gy + 1)
        lane = jnp.where(owner == here, -1, jnp.where(lane > 4, lane - 1, lane))
        hits = jnp.where(bins == lane, 1.0, 0.0)
        ranked = ranks(hits, above) + carry + bins.astype(F32) * TILE
        carry = carry + jnp.sum(hits, axis=1, keepdims=True)
        slot = jnp.sum(hits * ranked, axis=0, keepdims=True)
        slot_s[q : q + 1, :] = jnp.where(lane < 0, -1.0, slot)

    def compact(n, _):
        first = (n * TILE).astype(F32)
        moved = None
        for q in range(chunks):
            part = chosen_columns(
                pay3[:, q * TILE : (q + 1) * TILE], slot_s[q : q + 1, :], first
            )
            moved = part if moved is None else moved + part
        snd[n] = moved[0:24] + moved[32:56] + moved[64:88]
        return 0

    lax.fori_loop(0, 8, compact, 0)

    requests = [
        remote(snd.at[n], inbox.at[n], pay_send.at[n], pay_recv.at[n], at(dx, dy))
        for n, (dx, dy) in enumerate(LANES)
    ]
    for copy in requests:
        copy.start()

    inner_low = jnp.where(gy > 0, 1.0, 0.0).astype(F32)
    inner_high = jnp.where(gy < n_gy - 1, 1.0, 0.0).astype(F32)

    def clear(p, _):
        rhs[p] = jnp.zeros((3, ROWS, extent_z), F32)
        return 0

    lax.fori_loop(0, rhs.shape[0], clear, 0)

    def clear_frame(p, _):
        frame[p] = jnp.zeros((3, ROWS, extent_z), F32)
        return 0

    lax.fori_loop(0, planes, clear_frame, 0)

    def clear_beyond(p, _):
        fhl[p] = jnp.zeros((3 * ROWS, 2 * extent_z), BF16)
        return 0

    lax.fori_loop(planes, fhl.shape[0], clear_beyond, 0)

    def place(x, _):
        for c in range(3):
            plane = v_ref[c, x]
            frame[x + 2, c, 4 : 4 + span_y, :] = plane
            rhs[x + 4, c, 4 : 4 + span_y, :] = plane
        return 0

    lax.fori_loop(0, span_x, place, 0)
    for copy in halo:
        copy.wait()

    for x in range(span_x):
        for c in range(3):
            frame[x + 2, c, 2:4, :] = hy[0, c, 2 * x : 2 * x + 2, :] * inner_low
            frame[x + 2, c, 36:38, :] = hy[1, c, 2 * x : 2 * x + 2, :] * inner_high
    for side in range(2):
        for i in range(2):
            p = (0 if side == 0 else planes - 2) + i
            for c in range(3):
                frame[p, c, 4 : 4 + span_y, :] = hx[side, c, i]
                frame[p, c, 2:4, :] = hc[side * 2, 4 * c + 2 * i : 4 * c + 2 * i + 2, :] * inner_low
                frame[p, c, 36:38, :] = (
                    hc[side * 2 + 1, 4 * c + 2 * i : 4 * c + 2 * i + 2, :] * inner_high
                )

    def halve(p, _):
        high, low = split(frame[p].reshape(3 * ROWS, extent_z))
        fhl[p, :, 0:extent_z] = high
        fhl[p, :, extent_z : 2 * extent_z] = low
        return 0

    lax.fori_loop(0, planes, halve, 0)
    for copy in requests:
        copy.wait()
    arrived[...] = inbox[...]


def marker_kernel(
    fhl,
    rhs_in,
    home,
    arrived,
    rhs,
    acted,
    pay3,
    hit_s,
    rank_s,
    slot_s,
    tz,
    held,
    edge_v,
    edge,
    edge_sem,
):
    chunks = home.shape[1] // TILE
    every = chunks + 8
    extent_z = rhs.shape[3]
    bins = lax.broadcasted_iota(I32, (BINS, TILE), 0).astype(F32)

    def chunk(q):
        return home[0:24, q * TILE : (q + 1) * TILE] if q < chunks else arrived[q - chunks]

    totals = []
    for q in range(every):
        m = chunk(q)
        hits = jnp.where((bins == m[12:13]) & (m[22:23] > 0.5), 1.0, 0.0)
        hit_s[q * BINS : (q + 1) * BINS, :] = hits
        totals.append(jnp.sum(hits, axis=1, keepdims=True))
    rank_s[...] = ranks(hit_s[...], strictly_above(TILE))
    carries = []
    count = jnp.zeros((BINS, 1), F32)
    for q in range(every):
        carries.append(count)
        count = count + totals[q]
    count = jnp.broadcast_to(count, (BINS, 128))
    high, low = split(count)
    below = (
        lax.broadcasted_iota(I32, (BINS, BINS), 0) > lax.broadcasted_iota(I32, (BINS, BINS), 1)
    ).astype(BF16)
    start = jnp.dot(below, high, preferred_element_type=F32)
    start = start + jnp.dot(below, low, preferred_element_type=F32)
    opening = lax.broadcasted_iota(I32, (BINS, 128), 1).astype(F32) * TILE
    present = jnp.sum(count, axis=0, keepdims=True)
    closing = jnp.minimum(opening + TILE, present)
    first_bin = jnp.sum(jnp.where(start + count <= opening, 1.0, 0.0), axis=0, keepdims=True)
    last_bin = jnp.sum(jnp.where(start < closing, 1.0, 0.0), axis=0, keepdims=True) - 1.0
    edge_v[...] = jnp.concatenate(
        [first_bin, last_bin, present, jnp.zeros((5, 128), F32)], axis=0
    ).astype(I32)
    to_scalars = pltpu.make_async_copy(edge_v, edge, edge_sem)
    to_scalars.start()
    start = start[:, 0:1]
    for q in range(every):
        hits = hit_s[q * BINS : (q + 1) * BINS, :]
        ranked = rank_s[q * BINS : (q + 1) * BINS, :] + (carries[q] + start)
        slot = jnp.sum(hits * ranked, axis=0, keepdims=True)
        there = jnp.sum(hits, axis=0, keepdims=True)
        slot_s[q : q + 1, :] = jnp.where(there > 0.5, slot, -1.0)
        m = chunk(q)
        if q < chunks:
            source = jnp.zeros((1, TILE), F32)
        else:
            source = jnp.full((1, TILE), float(q - chunks + 1), F32)
        filled = jnp.concatenate([m[0:23], source, jnp.zeros((8, TILE), F32)], axis=0)
        pay3[q] = terms(filled)
    acted[...] = jnp.zeros_like(acted)

    def start_from(p, _):
        rhs[p] = rhs_in[p]
        return 0

    lax.fori_loop(0, rhs.shape[0], start_from, 0)
    slot_id = lax.broadcasted_iota(I32, (TILE, TILE), 0).astype(F32)

    def gather(n):
        wanted = slot_id + (n * TILE).astype(F32)
        moved = None
        for q in range(every):
            hit = jnp.where(wanted == slot_s[q : q + 1, :], 1.0, 0.0).astype(BF16)
            part = lax.dot_general(
                hit, pay3[q], (((1,), (1,)), ((), ())), preferred_element_type=F32
            )
            moved = part if moved is None else moved + part
        moved = jnp.concatenate([moved, jnp.zeros((TILE, 32), F32)], axis=1).T
        return moved[0:32] + moved[32:64] + moved[64:96]

    def prepare(m):
        cell_y = m[13:14].astype(I32)
        cell_z = m[14:15].astype(I32)
        z = lax.broadcasted_iota(I32, (extent_z, TILE), 0)
        table = pick((z - cell_z) & (extent_z - 1), [m[8 + i : 9 + i] for i in range(4)])
        high, low = split(table)
        y = lax.broadcasted_iota(I32, (ROWS, TILE), 0) - 2
        table_y = pick(y - cell_y, [m[4 + i : 5 + i] for i in range(4)])
        return high, low, table_y

    def x_table(m, plane):
        x = lax.broadcasted_iota(I32, (8, TILE), 0)
        return pick(x + plane - m[12:13].astype(I32), [m[i : i + 1] for i in range(4)])

    def sample(m, plane, high, low, table_y, totals):
        table_x = x_table(m, plane)
        folded_y = table_y.reshape(ROWS // 8, 8, TILE)
        both = fhl[pl.ds(plane, WINDOW)].reshape(WINDOW * 3 * ROWS, 2 * extent_z)
        left = jnp.concatenate([both, both[:, 0:extent_z]], axis=1)
        right = jnp.concatenate([high, high, low], axis=0)
        part = jnp.dot(left, right, preferred_element_type=F32)
        part = part.reshape(WINDOW, 3, ROWS // 8, 8, TILE)
        result = []
        for c in range(3):
            total = totals[c]
            for p in range(WINDOW):
                total = total + jnp.sum(part[p, c] * folded_y, axis=0) * table_x[p : p + 1]
            result.append(total)
        return tuple(result)

    def act(m, totals):
        totals = [jnp.sum(total, axis=0, keepdims=True) for total in totals]
        force = [m[16 + c : 17 + c] - totals[c] for c in range(3)]
        torque = cross([m[19 + c : 20 + c] for c in range(3)], force)
        acting = jnp.concatenate(force + list(torque) + [jnp.zeros((2, TILE), F32)], axis=0)
        group = m[23:24] * 2.0 + m[15:16]
        member = (
            (lax.broadcasted_iota(I32, (128, TILE), 0).astype(F32) == group)
            & (m[22:23] > 0.5)
        ).astype(F32)
        summed = lax.dot_general(
            terms(acting),
            member.astype(BF16),
            (((1,), (1,)), ((), ())),
            preferred_element_type=F32,
        )
        acted[...] += summed[0:8] + summed[8:16] + summed[16:24]
        return force

    def deposit(m, plane, force, z_high, z_low, table_y):
        table_x = x_table(m, plane)
        rows = []
        for p in range(WINDOW):
            for c in range(3):
                rows.append((force[c] * table_x[p : p + 1]) * table_y)
        high, low = split(jnp.concatenate(rows, axis=0))
        left = jnp.concatenate([high, low, high], axis=1)
        right = jnp.concatenate([z_high, z_high, z_low], axis=1)
        added = lax.dot_general(
            left, right, (((1,), (1,)), ((), ())), preferred_element_type=F32
        )
        rhs[pl.ds(plane + 2, WINDOW)] += added.reshape(WINDOW, 3, ROWS, extent_z)

    held[0] = gather(jnp.int32(0))
    to_scalars.wait()
    tiles = lax.shift_right_logical(edge[2, 0] + (TILE - 1), TILE.bit_length() - 1)
    nothing = (jnp.zeros((8, TILE), F32),) * 3

    def work(n, _):
        low_plane = edge[0, n]
        spans = (edge[1, n] + 3 - low_plane + WINDOW) // WINDOW
        slot = n & 1

        @pl.when(spans <= 1)
        def _narrow():
            m = held[slot]
            high, low, table_y = prepare(m)
            totals = sample(m, low_plane, high, low, table_y, nothing)
            following = gather(n + 1)
            force = act(m, totals)
            deposit(m, low_plane, force, high, low, table_y)
            held[1 - slot] = following

        @pl.when(spans > 1)
        def _wide():
            m = held[slot]
            high, low, table_y = prepare(m)
            tz[0] = high
            tz[1] = low

            def sample_span(j, totals):
                plane = low_plane + j * WINDOW
                return sample(held[slot], plane, tz[0], tz[1], table_y, totals)

            force = act(m, lax.fori_loop(0, spans, sample_span, nothing))

            def deposit_span(j, _):
                plane = low_plane + j * WINDOW
                deposit(held[slot], plane, force, tz[0], tz[1], table_y)
                return 0

            lax.fori_loop(0, spans, deposit_span, 0)
            held[1 - slot] = gather(n + 1)

        return 0

    lax.fori_loop(0, tiles, work, 0)


def wall_masks(gy, n_gy, span_y, extent_z):
    y = lax.broadcasted_iota(I32, (ROWS, extent_z), 0)
    low_edge = jnp.where(gy > 0, 0, HALO)
    high_edge = jnp.where(gy < n_gy - 1, ROWS, HALO + span_y)
    inside = jnp.where((y >= low_edge) & (y < high_edge), 1.0, 0.0).astype(F32)
    inside = jnp.concatenate([inside] * 3, axis=0)
    return inside, inside * (1.0 / (1.0 + 6.0 * DIFFUSION))


def relaxed(rhs, before, centre, after, scale):
    shape = rhs.shape
    flat = scale.shape
    centre = centre.reshape(flat)
    total = rhs.reshape(flat) + before.reshape(flat) + after.reshape(flat)
    total = total + pltpu.roll(centre, 1, 0) + pltpu.roll(centre, flat[0] - 1, 0)
    total = total + pltpu.roll(centre, 1, 1) + pltpu.roll(centre, flat[1] - 1, 1)
    return (total * scale).reshape(shape)


def strip_kernel(
    n_gx,
    n_gy,
    per_sphere,
    rhs,
    acted,
    mot_ref,
    cs_ref,
    cp_ref,
    nm_ref,
    ybuf,
    xbuf,
    mid_0,
    mid_1,
    mid_2,
    mid_3,
    done,
    sums,
    ret,
    agx,
    agy,
    ag1,
    moved_s,
    staged,
    ret_send,
    ret_recv,
    agx_send,
    agx_recv,
    agy_send,
    agy_recv,
    y_send,
    y_recv,
    x_send,
    x_recv,
):
    gx, gy, at = neighbours(n_gx, n_gy)
    here = gx * n_gy + gy
    planes = ybuf.shape[1]
    span_y = done.shape[2]
    peers = (
        [at(k, 0) for k in range(1, n_gx)]
        + [at(0, k) for k in range(1, n_gy)]
        + [at(dx, dy) for dx in (-1, 1) for dy in (-1, 1)]
    )
    barrier = greet(peers)
    inner_low = jnp.where(gy > 0, 1.0, 0.0).astype(F32)
    inner_high = jnp.where(gy < n_gy - 1, 1.0, 0.0).astype(F32)
    for n in range(8):
        sums[n] = pltpu.roll(acted[...], 128 - 2 * (n + 1), 1)
    replies = [
        remote(sums.at[n], ret.at[n], ret_send.at[n], ret_recv.at[n], at(-dx, -dy))
        for n, (dx, dy) in enumerate(LANES)
    ]
    lanes = lax.broadcasted_iota(I32, (8, 128), 1)
    row_id = lax.broadcasted_iota(I32, (8, 128), 0)
    pl.semaphore_wait(barrier, len(peers))

    def along_x(k):
        return remote(ag1.at[0], agx.at[k], agx_send.at[k], agx_recv.at[k], at(k, 0))

    def along_y(k):
        return remote(ag1.at[1], agy.at[k], agy_send.at[k], agy_recv.at[k], at(0, k))

    def sphere_step_one():
        for copy in replies:
            copy.wait()
        total = acted[...]
        for n in range(8):
            total = total + ret[n]
        start = jnp.zeros((8, 128), F32)
        for c in range(6):
            for s in range(2):
                start = jnp.where((row_id == c) & (lanes == s), mot_ref[s, c], start)
        moved = start - total * (RESPONSE / per_sphere)
        moved_s[...] = moved
        first = jnp.broadcast_to(moved[:, 0:1], (8, 128))
        other = pltpu.roll(jnp.broadcast_to(moved[:, 1:2], (8, 128)), 3, 0)
        ag1[0] = jnp.where(lanes == here, jnp.where(row_id < 3, first, other), 0.0)
        for k in range(1, n_gx):
            along_x(k).start()

    def sphere_step_two():
        for k in range(1, n_gx):
            along_x(k).wait()
        total = ag1[0]
        for k in range(1, n_gx):
            total = total + agx[k]
        ag1[1] = total
        for k in range(1, n_gy):
            along_y(k).start()

    def sphere_step_three():
        for k in range(1, n_gy):
            along_y(k).wait()
        total = ag1[1]
        for k in range(1, n_gy):
            total = total + agy[k]
        moved = moved_s[...]
        pull = jnp.zeros((8, 128), F32)
        for k in range(cs_ref.shape[0]):
            partner = cp_ref[k]
            own = cs_ref[k] - 2 * here
            chosen = jnp.sum(
                jnp.where(lanes == lax.shift_right_logical(partner, 1), total, 0.0),
                axis=1,
                keepdims=True,
            )
            chosen = jnp.broadcast_to(chosen, (8, 128))
            odd = jnp.broadcast_to(partner & 1, (8, 128)) == 1
            chosen = jnp.where(odd, pltpu.roll(chosen, 5, 0), chosen)
            pull = pull + jnp.where((lanes == own) & (row_id < 3), chosen - moved, 0.0)
        settled = jnp.concatenate(
            [moved + DASHPOT * pull, jnp.zeros((120, 128), F32)], axis=0
        )
        nm_ref[...] = settled.T[0:2, 0:6]

    def y_copies(g):
        copies = []
        for r, (first, count) in enumerate(RUNS[g]):
            lo = first + 2
            base = 4 * g + 2 * r
            copies.append(
                remote(
                    rhs.at[pl.ds(lo, count), :, pl.ds(0, 8)],
                    ybuf.at[1, pl.ds(first, count)],
                    y_send.at[base],
                    y_recv.at[base],
                    at(0, -1),
                )
            )
            copies.append(
                remote(
                    rhs.at[pl.ds(lo, count), :, pl.ds(ROWS - 8, 8)],
                    ybuf.at[0, pl.ds(first, count)],
                    y_send.at[base + 1],
                    y_recv.at[base + 1],
                    at(0, 1),
                )
            )
        return copies

    def x_copies(g):
        (low, count), (high, _) = RUNS[g]
        high = high - (planes - 6)
        return [
            remote(
                staged.at[1, pl.ds(low, count)],
                xbuf.at[1, pl.ds(low, count)],
                x_send.at[2 * g],
                x_recv.at[2 * g],
                at(-1, 0),
            ),
            remote(
                staged.at[0, pl.ds(high, count)],
                xbuf.at[0, pl.ds(high, count)],
                x_send.at[2 * g + 1],
                x_recv.at[2 * g + 1],
                at(1, 0),
            ),
        ]

    def with_strips(p):
        whole = rhs[p + 2]
        low = whole[:, 0:8] + ybuf[0, p] * inner_low
        high = whole[:, ROWS - 8 : ROWS] + ybuf[1, p] * inner_high
        return jnp.concatenate([low, whole[:, 8 : ROWS - 8], high], axis=1)

    def stage(g):
        for side, base in ((1, 0), (0, planes - 6)):
            first, count = RUNS[g][1 - side]
            for p in range(first, first + count):
                staged[side, p - base] = with_strips(p)

    for g in range(2):
        for copy in y_copies(g):
            copy.start()
    for copy in replies:
        copy.start()
    for g in range(2, 4):
        for copy in y_copies(g):
            copy.start()
    for g in range(2):
        for copy in y_copies(g):
            copy.wait()
        stage(g)
        for copy in x_copies(g):
            copy.start()
    sphere_step_one()
    for copy in y_copies(2):
        copy.wait()
    stage(2)
    for copy in x_copies(2):
        copy.start()
    for copy in y_copies(3):
        copy.wait()
    inside, scale = wall_masks(gy, n_gy, span_y, rhs.shape[3])
    span_mid = mid_0.shape[0]

    def begin(i, _):
        mid_0[i] = (with_strips(i + 4).reshape(inside.shape) * inside).reshape(mid_0.shape[1:])
        return 0

    lax.fori_loop(0, span_mid, begin, 0)
    sphere_step_two()
    stages = (mid_0, mid_1, mid_2, mid_3)
    for k in range(1, ITERS):
        source, target = stages[k - 1], stages[k]

        def step(s, _, source=source, target=target, k=k):
            for u in range(2):
                i = 2 * s + u
                target[i] = relaxed(
                    mid_0[i + k], source[i], source[i + 1], source[i + 2], scale
                )
            return 0

        lax.fori_loop(0, (span_mid - 2 * k) // 2, step, 0)
    for i in range(span_mid - 2 * ITERS):
        result = relaxed(mid_0[i + ITERS], mid_3[i], mid_3[i + 1], mid_3[i + 2], scale)
        for c in range(3):
            done[c, i] = result[c, HALO : HALO + span_y, :]
    sphere_step_three()
    for g in range(3):
        for copy in x_copies(g):
            copy.wait()


def relax_kernel(
    n_gy,
    rhs_in,
    ybuf,
    xbuf,
    mid_0,
    mid_1,
    mid_2,
    mid_3,
    done,
    nm_in,
    out_ref,
    nm_ref,
    rhs,
    one,
    two,
    three,
    staged,
    ring,
    sems,
    done_sem,
    nm_sem,
):
    gy = lax.axis_index("gy")
    planes = ybuf.shape[1]
    span_x = planes - 4
    span_y = out_ref.shape[2]
    whole_span = planes + 4
    middle = pltpu.make_async_copy(done, out_ref.at[:, 6 : span_x - 6], done_sem)
    middle.start()
    motion = pltpu.make_async_copy(nm_in, nm_ref, nm_sem)
    motion.start()
    inside, scale = wall_masks(gy, n_gy, span_y, rhs.shape[3])
    inner_low = jnp.where(gy > 0, 1.0, 0.0).astype(F32)
    inner_high = jnp.where(gy < n_gy - 1, 1.0, 0.0).astype(F32)
    for i in range(6):
        for x, beside in ((i, xbuf[0, i]), (planes - 2 + i, xbuf[1, i])):
            whole = rhs_in[x] + beside
            if 2 <= x < planes + 2:
                low = whole[:, 0:8] + ybuf[0, x - 2] * inner_low
                high = whole[:, ROWS - 8 : ROWS] + ybuf[1, x - 2] * inner_high
                whole = jnp.concatenate([low, whole[:, 8 : ROWS - 8], high], axis=1)
            rhs[x] = (whole.reshape(inside.shape) * inside).reshape(whole.shape)
    stages = (rhs, one, two, three)
    for k, (mid, count) in enumerate(((mid_0, 4), (mid_1, 2), (mid_2, 2), (mid_3, 2))):
        for i in range(count):
            stages[k][6 + k + i] = mid[i]
            stages[k][whole_span - 7 - k - i] = mid[mid.shape[0] - 1 - i]

    extent_z = rhs.shape[3]
    apart = lax.broadcasted_iota(I32, (2 * extent_z, extent_z), 0) - lax.broadcasted_iota(
        I32, (2 * extent_z, extent_z), 1
    )
    apart = apart & (extent_z - 1)
    ring[...] = jnp.where((apart == 1) | (apart == extent_z - 1), 1.0, 0.0).astype(BF16)

    def swept(k, places):
        source = stages[k - 1]
        flat = scale.shape
        high, low = split(jnp.concatenate([source[x].reshape(flat) for x in places], axis=0))
        along_z = jnp.dot(
            jnp.concatenate([high, low], axis=1), ring[...], preferred_element_type=F32
        )
        results = []
        for i, x in enumerate(places):
            centre = source[x].reshape(flat)
            total = rhs[x].reshape(flat) + source[x - 1].reshape(flat)
            total = total + source[x + 1].reshape(flat)
            total = total + pltpu.roll(centre, 1, 0) + pltpu.roll(centre, flat[0] - 1, 0)
            total = total + along_z[i * flat[0] : (i + 1) * flat[0]]
            results.append((total * scale).reshape(rhs.shape[1:]))
        return results

    for k in range(1, ITERS):

        def step(s, _, k=k):
            places = [
                first + 2 * s + u for first in (k, whole_span - 6 - k) for u in range(2)
            ]
            for x, result in zip(places, swept(k, places)):
                stages[k][x] = result
            return 0

        lax.fori_loop(0, 3, step, 0)

    def stores(s):
        return [
            pltpu.make_async_copy(
                staged.at[:, pl.ds(first + 2 * s, 2)],
                out_ref.at[:, pl.ds(first + 2 * s, 2)],
                sems.at[2 * s + side],
            )
            for side, first in enumerate((0, span_x - 6))
        ]

    def final(s, _):
        places = [first + 2 * s + u for first in (0, span_x - 6) for u in range(2)]
        for x, result in zip(places, swept(ITERS, [x + HALO for x in places])):
            for c in range(3):
                staged[c, x] = result[c, HALO : HALO + span_y, :]
        for copy in stores(s):
            copy.start()
        return 0

    lax.fori_loop(0, 3, final, 0)
    for s in range(3):
        for copy in stores(s):
            copy.wait()
    middle.wait()
    motion.wait()


def on_device(
    n_gx,
    n_gy,
    velocity,
    owner_block,
    base_x,
    base_y,
    base_z,
    delta_weights,
    marker_offset,
    sphere_motion,
    contact_sphere,
    contact_partner,
):
    span_x, span_y, extent_z = velocity.shape[1:]
    markers = base_x.shape[0]
    planes = span_x + 4
    every = markers // TILE + 8
    padded = planes + WINDOW - 1
    grown = (padded + 2, 3, ROWS, extent_z)
    vmem = pl.BlockSpec(memory_space=pltpu.VMEM)
    smem = pl.BlockSpec(memory_space=pltpu.SMEM)
    hbm = pl.BlockSpec(memory_space=pltpu.HBM)
    dma = pltpu.SemaphoreType.DMA
    motion = sphere_motion.T
    fhl, started, home, arrived = pl.pallas_call(
        functools.partial(request_kernel, n_gx, n_gy),
        out_shape=(
            jax.ShapeDtypeStruct((padded, 3 * ROWS, 2 * extent_z), BF16),
            jax.ShapeDtypeStruct(grown, F32),
            jax.ShapeDtypeStruct((32, markers), F32),
            jax.ShapeDtypeStruct((8, 24, TILE), F32),
        ),
        in_specs=[hbm] * 8,
        out_specs=(vmem,) * 4,
        scratch_shapes=[
            pltpu.VMEM(velocity.shape, F32),
            pltpu.VMEM((1, markers), I32),
            pltpu.VMEM((1, markers), I32),
            pltpu.VMEM((1, markers), I32),
            pltpu.VMEM((1, markers), I32),
            pltpu.VMEM((12, markers), F32),
            pltpu.VMEM((3, markers), F32),
            pltpu.SMEM((2, 6), F32),
            pltpu.VMEM((2, 3, 2, span_y, extent_z), F32),
            pltpu.VMEM((2, 3, 2 * span_x, extent_z), F32),
            pltpu.VMEM((4, 16, extent_z), F32),
            pltpu.VMEM((4, 16, extent_z), F32),
            pltpu.VMEM((2, 3, 2 * span_x, extent_z), F32),
            pltpu.VMEM((32, markers), F32),
            pltpu.VMEM((96, markers), BF16),
            pltpu.VMEM((8, TILE), F32),
            pltpu.VMEM((8, 24, TILE), F32),
            pltpu.VMEM((8, 24, TILE), F32),
            pltpu.VMEM((planes, 3, ROWS, extent_z), F32),
            dma((8,)),
            dma((8,)),
            dma((8,)),
            dma((8,)),
            dma((8,)),
        ],
        compiler_params=pltpu.CompilerParams(
            collective_id=0, has_side_effects=True, vmem_limit_bytes=24 << 20
        ),
        name="requests",
    )(
        *(
            pltpu.with_memory_space_constraint(array, pltpu.HBM)
            for array in (
                velocity,
                owner_block.reshape(1, markers),
                base_x.reshape(1, markers),
                base_y.reshape(1, markers),
                base_z.reshape(1, markers),
                delta_weights,
                marker_offset,
                motion,
            )
        )
    )
    rhs, acted = pl.pallas_call(
        marker_kernel,
        out_shape=(
            jax.ShapeDtypeStruct(grown, F32),
            jax.ShapeDtypeStruct((8, 128), F32),
        ),
        in_specs=[vmem] * 4,
        out_specs=(vmem,) * 2,
        scratch_shapes=[
            pltpu.VMEM((every, 96, TILE), BF16),
            pltpu.VMEM((every * BINS, TILE), F32),
            pltpu.VMEM((every * BINS, TILE), F32),
            pltpu.VMEM((every, TILE), F32),
            pltpu.VMEM((2, extent_z, TILE), BF16),
            pltpu.VMEM((2, 32, TILE), F32),
            pltpu.VMEM((8, 128), I32),
            pltpu.SMEM((8, 128), I32),
            dma,
        ],
        compiler_params=pltpu.CompilerParams(vmem_limit_bytes=24 << 20),
        name="markers",
    )(fhl, started, home, arrived)
    plane = (3, ROWS, extent_z)
    middle = planes - 8
    new_motion, *strips = pl.pallas_call(
        functools.partial(strip_kernel, n_gx, n_gy, markers // 2),
        out_shape=(
            jax.ShapeDtypeStruct(motion.shape, F32),
            jax.ShapeDtypeStruct((2, planes, 3, 8, extent_z), F32),
            jax.ShapeDtypeStruct((2, 6, 3, ROWS, extent_z), F32),
            jax.ShapeDtypeStruct((middle,) + plane, F32),
            jax.ShapeDtypeStruct((middle - 2,) + plane, F32),
            jax.ShapeDtypeStruct((middle - 4,) + plane, F32),
            jax.ShapeDtypeStruct((middle - 6,) + plane, F32),
            jax.ShapeDtypeStruct((3, middle - 8, span_y, extent_z), F32),
        ),
        in_specs=[vmem] * 2 + [smem] * 3,
        out_specs=(vmem,) * 8,
        scratch_shapes=[
            pltpu.VMEM((8, 8, 128), F32),
            pltpu.VMEM((8, 8, 128), F32),
            pltpu.VMEM((n_gx, 8, 128), F32),
            pltpu.VMEM((n_gy, 8, 128), F32),
            pltpu.VMEM((2, 8, 128), F32),
            pltpu.VMEM((8, 128), F32),
            pltpu.VMEM((2, 6, 3, ROWS, extent_z), F32),
            dma((8,)),
            dma((8,)),
            dma((n_gx,)),
            dma((n_gx,)),
            dma((n_gy,)),
            dma((n_gy,)),
            dma((16,)),
            dma((16,)),
            dma((6,)),
            dma((6,)),
        ],
        compiler_params=pltpu.CompilerParams(
            collective_id=1, has_side_effects=True, vmem_limit_bytes=24 << 20
        ),
        name="strips",
    )(rhs, acted, motion, contact_sphere, contact_partner)
    velocity_star, new_motion = pl.pallas_call(
        functools.partial(relax_kernel, n_gy),
        out_shape=(
            jax.ShapeDtypeStruct(velocity.shape, F32),
            jax.ShapeDtypeStruct(motion.shape, F32),
        ),
        in_specs=[vmem] * 9,
        out_specs=(hbm, hbm),
        scratch_shapes=[pltpu.VMEM((planes + 4,) + plane, F32)] * 4
        + [
            pltpu.VMEM(velocity.shape, F32),
            pltpu.VMEM((2 * extent_z, extent_z), BF16),
            dma((6,)),
            dma,
            dma,
        ],
        compiler_params=pltpu.CompilerParams(vmem_limit_bytes=24 << 20),
        name="relax",
    )(rhs, *strips, new_motion)
    return velocity_star, new_motion.T


def solution(mesh):
    placed = (
        P(None, "gx", "gy", None),
        P(("gx", "gy"), None),
        P(("gx", "gy")),
        P(("gx", "gy")),
        P(("gx", "gy")),
        P(None, ("gx", "gy")),
        P(None, ("gx", "gy")),
        P(None, ("gx", "gy")),
        P(("gx", "gy")),
        P(("gx", "gy")),
    )
    return jax.shard_map(
        functools.partial(on_device, mesh.shape["gx"], mesh.shape["gy"]),
        mesh=mesh,
        in_specs=placed,
        out_specs=(P(None, "gx", "gy", None), P(None, ("gx", "gy"))),
        check_vma=False,
    )
```

```python
import functools

import jax
import jax.numpy as jnp
from jax import lax
from jax.experimental import pallas as pl
from jax.experimental.pallas import tpu as pltpu
from jax.sharding import PartitionSpec as P

F32 = jnp.float32
BF16 = jnp.bfloat16
I32 = jnp.int32
MESH = pl.DeviceIdType.MESH

ITERS = 4
DIFFUSION = 1.0
RESPONSE = 0.5
DASHPOT = 0.1

TILE = 256
BINS = 32
WINDOW = 6
ROWS = 40
HALO = 4
LANES = [(dx, dy) for dx in (-1, 0, 1) for dy in (-1, 0, 1) if (dx, dy) != (0, 0)]
DIAGONALS = [(dx, dy) for dx, dy in LANES if dx * dy != 0]
RUNS = [((0, 1), (19, 1)), ((1, 2), (17, 2)), ((3, 3), (14, 3)), ((6, 8),)]


def split(values):
    high = values.astype(BF16)
    low = (values - high.astype(F32)).astype(BF16)
    return high, low


def pick(distance, weights):
    result = jnp.where(distance == 3, weights[3], 0.0)
    for k in (2, 1, 0):
        result = jnp.where(distance == k, weights[k], result)
    return result


def cross(a, b):
    return (
        a[1] * b[2] - a[2] * b[1],
        a[2] * b[0] - a[0] * b[2],
        a[0] * b[1] - a[1] * b[0],
    )


def remote(src, dst, send, recv, peer):
    return pltpu.make_async_remote_copy(
        src_ref=src,
        dst_ref=dst,
        send_sem=send,
        recv_sem=recv,
        device_id=peer,
        device_id_type=MESH,
    )


def greet(peers):
    barrier = pltpu.get_barrier_semaphore()
    for peer in peers:
        pl.semaphore_signal(barrier, inc=1, device_id=peer, device_id_type=MESH)
    return barrier


def neighbours(n_gx, n_gy):
    gx = lax.axis_index("gx")
    gy = lax.axis_index("gy")

    def at(dx, dy):
        return (lax.rem(gx + (dx + n_gx), n_gx), lax.rem(gy + (dy + n_gy), n_gy))

    return gx, gy, at


def terms(values):
    parts = []
    rest = values
    for _ in range(3):
        part = rest.astype(BF16)
        parts.append(part)
        rest = rest - part.astype(F32)
    return jnp.concatenate(parts, axis=0)


def chosen_columns(parts, slots, first):
    wanted = lax.broadcasted_iota(I32, (TILE, TILE), 0).astype(F32) + first
    hit = jnp.where(wanted == slots, 1.0, 0.0).astype(BF16)
    return lax.dot_general(parts, hit, (((1,), (1,)), ((), ())), preferred_element_type=F32)


def ranks(hits, above):
    return jnp.dot(hits.astype(BF16), above, preferred_element_type=F32)


def strictly_above(size):
    return (
        lax.broadcasted_iota(I32, (size, size), 0) < lax.broadcasted_iota(I32, (size, size), 1)
    ).astype(BF16)


def request_kernel(
    n_gx,
    n_gy,
    v_hbm,
    own_hbm,
    bx_hbm,
    by_hbm,
    bz_hbm,
    dw_hbm,
    off_hbm,
    mot_hbm,
    fhl,
    rhs,
    home,
    arrived,
    v_ref,
    own_ref,
    bx_ref,
    by_ref,
    bz_ref,
    dw_ref,
    off_ref,
    mot_ref,
    hx,
    hy,
    hc,
    corner,
    edges,
    pay,
    pay3,
    slot_s,
    snd,
    inbox,
    frame,
    in_sem,
    halo_send,
    halo_recv,
    pay_send,
    pay_recv,
):
    gx, gy, at = neighbours(n_gx, n_gy)
    here = gx * n_gy + gy
    barrier = greet([at(dx, dy) for dx, dy in LANES])
    loads = [
        pltpu.make_async_copy(src, dst, in_sem.at[i])
        for i, (src, dst) in enumerate(
            (
                (v_hbm, v_ref),
                (own_hbm, own_ref),
                (bx_hbm, bx_ref),
                (by_hbm, by_ref),
                (bz_hbm, bz_ref),
                (dw_hbm, dw_ref),
                (off_hbm, off_ref),
                (mot_hbm, mot_ref),
            )
        )
    ]
    for copy in loads:
        copy.start()
    markers = dw_ref.shape[1]
    chunks = markers // TILE
    span_x = v_ref.shape[1]
    span_y = v_ref.shape[2]
    extent_z = v_ref.shape[3]
    planes = span_x + 4
    for copy in loads:
        copy.wait()

    last = span_x - 2
    pl.semaphore_wait(barrier, len(LANES))
    halo = []
    halo.append(remote(v_ref.at[:, 0:2], hx.at[1], halo_send.at[0], halo_recv.at[0], at(-1, 0)))
    halo.append(
        remote(v_ref.at[:, last:span_x], hx.at[0], halo_send.at[1], halo_recv.at[1], at(1, 0))
    )
    halo.append(remote(edges.at[0], hy.at[1], halo_send.at[2], halo_recv.at[2], at(0, -1)))
    halo.append(remote(edges.at[1], hy.at[0], halo_send.at[3], halo_recv.at[3], at(0, 1)))
    for k, (dx, dy) in enumerate(DIAGONALS):
        slot = (1 if dx < 0 else 0) * 2 + (1 if dy < 0 else 0)
        halo.append(
            remote(
                corner.at[k], hc.at[slot], halo_send.at[4 + k], halo_recv.at[4 + k], at(dx, dy)
            )
        )
    corner[...] = jnp.zeros_like(corner)
    for k, (dx, dy) in enumerate(DIAGONALS):
        x0 = 0 if dx < 0 else last
        y0 = 0 if dy < 0 else span_y - 2
        for c in range(3):
            for i in range(2):
                row = 4 * c + 2 * i
                corner[k, row : row + 2, :] = v_ref[c, x0 + i, y0 : y0 + 2, :]
    for copy in halo[4:] + halo[0:2]:
        copy.start()
    for side, y0 in enumerate((0, span_y - 2)):
        for c in range(3):
            for x in range(span_x):
                edges[side, c, 2 * x : 2 * x + 2, :] = v_ref[c, x, y0 : y0 + 2, :]
    for copy in halo[2:4]:
        copy.start()

    pay[0:12, :] = dw_ref[...]
    pay[12:13, :] = bx_ref[...].astype(F32)
    pay[13:14, :] = by_ref[...].astype(F32)
    pay[14:15, :] = bz_ref[...].astype(F32)
    per_sphere = markers // 2
    second = (lax.broadcasted_iota(I32, (1, markers), 1) >= per_sphere).astype(F32)
    pay[15:16, :] = second
    motion = [mot_ref[0, c] * (1.0 - second) + mot_ref[1, c] * second for c in range(6)]
    offset = [off_ref[c : c + 1, :] for c in range(3)]
    swing = cross(motion[3:6], offset)
    for c in range(3):
        pay[16 + c : 17 + c, :] = motion[c] + swing[c]
        pay[19 + c : 20 + c, :] = offset[c]
    pay[22:23, :] = jnp.ones((1, markers), F32)
    pay[23:32, :] = jnp.zeros((9, markers), F32)
    whole = pay[...]
    pay3[...] = terms(whole)
    home[...] = whole
    home[22:23, :] = (own_ref[...] == here).astype(F32)

    above = strictly_above(TILE)
    bins = lax.broadcasted_iota(I32, (8, TILE), 0)
    carry = jnp.zeros((8, 1), F32)
    for q in range(chunks):
        owner = own_ref[:, q * TILE : (q + 1) * TILE]
        owner_x = lax.shift_right_logical(owner, n_gy.bit_length() - 1)
        owner_y = owner & (n_gy - 1)
        step_x = (owner_x - gx + 1) & (n_gx - 1)
        lane = step_x * 3 + (owner_y - gy + 1)
        lane = jnp.where(owner == here, -1, jnp.where(lane > 4, lane - 1, lane))
        hits = jnp.where(bins == lane, 1.0, 0.0)
        ranked = ranks(hits, above) + carry + bins.astype(F32) * TILE
        carry = carry + jnp.sum(hits, axis=1, keepdims=True)
        slot = jnp.sum(hits * ranked, axis=0, keepdims=True)
        slot_s[q : q + 1, :] = jnp.where(lane < 0, -1.0, slot)

    def compact(n, _):
        first = (n * TILE).astype(F32)
        moved = None
        for q in range(chunks):
            part = chosen_columns(
                pay3[:, q * TILE : (q + 1) * TILE], slot_s[q : q + 1, :], first
            )
            moved = part if moved is None else moved + part
        snd[n] = moved[0:24] + moved[32:56] + moved[64:88]
        return 0

    lax.fori_loop(0, 8, compact, 0)

    requests = [
        remote(snd.at[n], inbox.at[n], pay_send.at[n], pay_recv.at[n], at(dx, dy))
        for n, (dx, dy) in enumerate(LANES)
    ]
    for copy in requests:
        copy.start()

    inner_low = jnp.where(gy > 0, 1.0, 0.0).astype(F32)
    inner_high = jnp.where(gy < n_gy - 1, 1.0, 0.0).astype(F32)

    def clear(p, _):
        rhs[p] = jnp.zeros((3, ROWS, extent_z), F32)
        return 0

    lax.fori_loop(0, rhs.shape[0], clear, 0)

    def clear_frame(p, _):
        frame[p] = jnp.zeros((3, ROWS, extent_z), F32)
        return 0

    lax.fori_loop(0, planes, clear_frame, 0)

    def clear_beyond(p, _):
        fhl[p] = jnp.zeros((3 * ROWS, 2 * extent_z), BF16)
        return 0

    lax.fori_loop(planes, fhl.shape[0], clear_beyond, 0)

    def place(x, _):
        for c in range(3):
            plane = v_ref[c, x]
            frame[x + 2, c, 4 : 4 + span_y, :] = plane
            rhs[x + 4, c, 4 : 4 + span_y, :] = plane
        return 0

    lax.fori_loop(0, span_x, place, 0)
    for copy in halo:
        copy.wait()

    for x in range(span_x):
        for c in range(3):
            frame[x + 2, c, 2:4, :] = hy[0, c, 2 * x : 2 * x + 2, :] * inner_low
            frame[x + 2, c, 36:38, :] = hy[1, c, 2 * x : 2 * x + 2, :] * inner_high
    for side in range(2):
        for i in range(2):
            p = (0 if side == 0 else planes - 2) + i
            for c in range(3):
                frame[p, c, 4 : 4 + span_y, :] = hx[side, c, i]
                frame[p, c, 2:4, :] = hc[side * 2, 4 * c + 2 * i : 4 * c + 2 * i + 2, :] * inner_low
                frame[p, c, 36:38, :] = (
                    hc[side * 2 + 1, 4 * c + 2 * i : 4 * c + 2 * i + 2, :] * inner_high
                )

    def halve(p, _):
        high, low = split(frame[p].reshape(3 * ROWS, extent_z))
        fhl[p, :, 0:extent_z] = high
        fhl[p, :, extent_z : 2 * extent_z] = low
        return 0

    lax.fori_loop(0, planes, halve, 0)
    for copy in requests:
        copy.wait()
    arrived[...] = inbox[...]


def marker_kernel(
    fhl,
    rhs_in,
    home,
    arrived,
    rhs,
    acted,
    pay3,
    hit_s,
    rank_s,
    slot_s,
    tz,
    held,
    edge_v,
    edge,
    edge_sem,
):
    chunks = home.shape[1] // TILE
    every = chunks + 8
    extent_z = rhs.shape[3]
    bins = lax.broadcasted_iota(I32, (BINS, TILE), 0).astype(F32)

    def chunk(q):
        return home[0:24, q * TILE : (q + 1) * TILE] if q < chunks else arrived[q - chunks]

    totals = []
    for q in range(every):
        m = chunk(q)
        hits = jnp.where((bins == m[12:13]) & (m[22:23] > 0.5), 1.0, 0.0)
        hit_s[q * BINS : (q + 1) * BINS, :] = hits
        totals.append(jnp.sum(hits, axis=1, keepdims=True))
    rank_s[...] = ranks(hit_s[...], strictly_above(TILE))
    carries = []
    count = jnp.zeros((BINS, 1), F32)
    for q in range(every):
        carries.append(count)
        count = count + totals[q]
    count = jnp.broadcast_to(count, (BINS, 128))
    high, low = split(count)
    below = (
        lax.broadcasted_iota(I32, (BINS, BINS), 0) > lax.broadcasted_iota(I32, (BINS, BINS), 1)
    ).astype(BF16)
    start = jnp.dot(below, high, preferred_element_type=F32)
    start = start + jnp.dot(below, low, preferred_element_type=F32)
    opening = lax.broadcasted_iota(I32, (BINS, 128), 1).astype(F32) * TILE
    present = jnp.sum(count, axis=0, keepdims=True)
    closing = jnp.minimum(opening + TILE, present)
    first_bin = jnp.sum(jnp.where(start + count <= opening, 1.0, 0.0), axis=0, keepdims=True)
    last_bin = jnp.sum(jnp.where(start < closing, 1.0, 0.0), axis=0, keepdims=True) - 1.0
    edge_v[...] = jnp.concatenate(
        [first_bin, last_bin, present, jnp.zeros((5, 128), F32)], axis=0
    ).astype(I32)
    to_scalars = pltpu.make_async_copy(edge_v, edge, edge_sem)
    to_scalars.start()
    start = start[:, 0:1]
    for q in range(every):
        hits = hit_s[q * BINS : (q + 1) * BINS, :]
        ranked = rank_s[q * BINS : (q + 1) * BINS, :] + (carries[q] + start)
        slot = jnp.sum(hits * ranked, axis=0, keepdims=True)
        there = jnp.sum(hits, axis=0, keepdims=True)
        slot_s[q : q + 1, :] = jnp.where(there > 0.5, slot, -1.0)
        m = chunk(q)
        if q < chunks:
            source = jnp.zeros((1, TILE), F32)
        else:
            source = jnp.full((1, TILE), float(q - chunks + 1), F32)
        filled = jnp.concatenate([m[0:23], source, jnp.zeros((8, TILE), F32)], axis=0)
        pay3[q] = terms(filled)
    acted[...] = jnp.zeros_like(acted)

    def start_from(p, _):
        rhs[p] = rhs_in[p]
        return 0

    lax.fori_loop(0, rhs.shape[0], start_from, 0)
    slot_id = lax.broadcasted_iota(I32, (TILE, TILE), 0).astype(F32)

    def gather(n):
        wanted = slot_id + (n * TILE).astype(F32)
        moved = None
        for q in range(every):
            hit = jnp.where(wanted == slot_s[q : q + 1, :], 1.0, 0.0).astype(BF16)
            part = lax.dot_general(
                hit, pay3[q], (((1,), (1,)), ((), ())), preferred_element_type=F32
            )
            moved = part if moved is None else moved + part
        moved = jnp.concatenate([moved, jnp.zeros((TILE, 32), F32)], axis=1).T
        return moved[0:32] + moved[32:64] + moved[64:96]

    def prepare(m):
        cell_y = m[13:14].astype(I32)
        cell_z = m[14:15].astype(I32)
        z = lax.broadcasted_iota(I32, (extent_z, TILE), 0)
        table = pick((z - cell_z) & (extent_z - 1), [m[8 + i : 9 + i] for i in range(4)])
        high, low = split(table)
        y = lax.broadcasted_iota(I32, (ROWS, TILE), 0) - 2
        table_y = pick(y - cell_y, [m[4 + i : 5 + i] for i in range(4)])
        return high, low, table_y

    def x_table(m, plane):
        x = lax.broadcasted_iota(I32, (8, TILE), 0)
        return pick(x + plane - m[12:13].astype(I32), [m[i : i + 1] for i in range(4)])

    def sample(m, plane, high, low, table_y, totals):
        table_x = x_table(m, plane)
        folded_y = table_y.reshape(ROWS // 8, 8, TILE)
        both = fhl[pl.ds(plane, WINDOW)].reshape(WINDOW * 3 * ROWS, 2 * extent_z)
        left = jnp.concatenate([both, both[:, 0:extent_z]], axis=1)
        right = jnp.concatenate([high, high, low], axis=0)
        part = jnp.dot(left, right, preferred_element_type=F32)
        part = part.reshape(WINDOW, 3, ROWS // 8, 8, TILE)
        result = []
        for c in range(3):
            total = totals[c]
            for p in range(WINDOW):
                total = total + jnp.sum(part[p, c] * folded_y, axis=0) * table_x[p : p + 1]
            result.append(total)
        return tuple(result)

    def act(m, totals):
        totals = [jnp.sum(total, axis=0, keepdims=True) for total in totals]
        force = [m[16 + c : 17 + c] - totals[c] for c in range(3)]
        torque = cross([m[19 + c : 20 + c] for c in range(3)], force)
        acting = jnp.concatenate(force + list(torque) + [jnp.zeros((2, TILE), F32)], axis=0)
        group = m[23:24] * 2.0 + m[15:16]
        member = (
            (lax.broadcasted_iota(I32, (128, TILE), 0).astype(F32) == group)
            & (m[22:23] > 0.5)
        ).astype(F32)
        summed = lax.dot_general(
            terms(acting),
            member.astype(BF16),
            (((1,), (1,)), ((), ())),
            preferred_element_type=F32,
        )
        acted[...] += summed[0:8] + summed[8:16] + summed[16:24]
        return force

    def deposit(m, plane, force, z_high, z_low, table_y):
        table_x = x_table(m, plane)
        rows = []
        for p in range(WINDOW):
            for c in range(3):
                rows.append((force[c] * table_x[p : p + 1]) * table_y)
        high, low = split(jnp.concatenate(rows, axis=0))
        left = jnp.concatenate([high, low, high], axis=1)
        right = jnp.concatenate([z_high, z_high, z_low], axis=1)
        added = lax.dot_general(
            left, right, (((1,), (1,)), ((), ())), preferred_element_type=F32
        )
        rhs[pl.ds(plane + 2, WINDOW)] += added.reshape(WINDOW, 3, ROWS, extent_z)

    held[0] = gather(jnp.int32(0))
    to_scalars.wait()
    tiles = lax.shift_right_logical(edge[2, 0] + (TILE - 1), TILE.bit_length() - 1)
    nothing = (jnp.zeros((8, TILE), F32),) * 3

    def work(n, _):
        low_plane = edge[0, n]
        spans = (edge[1, n] + 3 - low_plane + WINDOW) // WINDOW
        slot = n & 1

        @pl.when(spans <= 1)
        def _narrow():
            m = held[slot]
            high, low, table_y = prepare(m)
            totals = sample(m, low_plane, high, low, table_y, nothing)
            following = gather(n + 1)
            force = act(m, totals)
            deposit(m, low_plane, force, high, low, table_y)
            held[1 - slot] = following

        @pl.when(spans > 1)
        def _wide():
            m = held[slot]
            high, low, table_y = prepare(m)
            tz[0] = high
            tz[1] = low

            def sample_span(j, totals):
                plane = low_plane + j * WINDOW
                return sample(held[slot], plane, tz[0], tz[1], table_y, totals)

            force = act(m, lax.fori_loop(0, spans, sample_span, nothing))

            def deposit_span(j, _):
                plane = low_plane + j * WINDOW
                deposit(held[slot], plane, force, tz[0], tz[1], table_y)
                return 0

            lax.fori_loop(0, spans, deposit_span, 0)
            held[1 - slot] = gather(n + 1)

        return 0

    lax.fori_loop(0, tiles, work, 0)


def wall_masks(gy, n_gy, span_y, extent_z):
    y = lax.broadcasted_iota(I32, (ROWS, extent_z), 0)
    low_edge = jnp.where(gy > 0, 0, HALO)
    high_edge = jnp.where(gy < n_gy - 1, ROWS, HALO + span_y)
    inside = jnp.where((y >= low_edge) & (y < high_edge), 1.0, 0.0).astype(F32)
    inside = jnp.concatenate([inside] * 3, axis=0)
    return inside, inside * (1.0 / (1.0 + 6.0 * DIFFUSION))


def relaxed(rhs, before, centre, after, scale):
    shape = rhs.shape
    flat = scale.shape
    centre = centre.reshape(flat)
    total = rhs.reshape(flat) + before.reshape(flat) + after.reshape(flat)
    total = total + pltpu.roll(centre, 1, 0) + pltpu.roll(centre, flat[0] - 1, 0)
    total = total + pltpu.roll(centre, 1, 1) + pltpu.roll(centre, flat[1] - 1, 1)
    return (total * scale).reshape(shape)


def strip_kernel(
    n_gx,
    n_gy,
    per_sphere,
    rhs,
    acted,
    mot_ref,
    cs_ref,
    cp_ref,
    nm_ref,
    ybuf,
    xbuf,
    mid_0,
    mid_1,
    mid_2,
    mid_3,
    done,
    sums,
    ret,
    agx,
    agy,
    ag1,
    moved_s,
    staged,
    ret_send,
    ret_recv,
    agx_send,
    agx_recv,
    agy_send,
    agy_recv,
    y_send,
    y_recv,
    x_send,
    x_recv,
):
    gx, gy, at = neighbours(n_gx, n_gy)
    here = gx * n_gy + gy
    planes = ybuf.shape[1]
    span_y = done.shape[2]
    peers = (
        [at(k, 0) for k in range(1, n_gx)]
        + [at(0, k) for k in range(1, n_gy)]
        + [at(dx, dy) for dx in (-1, 1) for dy in (-1, 1)]
    )
    barrier = greet(peers)
    inner_low = jnp.where(gy > 0, 1.0, 0.0).astype(F32)
    inner_high = jnp.where(gy < n_gy - 1, 1.0, 0.0).astype(F32)
    for n in range(8):
        sums[n] = pltpu.roll(acted[...], 128 - 2 * (n + 1), 1)
    replies = [
        remote(sums.at[n], ret.at[n], ret_send.at[n], ret_recv.at[n], at(-dx, -dy))
        for n, (dx, dy) in enumerate(LANES)
    ]
    lanes = lax.broadcasted_iota(I32, (8, 128), 1)
    row_id = lax.broadcasted_iota(I32, (8, 128), 0)
    pl.semaphore_wait(barrier, len(peers))

    def along_x(k):
        return remote(ag1.at[0], agx.at[k], agx_send.at[k], agx_recv.at[k], at(k, 0))

    def along_y(k):
        return remote(ag1.at[1], agy.at[k], agy_send.at[k], agy_recv.at[k], at(0, k))

    def sphere_step_one():
        for copy in replies:
            copy.wait()
        total = acted[...]
        for n in range(8):
            total = total + ret[n]
        start = jnp.zeros((8, 128), F32)
        for c in range(6):
            for s in range(2):
                start = jnp.where((row_id == c) & (lanes == s), mot_ref[s, c], start)
        moved = start - total * (RESPONSE / per_sphere)
        moved_s[...] = moved
        lane = lanes[0:1]
        message = jnp.zeros((1, 128), F32)
        for sphere in range(2):
            for c in range(3):
                message = jnp.where(
                    lane == 3 * sphere + c, moved[c : c + 1, sphere : sphere + 1], message
                )
        ag1[0] = message
        for k in range(1, n_gx):
            along_x(k).start()

    def sphere_step_two():
        for k in range(1, n_gx):
            along_x(k).wait()
        total = ag1[0]
        for k in range(1, n_gx):
            total = total + pltpu.roll(agx[k], 6 * k, 1)
        ag1[1] = total
        for k in range(1, n_gy):
            along_y(k).start()

    def sphere_step_three():
        for k in range(1, n_gy):
            along_y(k).wait()
        table = jnp.concatenate([ag1[1]] + [agy[k] for k in range(1, n_gy)], axis=0)
        moved = moved_s[...]
        pull = jnp.zeros((8, 128), F32)
        for k in range(cs_ref.shape[0]):
            partner = cp_ref[k]
            own = cs_ref[k] - 2 * here
            holder = lax.shift_right_logical(partner, 1)
            holder_x = lax.shift_right_logical(holder, n_gy.bit_length() - 1)
            row = (gy - (holder & (n_gy - 1)) + n_gy) & (n_gy - 1)
            lane = 6 * ((gx - holder_x + n_gx) & (n_gx - 1)) + 3 * (partner & 1)
            mine = jnp.where(row_id == row, table, 0.0)
            for c in range(3):
                chosen = jnp.sum(
                    jnp.where(lanes == lane + c, mine, 0.0), axis=(0, 1), keepdims=True
                )
                pull = pull + jnp.where((lanes == own) & (row_id == c), chosen - moved, 0.0)
        settled = jnp.concatenate(
            [moved + DASHPOT * pull, jnp.zeros((120, 128), F32)], axis=0
        )
        nm_ref[...] = settled.T[0:2, 0:6]

    def y_copies(g):
        copies = []
        for r, (first, count) in enumerate(RUNS[g]):
            lo = first + 2
            base = 4 * g + 2 * r
            copies.append(
                remote(
                    rhs.at[pl.ds(lo, count), :, pl.ds(0, 8)],
                    ybuf.at[1, pl.ds(first, count)],
                    y_send.at[base],
                    y_recv.at[base],
                    at(0, -1),
                )
            )
            copies.append(
                remote(
                    rhs.at[pl.ds(lo, count), :, pl.ds(ROWS - 8, 8)],
                    ybuf.at[0, pl.ds(first, count)],
                    y_send.at[base + 1],
                    y_recv.at[base + 1],
                    at(0, 1),
                )
            )
        return copies

    def x_copies(g):
        (low, count), (high, _) = RUNS[g]
        high = high - (planes - 6)
        return [
            remote(
                staged.at[1, pl.ds(low, count)],
                xbuf.at[1, pl.ds(low, count)],
                x_send.at[2 * g],
                x_recv.at[2 * g],
                at(-1, 0),
            ),
            remote(
                staged.at[0, pl.ds(high, count)],
                xbuf.at[0, pl.ds(high, count)],
                x_send.at[2 * g + 1],
                x_recv.at[2 * g + 1],
                at(1, 0),
            ),
        ]

    def with_strips(p):
        whole = rhs[p + 2]
        low = whole[:, 0:8] + ybuf[0, p] * inner_low
        high = whole[:, ROWS - 8 : ROWS] + ybuf[1, p] * inner_high
        return jnp.concatenate([low, whole[:, 8 : ROWS - 8], high], axis=1)

    def stage(g):
        for side, base in ((1, 0), (0, planes - 6)):
            first, count = RUNS[g][1 - side]
            for p in range(first, first + count):
                staged[side, p - base] = with_strips(p)

    for g in range(2):
        for copy in y_copies(g):
            copy.start()
    for copy in replies:
        copy.start()
    for g in range(2, 4):
        for copy in y_copies(g):
            copy.start()
    for g in range(2):
        for copy in y_copies(g):
            copy.wait()
        stage(g)
        for copy in x_copies(g):
            copy.start()
    sphere_step_one()
    for copy in y_copies(2):
        copy.wait()
    stage(2)
    for copy in x_copies(2):
        copy.start()
    for copy in y_copies(3):
        copy.wait()
    inside, scale = wall_masks(gy, n_gy, span_y, rhs.shape[3])
    span_mid = mid_0.shape[0]

    def begin(i, _):
        mid_0[i] = (with_strips(i + 4).reshape(inside.shape) * inside).reshape(mid_0.shape[1:])
        return 0

    lax.fori_loop(0, span_mid, begin, 0)
    sphere_step_two()
    stages = (mid_0, mid_1, mid_2, mid_3)
    for k in range(1, ITERS):
        source, target = stages[k - 1], stages[k]

        def step(s, _, source=source, target=target, k=k):
            for u in range(2):
                i = 2 * s + u
                target[i] = relaxed(
                    mid_0[i + k], source[i], source[i + 1], source[i + 2], scale
                )
            return 0

        lax.fori_loop(0, (span_mid - 2 * k) // 2, step, 0)
    for i in range(span_mid - 2 * ITERS):
        result = relaxed(mid_0[i + ITERS], mid_3[i], mid_3[i + 1], mid_3[i + 2], scale)
        for c in range(3):
            done[c, i] = result[c, HALO : HALO + span_y, :]
    sphere_step_three()
    for g in range(3):
        for copy in x_copies(g):
            copy.wait()


def relax_kernel(
    n_gy,
    rhs_in,
    ybuf,
    xbuf,
    mid_0,
    mid_1,
    mid_2,
    mid_3,
    done,
    nm_in,
    out_ref,
    nm_ref,
    rhs,
    one,
    two,
    three,
    staged,
    ring,
    sems,
    done_sem,
    nm_sem,
):
    gy = lax.axis_index("gy")
    planes = ybuf.shape[1]
    span_x = planes - 4
    span_y = out_ref.shape[2]
    whole_span = planes + 4
    middle = pltpu.make_async_copy(done, out_ref.at[:, 6 : span_x - 6], done_sem)
    middle.start()
    motion = pltpu.make_async_copy(nm_in, nm_ref, nm_sem)
    motion.start()
    inside, scale = wall_masks(gy, n_gy, span_y, rhs.shape[3])
    inner_low = jnp.where(gy > 0, 1.0, 0.0).astype(F32)
    inner_high = jnp.where(gy < n_gy - 1, 1.0, 0.0).astype(F32)
    for i in range(6):
        for x, beside in ((i, xbuf[0, i]), (planes - 2 + i, xbuf[1, i])):
            whole = rhs_in[x] + beside
            if 2 <= x < planes + 2:
                low = whole[:, 0:8] + ybuf[0, x - 2] * inner_low
                high = whole[:, ROWS - 8 : ROWS] + ybuf[1, x - 2] * inner_high
                whole = jnp.concatenate([low, whole[:, 8 : ROWS - 8], high], axis=1)
            rhs[x] = (whole.reshape(inside.shape) * inside).reshape(whole.shape)
    stages = (rhs, one, two, three)
    for k, (mid, count) in enumerate(((mid_0, 4), (mid_1, 2), (mid_2, 2), (mid_3, 2))):
        for i in range(count):
            stages[k][6 + k + i] = mid[i]
            stages[k][whole_span - 7 - k - i] = mid[mid.shape[0] - 1 - i]

    extent_z = rhs.shape[3]
    apart = lax.broadcasted_iota(I32, (2 * extent_z, extent_z), 0) - lax.broadcasted_iota(
        I32, (2 * extent_z, extent_z), 1
    )
    apart = apart & (extent_z - 1)
    ring[...] = jnp.where((apart == 1) | (apart == extent_z - 1), 1.0, 0.0).astype(BF16)

    def swept(k, places):
        source = stages[k - 1]
        flat = scale.shape
        high, low = split(jnp.concatenate([source[x].reshape(flat) for x in places], axis=0))
        along_z = jnp.dot(
            jnp.concatenate([high, low], axis=1), ring[...], preferred_element_type=F32
        )
        results = []
        for i, x in enumerate(places):
            centre = source[x].reshape(flat)
            total = rhs[x].reshape(flat) + source[x - 1].reshape(flat)
            total = total + source[x + 1].reshape(flat)
            total = total + pltpu.roll(centre, 1, 0) + pltpu.roll(centre, flat[0] - 1, 0)
            total = total + along_z[i * flat[0] : (i + 1) * flat[0]]
            results.append((total * scale).reshape(rhs.shape[1:]))
        return results

    sides = (0, span_x - 6)
    for k in range(1, ITERS):
        places = [k + u for u in range(6)] + [whole_span - 6 - k + u for u in range(6)]
        for x, result in zip(places, swept(k, places)):
            stages[k][x] = result

    stores = []
    for s in range(2):
        places = [first + 3 * s + u for first in sides for u in range(3)]
        for x, result in zip(places, swept(ITERS, [x + HALO for x in places])):
            for c in range(3):
                staged[c, x] = result[c, HALO : HALO + span_y, :]
        for side, first in enumerate(sides):
            window = slice(first + 3 * s, first + 3 * s + 3)
            stores.append(
                pltpu.make_async_copy(
                    staged.at[:, window], out_ref.at[:, window], sems.at[2 * s + side]
                )
            )
            stores[-1].start()
    for copy in stores:
        copy.wait()
    middle.wait()
    motion.wait()


def on_device(
    n_gx,
    n_gy,
    velocity,
    owner_block,
    base_x,
    base_y,
    base_z,
    delta_weights,
    marker_offset,
    sphere_motion,
    contact_sphere,
    contact_partner,
):
    span_x, span_y, extent_z = velocity.shape[1:]
    markers = base_x.shape[0]
    planes = span_x + 4
    every = markers // TILE + 8
    padded = planes + WINDOW - 1
    grown = (padded + 2, 3, ROWS, extent_z)
    vmem = pl.BlockSpec(memory_space=pltpu.VMEM)
    smem = pl.BlockSpec(memory_space=pltpu.SMEM)
    hbm = pl.BlockSpec(memory_space=pltpu.HBM)
    dma = pltpu.SemaphoreType.DMA
    motion = sphere_motion.T
    fhl, started, home, arrived = pl.pallas_call(
        functools.partial(request_kernel, n_gx, n_gy),
        out_shape=(
            jax.ShapeDtypeStruct((padded, 3 * ROWS, 2 * extent_z), BF16),
            jax.ShapeDtypeStruct(grown, F32),
            jax.ShapeDtypeStruct((32, markers), F32),
            jax.ShapeDtypeStruct((8, 24, TILE), F32),
        ),
        in_specs=[hbm] * 8,
        out_specs=(vmem,) * 4,
        scratch_shapes=[
            pltpu.VMEM(velocity.shape, F32),
            pltpu.VMEM((1, markers), I32),
            pltpu.VMEM((1, markers), I32),
            pltpu.VMEM((1, markers), I32),
            pltpu.VMEM((1, markers), I32),
            pltpu.VMEM((12, markers), F32),
            pltpu.VMEM((3, markers), F32),
            pltpu.SMEM((2, 6), F32),
            pltpu.VMEM((2, 3, 2, span_y, extent_z), F32),
            pltpu.VMEM((2, 3, 2 * span_x, extent_z), F32),
            pltpu.VMEM((4, 16, extent_z), F32),
            pltpu.VMEM((4, 16, extent_z), F32),
            pltpu.VMEM((2, 3, 2 * span_x, extent_z), F32),
            pltpu.VMEM((32, markers), F32),
            pltpu.VMEM((96, markers), BF16),
            pltpu.VMEM((8, TILE), F32),
            pltpu.VMEM((8, 24, TILE), F32),
            pltpu.VMEM((8, 24, TILE), F32),
            pltpu.VMEM((planes, 3, ROWS, extent_z), F32),
            dma((8,)),
            dma((8,)),
            dma((8,)),
            dma((8,)),
            dma((8,)),
        ],
        compiler_params=pltpu.CompilerParams(
            collective_id=0, has_side_effects=True, vmem_limit_bytes=24 << 20
        ),
        name="requests",
    )(
        *(
            pltpu.with_memory_space_constraint(array, pltpu.HBM)
            for array in (
                velocity,
                owner_block.reshape(1, markers),
                base_x.reshape(1, markers),
                base_y.reshape(1, markers),
                base_z.reshape(1, markers),
                delta_weights,
                marker_offset,
                motion,
            )
        )
    )
    rhs, acted = pl.pallas_call(
        marker_kernel,
        out_shape=(
            jax.ShapeDtypeStruct(grown, F32),
            jax.ShapeDtypeStruct((8, 128), F32),
        ),
        in_specs=[vmem] * 4,
        out_specs=(vmem,) * 2,
        scratch_shapes=[
            pltpu.VMEM((every, 96, TILE), BF16),
            pltpu.VMEM((every * BINS, TILE), F32),
            pltpu.VMEM((every * BINS, TILE), F32),
            pltpu.VMEM((every, TILE), F32),
            pltpu.VMEM((2, extent_z, TILE), BF16),
            pltpu.VMEM((2, 32, TILE), F32),
            pltpu.VMEM((8, 128), I32),
            pltpu.SMEM((8, 128), I32),
            dma,
        ],
        compiler_params=pltpu.CompilerParams(vmem_limit_bytes=24 << 20),
        name="markers",
    )(fhl, started, home, arrived)
    plane = (3, ROWS, extent_z)
    middle = planes - 8
    new_motion, *strips = pl.pallas_call(
        functools.partial(strip_kernel, n_gx, n_gy, markers // 2),
        out_shape=(
            jax.ShapeDtypeStruct(motion.shape, F32),
            jax.ShapeDtypeStruct((2, planes, 3, 8, extent_z), F32),
            jax.ShapeDtypeStruct((2, 6, 3, ROWS, extent_z), F32),
            jax.ShapeDtypeStruct((middle,) + plane, F32),
            jax.ShapeDtypeStruct((middle - 2,) + plane, F32),
            jax.ShapeDtypeStruct((middle - 4,) + plane, F32),
            jax.ShapeDtypeStruct((middle - 6,) + plane, F32),
            jax.ShapeDtypeStruct((3, middle - 8, span_y, extent_z), F32),
        ),
        in_specs=[vmem] * 2 + [smem] * 3,
        out_specs=(vmem,) * 8,
        scratch_shapes=[
            pltpu.VMEM((8, 8, 128), F32),
            pltpu.VMEM((8, 8, 128), F32),
            pltpu.VMEM((n_gx, 1, 128), F32),
            pltpu.VMEM((n_gy, 1, 128), F32),
            pltpu.VMEM((2, 1, 128), F32),
            pltpu.VMEM((8, 128), F32),
            pltpu.VMEM((2, 6, 3, ROWS, extent_z), F32),
            dma((8,)),
            dma((8,)),
            dma((n_gx,)),
            dma((n_gx,)),
            dma((n_gy,)),
            dma((n_gy,)),
            dma((16,)),
            dma((16,)),
            dma((6,)),
            dma((6,)),
        ],
        compiler_params=pltpu.CompilerParams(
            collective_id=1, has_side_effects=True, vmem_limit_bytes=24 << 20
        ),
        name="strips",
    )(rhs, acted, motion, contact_sphere, contact_partner)
    velocity_star, new_motion = pl.pallas_call(
        functools.partial(relax_kernel, n_gy),
        out_shape=(
            jax.ShapeDtypeStruct(velocity.shape, F32),
            jax.ShapeDtypeStruct(motion.shape, F32),
        ),
        in_specs=[vmem] * 9,
        out_specs=(hbm, hbm),
        scratch_shapes=[pltpu.VMEM((planes + 4,) + plane, F32)] * 4
        + [
            pltpu.VMEM(velocity.shape, F32),
            pltpu.VMEM((2 * extent_z, extent_z), BF16),
            dma((6,)),
            dma,
            dma,
        ],
        compiler_params=pltpu.CompilerParams(vmem_limit_bytes=24 << 20),
        name="relax",
    )(rhs, *strips, new_motion)
    return velocity_star, new_motion.T


def solution(mesh):
    placed = (
        P(None, "gx", "gy", None),
        P(("gx", "gy"), None),
        P(("gx", "gy")),
        P(("gx", "gy")),
        P(("gx", "gy")),
        P(None, ("gx", "gy")),
        P(None, ("gx", "gy")),
        P(None, ("gx", "gy")),
        P(("gx", "gy")),
        P(("gx", "gy")),
    )
    return jax.shard_map(
        functools.partial(on_device, mesh.shape["gx"], mesh.shape["gy"]),
        mesh=mesh,
        in_specs=placed,
        out_specs=(P(None, "gx", "gy", None), P(None, ("gx", "gy"))),
        check_vma=False,
    )
```

```python
import functools

import jax
import jax.numpy as jnp
from jax import lax
from jax.experimental import pallas as pl
from jax.experimental.pallas import tpu as pltpu
from jax.sharding import PartitionSpec as P

F32 = jnp.float32
BF16 = jnp.bfloat16
I32 = jnp.int32
MESH = pl.DeviceIdType.MESH

ITERS = 4
DIFFUSION = 1.0
RESPONSE = 0.5
DASHPOT = 0.1

TILE = 256
BINS = 32
WINDOW = 6
ROWS = 40
HALO = 4
LANES = [(dx, dy) for dx in (-1, 0, 1) for dy in (-1, 0, 1) if (dx, dy) != (0, 0)]
DIAGONALS = [(dx, dy) for dx, dy in LANES if dx * dy != 0]
RUNS = [
    ((0, 1), (19, 1)),
    ((1, 2), (17, 2)),
    ((3, 2), (15, 2)),
    ((5, 1), (14, 1)),
    ((6, 8),),
]
X_RUNS = len(RUNS) - 1


def split(values):
    high = values.astype(BF16)
    low = (values - high.astype(F32)).astype(BF16)
    return high, low


def pick(distance, weights):
    result = jnp.where(distance == 3, weights[3], 0.0)
    for k in (2, 1, 0):
        result = jnp.where(distance == k, weights[k], result)
    return result


def cross(a, b):
    return (
        a[1] * b[2] - a[2] * b[1],
        a[2] * b[0] - a[0] * b[2],
        a[0] * b[1] - a[1] * b[0],
    )


def remote(src, dst, send, recv, peer):
    return pltpu.make_async_remote_copy(
        src_ref=src,
        dst_ref=dst,
        send_sem=send,
        recv_sem=recv,
        device_id=peer,
        device_id_type=MESH,
    )


def greet(peers):
    barrier = pltpu.get_barrier_semaphore()
    for peer in peers:
        pl.semaphore_signal(barrier, inc=1, device_id=peer, device_id_type=MESH)
    return barrier


def neighbours(n_gx, n_gy):
    gx = lax.axis_index("gx")
    gy = lax.axis_index("gy")

    def at(dx, dy):
        return (lax.rem(gx + (dx + n_gx), n_gx), lax.rem(gy + (dy + n_gy), n_gy))

    return gx, gy, at


def terms(values):
    parts = []
    rest = values
    for _ in range(3):
        part = rest.astype(BF16)
        parts.append(part)
        rest = rest - part.astype(F32)
    return jnp.concatenate(parts, axis=0)


def chosen_columns(parts, slots, first):
    wanted = lax.broadcasted_iota(I32, (TILE, TILE), 0).astype(F32) + first
    hit = jnp.where(wanted == slots, 1.0, 0.0).astype(BF16)
    return lax.dot_general(parts, hit, (((1,), (1,)), ((), ())), preferred_element_type=F32)


def ranks(hits, above):
    return jnp.dot(hits.astype(BF16), above, preferred_element_type=F32)


def strictly_above(size):
    return (
        lax.broadcasted_iota(I32, (size, size), 0) < lax.broadcasted_iota(I32, (size, size), 1)
    ).astype(BF16)


def request_kernel(
    n_gx,
    n_gy,
    v_hbm,
    own_hbm,
    bx_hbm,
    by_hbm,
    bz_hbm,
    dw_hbm,
    off_hbm,
    mot_hbm,
    fhl,
    rhs,
    home,
    arrived,
    v_ref,
    own_ref,
    bx_ref,
    by_ref,
    bz_ref,
    dw_ref,
    off_ref,
    mot_ref,
    hx,
    hy,
    hc,
    corner,
    edges,
    pay,
    pay3,
    slot_s,
    snd,
    inbox,
    frame,
    in_sem,
    halo_send,
    halo_recv,
    pay_send,
    pay_recv,
):
    gx, gy, at = neighbours(n_gx, n_gy)
    here = gx * n_gy + gy
    barrier = greet([at(dx, dy) for dx, dy in LANES])
    loads = [
        pltpu.make_async_copy(src, dst, in_sem.at[i])
        for i, (src, dst) in enumerate(
            (
                (v_hbm, v_ref),
                (own_hbm, own_ref),
                (bx_hbm, bx_ref),
                (by_hbm, by_ref),
                (bz_hbm, bz_ref),
                (dw_hbm, dw_ref),
                (off_hbm, off_ref),
                (mot_hbm, mot_ref),
            )
        )
    ]
    for copy in loads:
        copy.start()
    markers = dw_ref.shape[1]
    chunks = markers // TILE
    span_x = v_ref.shape[1]
    span_y = v_ref.shape[2]
    extent_z = v_ref.shape[3]
    planes = span_x + 4
    for copy in loads:
        copy.wait()

    last = span_x - 2
    pl.semaphore_wait(barrier, len(LANES))
    halo = []
    halo.append(remote(v_ref.at[:, 0:2], hx.at[1], halo_send.at[0], halo_recv.at[0], at(-1, 0)))
    halo.append(
        remote(v_ref.at[:, last:span_x], hx.at[0], halo_send.at[1], halo_recv.at[1], at(1, 0))
    )
    halo.append(remote(edges.at[0], hy.at[1], halo_send.at[2], halo_recv.at[2], at(0, -1)))
    halo.append(remote(edges.at[1], hy.at[0], halo_send.at[3], halo_recv.at[3], at(0, 1)))
    for k, (dx, dy) in enumerate(DIAGONALS):
        slot = (1 if dx < 0 else 0) * 2 + (1 if dy < 0 else 0)
        halo.append(
            remote(
                corner.at[k], hc.at[slot], halo_send.at[4 + k], halo_recv.at[4 + k], at(dx, dy)
            )
        )
    corner[...] = jnp.zeros_like(corner)
    for k, (dx, dy) in enumerate(DIAGONALS):
        x0 = 0 if dx < 0 else last
        y0 = 0 if dy < 0 else span_y - 2
        for c in range(3):
            for i in range(2):
                row = 4 * c + 2 * i
                corner[k, row : row + 2, :] = v_ref[c, x0 + i, y0 : y0 + 2, :]
    for copy in halo[4:] + halo[0:2]:
        copy.start()
    for side, y0 in enumerate((0, span_y - 2)):
        for c in range(3):
            for x in range(span_x):
                edges[side, c, 2 * x : 2 * x + 2, :] = v_ref[c, x, y0 : y0 + 2, :]
    for copy in halo[2:4]:
        copy.start()

    pay[0:12, :] = dw_ref[...]
    pay[12:13, :] = bx_ref[...].astype(F32)
    pay[13:14, :] = by_ref[...].astype(F32)
    pay[14:15, :] = bz_ref[...].astype(F32)
    per_sphere = markers // 2
    second = (lax.broadcasted_iota(I32, (1, markers), 1) >= per_sphere).astype(F32)
    pay[15:16, :] = second
    motion = [mot_ref[0, c] * (1.0 - second) + mot_ref[1, c] * second for c in range(6)]
    offset = [off_ref[c : c + 1, :] for c in range(3)]
    swing = cross(motion[3:6], offset)
    for c in range(3):
        pay[16 + c : 17 + c, :] = motion[c] + swing[c]
        pay[19 + c : 20 + c, :] = offset[c]
    pay[22:23, :] = jnp.ones((1, markers), F32)
    pay[23:32, :] = jnp.zeros((9, markers), F32)
    whole = pay[...]
    pay3[...] = terms(whole)
    home[...] = whole
    home[22:23, :] = (own_ref[...] == here).astype(F32)

    above = strictly_above(TILE)
    bins = lax.broadcasted_iota(I32, (8, TILE), 0)
    carry = jnp.zeros((8, 1), F32)
    for q in range(chunks):
        owner = own_ref[:, q * TILE : (q + 1) * TILE]
        owner_x = lax.shift_right_logical(owner, n_gy.bit_length() - 1)
        owner_y = owner & (n_gy - 1)
        step_x = (owner_x - gx + 1) & (n_gx - 1)
        lane = step_x * 3 + (owner_y - gy + 1)
        lane = jnp.where(owner == here, -1, jnp.where(lane > 4, lane - 1, lane))
        hits = jnp.where(bins == lane, 1.0, 0.0)
        ranked = ranks(hits, above) + carry + bins.astype(F32) * TILE
        carry = carry + jnp.sum(hits, axis=1, keepdims=True)
        slot = jnp.sum(hits * ranked, axis=0, keepdims=True)
        slot_s[q : q + 1, :] = jnp.where(lane < 0, -1.0, slot)

    def compact(n, _):
        first = (n * TILE).astype(F32)
        moved = None
        for q in range(chunks):
            part = chosen_columns(
                pay3[:, q * TILE : (q + 1) * TILE], slot_s[q : q + 1, :], first
            )
            moved = part if moved is None else moved + part
        snd[n] = moved[0:24] + moved[32:56] + moved[64:88]
        return 0

    lax.fori_loop(0, 8, compact, 0)

    requests = [
        remote(snd.at[n], inbox.at[n], pay_send.at[n], pay_recv.at[n], at(dx, dy))
        for n, (dx, dy) in enumerate(LANES)
    ]
    for copy in requests:
        copy.start()

    inner_low = jnp.where(gy > 0, 1.0, 0.0).astype(F32)
    inner_high = jnp.where(gy < n_gy - 1, 1.0, 0.0).astype(F32)

    def clear(p, _):
        rhs[p] = jnp.zeros((3, ROWS, extent_z), F32)
        return 0

    lax.fori_loop(0, rhs.shape[0], clear, 0)

    def clear_frame(p, _):
        frame[p] = jnp.zeros((3, ROWS, extent_z), F32)
        return 0

    lax.fori_loop(0, planes, clear_frame, 0)

    def clear_beyond(p, _):
        fhl[p] = jnp.zeros((3 * ROWS, 2 * extent_z), BF16)
        return 0

    lax.fori_loop(planes, fhl.shape[0], clear_beyond, 0)

    def place(x, _):
        for c in range(3):
            plane = v_ref[c, x]
            frame[x + 2, c, 4 : 4 + span_y, :] = plane
            rhs[x + 4, c, 4 : 4 + span_y, :] = plane
        return 0

    lax.fori_loop(0, span_x, place, 0)
    for copy in halo:
        copy.wait()

    for x in range(span_x):
        for c in range(3):
            frame[x + 2, c, 2:4, :] = hy[0, c, 2 * x : 2 * x + 2, :] * inner_low
            frame[x + 2, c, 36:38, :] = hy[1, c, 2 * x : 2 * x + 2, :] * inner_high
    for side in range(2):
        for i in range(2):
            p = (0 if side == 0 else planes - 2) + i
            for c in range(3):
                frame[p, c, 4 : 4 + span_y, :] = hx[side, c, i]
                frame[p, c, 2:4, :] = hc[side * 2, 4 * c + 2 * i : 4 * c + 2 * i + 2, :] * inner_low
                frame[p, c, 36:38, :] = (
                    hc[side * 2 + 1, 4 * c + 2 * i : 4 * c + 2 * i + 2, :] * inner_high
                )

    def halve(p, _):
        high, low = split(frame[p].reshape(3 * ROWS, extent_z))
        fhl[p, :, 0:extent_z] = high
        fhl[p, :, extent_z : 2 * extent_z] = low
        return 0

    lax.fori_loop(0, planes, halve, 0)
    for copy in requests:
        copy.wait()
    arrived[...] = inbox[...]


def marker_kernel(
    fhl,
    rhs_in,
    home,
    arrived,
    rhs,
    acted,
    pay3,
    hit_s,
    rank_s,
    slot_s,
    tz,
    held,
    edge_v,
    edge,
    edge_sem,
):
    chunks = home.shape[1] // TILE
    every = chunks + 8
    extent_z = rhs.shape[3]
    bins = lax.broadcasted_iota(I32, (BINS, TILE), 0).astype(F32)

    def chunk(q):
        return home[0:24, q * TILE : (q + 1) * TILE] if q < chunks else arrived[q - chunks]

    totals = []
    for q in range(every):
        m = chunk(q)
        hits = jnp.where((bins == m[12:13]) & (m[22:23] > 0.5), 1.0, 0.0)
        hit_s[q * BINS : (q + 1) * BINS, :] = hits
        totals.append(jnp.sum(hits, axis=1, keepdims=True))
    rank_s[...] = ranks(hit_s[...], strictly_above(TILE))
    carries = []
    count = jnp.zeros((BINS, 1), F32)
    for q in range(every):
        carries.append(count)
        count = count + totals[q]
    count = jnp.broadcast_to(count, (BINS, 128))
    high, low = split(count)
    below = (
        lax.broadcasted_iota(I32, (BINS, BINS), 0) > lax.broadcasted_iota(I32, (BINS, BINS), 1)
    ).astype(BF16)
    start = jnp.dot(below, high, preferred_element_type=F32)
    start = start + jnp.dot(below, low, preferred_element_type=F32)
    opening = lax.broadcasted_iota(I32, (BINS, 128), 1).astype(F32) * TILE
    present = jnp.sum(count, axis=0, keepdims=True)
    closing = jnp.minimum(opening + TILE, present)
    first_bin = jnp.sum(jnp.where(start + count <= opening, 1.0, 0.0), axis=0, keepdims=True)
    last_bin = jnp.sum(jnp.where(start < closing, 1.0, 0.0), axis=0, keepdims=True) - 1.0
    edge_v[...] = jnp.concatenate(
        [first_bin, last_bin, present, jnp.zeros((5, 128), F32)], axis=0
    ).astype(I32)
    to_scalars = pltpu.make_async_copy(edge_v, edge, edge_sem)
    to_scalars.start()
    start = start[:, 0:1]
    for q in range(every):
        hits = hit_s[q * BINS : (q + 1) * BINS, :]
        ranked = rank_s[q * BINS : (q + 1) * BINS, :] + (carries[q] + start)
        slot = jnp.sum(hits * ranked, axis=0, keepdims=True)
        there = jnp.sum(hits, axis=0, keepdims=True)
        slot_s[q : q + 1, :] = jnp.where(there > 0.5, slot, -1.0)
        m = chunk(q)
        if q < chunks:
            source = jnp.zeros((1, TILE), F32)
        else:
            source = jnp.full((1, TILE), float(q - chunks + 1), F32)
        filled = jnp.concatenate([m[0:23], source, jnp.zeros((8, TILE), F32)], axis=0)
        pay3[q] = terms(filled)
    acted[...] = jnp.zeros_like(acted)

    def start_from(p, _):
        rhs[p] = rhs_in[p]
        return 0

    lax.fori_loop(0, rhs.shape[0], start_from, 0)
    slot_id = lax.broadcasted_iota(I32, (TILE, TILE), 0).astype(F32)

    def gather(n):
        wanted = slot_id + (n * TILE).astype(F32)
        moved = None
        for q in range(every):
            hit = jnp.where(wanted == slot_s[q : q + 1, :], 1.0, 0.0).astype(BF16)
            part = lax.dot_general(
                hit, pay3[q], (((1,), (1,)), ((), ())), preferred_element_type=F32
            )
            moved = part if moved is None else moved + part
        moved = jnp.concatenate([moved, jnp.zeros((TILE, 32), F32)], axis=1).T
        return moved[0:32] + moved[32:64] + moved[64:96]

    def prepare(m):
        cell_y = m[13:14].astype(I32)
        cell_z = m[14:15].astype(I32)
        z = lax.broadcasted_iota(I32, (extent_z, TILE), 0)
        table = pick((z - cell_z) & (extent_z - 1), [m[8 + i : 9 + i] for i in range(4)])
        high, low = split(table)
        y = lax.broadcasted_iota(I32, (ROWS, TILE), 0) - 2
        table_y = pick(y - cell_y, [m[4 + i : 5 + i] for i in range(4)])
        return high, low, table_y

    def x_table(m, plane):
        x = lax.broadcasted_iota(I32, (8, TILE), 0)
        return pick(x + plane - m[12:13].astype(I32), [m[i : i + 1] for i in range(4)])

    def sample(m, plane, high, low, table_y, totals):
        table_x = x_table(m, plane)
        folded_y = table_y.reshape(ROWS // 8, 8, TILE)
        both = fhl[pl.ds(plane, WINDOW)].reshape(WINDOW * 3 * ROWS, 2 * extent_z)
        left = jnp.concatenate([both, both[:, 0:extent_z]], axis=1)
        right = jnp.concatenate([high, high, low], axis=0)
        part = jnp.dot(left, right, preferred_element_type=F32)
        part = part.reshape(WINDOW, 3, ROWS // 8, 8, TILE)
        result = []
        for c in range(3):
            total = totals[c]
            for p in range(WINDOW):
                total = total + jnp.sum(part[p, c] * folded_y, axis=0) * table_x[p : p + 1]
            result.append(total)
        return tuple(result)

    def act(m, totals):
        totals = [jnp.sum(total, axis=0, keepdims=True) for total in totals]
        force = [m[16 + c : 17 + c] - totals[c] for c in range(3)]
        torque = cross([m[19 + c : 20 + c] for c in range(3)], force)
        acting = jnp.concatenate(force + list(torque) + [jnp.zeros((2, TILE), F32)], axis=0)
        group = m[23:24] * 2.0 + m[15:16]
        member = (
            (lax.broadcasted_iota(I32, (128, TILE), 0).astype(F32) == group)
            & (m[22:23] > 0.5)
        ).astype(F32)
        summed = lax.dot_general(
            terms(acting),
            member.astype(BF16),
            (((1,), (1,)), ((), ())),
            preferred_element_type=F32,
        )
        acted[...] += summed[0:8] + summed[8:16] + summed[16:24]
        return force

    def deposit(m, plane, force, z_high, z_low, table_y):
        table_x = x_table(m, plane)
        rows = []
        for p in range(WINDOW):
            for c in range(3):
                rows.append((force[c] * table_x[p : p + 1]) * table_y)
        high, low = split(jnp.concatenate(rows, axis=0))
        left = jnp.concatenate([high, low, high], axis=1)
        right = jnp.concatenate([z_high, z_high, z_low], axis=1)
        added = lax.dot_general(
            left, right, (((1,), (1,)), ((), ())), preferred_element_type=F32
        )
        rhs[pl.ds(plane + 2, WINDOW)] += added.reshape(WINDOW, 3, ROWS, extent_z)

    held[0] = gather(jnp.int32(0))
    to_scalars.wait()
    tiles = lax.shift_right_logical(edge[2, 0] + (TILE - 1), TILE.bit_length() - 1)
    nothing = (jnp.zeros((8, TILE), F32),) * 3

    def work(n, _):
        low_plane = edge[0, n]
        spans = (edge[1, n] + 3 - low_plane + WINDOW) // WINDOW
        slot = n & 1

        @pl.when(spans <= 1)
        def _narrow():
            m = held[slot]
            high, low, table_y = prepare(m)
            totals = sample(m, low_plane, high, low, table_y, nothing)
            following = gather(n + 1)
            force = act(m, totals)
            deposit(m, low_plane, force, high, low, table_y)
            held[1 - slot] = following

        @pl.when(spans > 1)
        def _wide():
            m = held[slot]
            high, low, table_y = prepare(m)
            tz[0] = high
            tz[1] = low

            def sample_span(j, totals):
                plane = low_plane + j * WINDOW
                return sample(held[slot], plane, tz[0], tz[1], table_y, totals)

            force = act(m, lax.fori_loop(0, spans, sample_span, nothing))

            def deposit_span(j, _):
                plane = low_plane + j * WINDOW
                deposit(held[slot], plane, force, tz[0], tz[1], table_y)
                return 0

            lax.fori_loop(0, spans, deposit_span, 0)
            held[1 - slot] = gather(n + 1)

        return 0

    lax.fori_loop(0, tiles, work, 0)


def wall_masks(gy, n_gy, span_y, extent_z):
    y = lax.broadcasted_iota(I32, (ROWS, extent_z), 0)
    low_edge = jnp.where(gy > 0, 0, HALO)
    high_edge = jnp.where(gy < n_gy - 1, ROWS, HALO + span_y)
    inside = jnp.where((y >= low_edge) & (y < high_edge), 1.0, 0.0).astype(F32)
    inside = jnp.concatenate([inside] * 3, axis=0)
    return inside, inside * (1.0 / (1.0 + 6.0 * DIFFUSION))


def relaxed(rhs, before, centre, after, scale):
    shape = rhs.shape
    flat = scale.shape
    centre = centre.reshape(flat)
    total = rhs.reshape(flat) + before.reshape(flat) + after.reshape(flat)
    total = total + pltpu.roll(centre, 1, 0) + pltpu.roll(centre, flat[0] - 1, 0)
    total = total + pltpu.roll(centre, 1, 1) + pltpu.roll(centre, flat[1] - 1, 1)
    return (total * scale).reshape(shape)


def strip_kernel(
    n_gx,
    n_gy,
    per_sphere,
    rhs,
    acted,
    mot_ref,
    cs_ref,
    cp_ref,
    nm_ref,
    xbuf,
    level_0,
    level_1,
    level_2,
    level_3,
    done,
    ybuf,
    sums,
    ret,
    agx,
    agy,
    ag1,
    moved_s,
    staged,
    ret_send,
    ret_recv,
    agx_send,
    agx_recv,
    agy_send,
    agy_recv,
    y_send,
    y_recv,
    x_send,
    x_recv,
):
    gx, gy, at = neighbours(n_gx, n_gy)
    here = gx * n_gy + gy
    planes = ybuf.shape[1]
    span_y = done.shape[2]
    peers = (
        [at(k, 0) for k in range(1, n_gx)]
        + [at(0, k) for k in range(1, n_gy)]
        + [at(dx, dy) for dx in (-1, 1) for dy in (-1, 1)]
    )
    barrier = greet(peers)
    inner_low = jnp.where(gy > 0, 1.0, 0.0).astype(F32)
    inner_high = jnp.where(gy < n_gy - 1, 1.0, 0.0).astype(F32)
    replies = [
        remote(sums.at[n], ret.at[n], ret_send.at[n], ret_recv.at[n], at(-dx, -dy))
        for n, (dx, dy) in enumerate(LANES)
    ]
    lanes = lax.broadcasted_iota(I32, (8, 128), 1)
    row_id = lax.broadcasted_iota(I32, (8, 128), 0)
    pl.semaphore_wait(barrier, len(peers))

    def along_x(k):
        return remote(ag1.at[0], agx.at[k], agx_send.at[k], agx_recv.at[k], at(k, 0))

    def along_y(k):
        return remote(ag1.at[1], agy.at[k], agy_send.at[k], agy_recv.at[k], at(0, k))

    def sphere_step_one():
        for copy in replies:
            copy.wait()
        total = acted[...]
        for n in range(8):
            total = total + ret[n]
        start = jnp.zeros((8, 128), F32)
        for c in range(6):
            for s in range(2):
                start = jnp.where((row_id == c) & (lanes == s), mot_ref[s, c], start)
        moved = start - total * (RESPONSE / per_sphere)
        moved_s[...] = moved
        lane = lanes[0:1]
        message = jnp.zeros((1, 128), F32)
        for sphere in range(2):
            for c in range(3):
                message = jnp.where(
                    lane == 3 * sphere + c, moved[c : c + 1, sphere : sphere + 1], message
                )
        ag1[0] = message
        for k in range(1, n_gx):
            along_x(k).start()

    def sphere_step_two():
        for k in range(1, n_gx):
            along_x(k).wait()
        total = ag1[0]
        for k in range(1, n_gx):
            total = total + pltpu.roll(agx[k], 6 * k, 1)
        ag1[1] = total
        for k in range(1, n_gy):
            along_y(k).start()

    def sphere_step_three():
        for k in range(1, n_gy):
            along_y(k).wait()
        table = jnp.concatenate([ag1[1]] + [agy[k] for k in range(1, n_gy)], axis=0)
        moved = moved_s[...]
        pull = jnp.zeros((8, 128), F32)
        for k in range(cs_ref.shape[0]):
            partner = cp_ref[k]
            own = cs_ref[k] - 2 * here
            holder = lax.shift_right_logical(partner, 1)
            holder_x = lax.shift_right_logical(holder, n_gy.bit_length() - 1)
            row = (gy - (holder & (n_gy - 1)) + n_gy) & (n_gy - 1)
            lane = 6 * ((gx - holder_x + n_gx) & (n_gx - 1)) + 3 * (partner & 1)
            mine = jnp.where(row_id == row, table, 0.0)
            for c in range(3):
                chosen = jnp.sum(
                    jnp.where(lanes == lane + c, mine, 0.0), axis=(0, 1), keepdims=True
                )
                pull = pull + jnp.where((lanes == own) & (row_id == c), chosen - moved, 0.0)
        settled = jnp.concatenate(
            [moved + DASHPOT * pull, jnp.zeros((120, 128), F32)], axis=0
        )
        nm_ref[...] = settled.T[0:2, 0:6]

    def y_copies(g):
        copies = []
        for r, (first, count) in enumerate(RUNS[g]):
            lo = first + 2
            base = 4 * g + 2 * r
            copies.append(
                remote(
                    rhs.at[pl.ds(lo, count), :, pl.ds(0, 8)],
                    ybuf.at[1, pl.ds(first, count)],
                    y_send.at[base],
                    y_recv.at[base],
                    at(0, -1),
                )
            )
            copies.append(
                remote(
                    rhs.at[pl.ds(lo, count), :, pl.ds(ROWS - 8, 8)],
                    ybuf.at[0, pl.ds(first, count)],
                    y_send.at[base + 1],
                    y_recv.at[base + 1],
                    at(0, 1),
                )
            )
        return copies

    def x_copies(g):
        (low, count), (high, _) = RUNS[g]
        high = high - (planes - 6)
        return [
            remote(
                staged.at[1, pl.ds(low, count)],
                xbuf.at[1, pl.ds(low, count)],
                x_send.at[2 * g],
                x_recv.at[2 * g],
                at(-1, 0),
            ),
            remote(
                staged.at[0, pl.ds(high, count)],
                xbuf.at[0, pl.ds(high, count)],
                x_send.at[2 * g + 1],
                x_recv.at[2 * g + 1],
                at(1, 0),
            ),
        ]

    def with_strips(p):
        whole = rhs[p + 2]
        low = whole[:, 0:8] + ybuf[0, p] * inner_low
        high = whole[:, ROWS - 8 : ROWS] + ybuf[1, p] * inner_high
        return jnp.concatenate([low, whole[:, 8 : ROWS - 8], high], axis=1)

    def stage(g):
        for side, base in ((1, 0), (0, planes - 6)):
            first, count = RUNS[g][1 - side]
            for p in range(first, first + count):
                staged[side, p - base] = with_strips(p)

    for g in range(2):
        for copy in y_copies(g):
            copy.start()
    for n in range(8):
        sums[n] = pltpu.roll(acted[...], 128 - 2 * (n + 1), 1)
    for copy in replies:
        copy.start()
    for g in range(2, X_RUNS + 1):
        for copy in y_copies(g):
            copy.start()
    for g in range(2):
        for copy in y_copies(g):
            copy.wait()
        stage(g)
        for copy in x_copies(g):
            copy.start()
    sphere_step_one()
    for g in range(2, X_RUNS):
        for copy in y_copies(g):
            copy.wait()
        stage(g)
        for copy in x_copies(g):
            copy.start()
    for copy in y_copies(X_RUNS):
        copy.wait()
    inside, scale = wall_masks(gy, n_gy, span_y, rhs.shape[3])
    plane = rhs.shape[1:]
    stages = (level_0, level_1, level_2, level_3)
    first, last = 6, planes - 3

    def begin(x, _):
        level_0[x] = (with_strips(x - 2).reshape(inside.shape) * inside).reshape(plane)
        return 0

    lax.fori_loop(first, last + 1, begin, 0)

    def swept(k, x):
        source = stages[k - 1]
        return relaxed(level_0[x], source[x - 1], source[x], source[x + 1], scale)

    def finish(x):
        result = swept(ITERS, x)
        for c in range(3):
            done[c, x - HALO - 1] = result[c, HALO : HALO + span_y, :]

    for k in range(1, ITERS):

        def step(s, _, k=k):
            for u in range(2):
                x = first + k + 2 * s + u
                stages[k][x] = swept(k, x)
            return 0

        lax.fori_loop(0, (last - first + 1 - 2 * k) // 2, step, 0)
    for x in range(first + ITERS, last - ITERS + 1):
        finish(x)

    for g in range(X_RUNS - 1):
        for copy in x_copies(g):
            copy.wait()
        (low, count), _ = RUNS[g]
        left = list(range(5 - low - count + 1, 5 - low + 1))
        right = list(range(planes - 2 + low, planes - 2 + low + count))
        for x, beside in [(x, xbuf[0, x]) for x in left] + [
            (x, xbuf[1, x - planes + 2]) for x in right
        ]:
            whole = beside + (with_strips(x - 2) if 2 <= x < planes + 2 else rhs[x])
            level_0[x] = (whole.reshape(inside.shape) * inside).reshape(plane)
        for k in range(1, ITERS):
            for x in [x + k for x in left] + [x - k for x in right]:
                stages[k][x] = swept(k, x)
        for x in [x + ITERS for x in left] + [x - ITERS for x in right]:
            finish(x)
        if g == 0:
            sphere_step_two()
        if g == 1:
            sphere_step_three()
    for copy in x_copies(X_RUNS - 1):
        copy.wait()


def relax_kernel(
    n_gy, rhs, xbuf, level_0, level_1, level_2, level_3, done, nm_in, out_ref, nm_ref, staged, sems
):
    gy = lax.axis_index("gy")
    top = level_0.shape[0] - 1
    span_x = top + 1 - 2 * HALO
    span_y = out_ref.shape[2]
    copies = [
        pltpu.make_async_copy(done, out_ref.at[:, 1 : span_x - 1], sems.at[0]),
        pltpu.make_async_copy(nm_in, nm_ref, sems.at[1]),
    ]
    for copy in copies:
        copy.start()
    inside, scale = wall_masks(gy, n_gy, span_y, rhs.shape[3])
    plane = rhs.shape[1:]
    stages = (level_0, level_1, level_2, level_3)
    for side, (edge, inward) in enumerate(((0, 1), (top, -1))):
        whole = rhs[edge] + xbuf[side, 0 if side == 0 else 5]
        outer = (whole.reshape(inside.shape) * inside).reshape(plane)
        for k in range(1, ITERS + 1):
            x = edge + inward * k
            source = stages[k - 1]
            outer = relaxed(level_0[x], outer, source[x], source[x + inward], scale)
        x = 0 if side == 0 else span_x - 1
        for c in range(3):
            staged[side, c, 0] = outer[c, HALO : HALO + span_y, :]
        copies.append(
            pltpu.make_async_copy(staged.at[side], out_ref.at[:, x : x + 1], sems.at[2 + side])
        )
        copies[-1].start()
    for copy in copies:
        copy.wait()


def on_device(
    n_gx,
    n_gy,
    velocity,
    owner_block,
    base_x,
    base_y,
    base_z,
    delta_weights,
    marker_offset,
    sphere_motion,
    contact_sphere,
    contact_partner,
):
    span_x, span_y, extent_z = velocity.shape[1:]
    markers = base_x.shape[0]
    planes = span_x + 4
    every = markers // TILE + 8
    padded = planes + WINDOW - 1
    grown = (padded + 2, 3, ROWS, extent_z)
    vmem = pl.BlockSpec(memory_space=pltpu.VMEM)
    smem = pl.BlockSpec(memory_space=pltpu.SMEM)
    hbm = pl.BlockSpec(memory_space=pltpu.HBM)
    dma = pltpu.SemaphoreType.DMA
    motion = sphere_motion.T
    fhl, started, home, arrived = pl.pallas_call(
        functools.partial(request_kernel, n_gx, n_gy),
        out_shape=(
            jax.ShapeDtypeStruct((padded, 3 * ROWS, 2 * extent_z), BF16),
            jax.ShapeDtypeStruct(grown, F32),
            jax.ShapeDtypeStruct((32, markers), F32),
            jax.ShapeDtypeStruct((8, 24, TILE), F32),
        ),
        in_specs=[hbm] * 8,
        out_specs=(vmem,) * 4,
        scratch_shapes=[
            pltpu.VMEM(velocity.shape, F32),
            pltpu.VMEM((1, markers), I32),
            pltpu.VMEM((1, markers), I32),
            pltpu.VMEM((1, markers), I32),
            pltpu.VMEM((1, markers), I32),
            pltpu.VMEM((12, markers), F32),
            pltpu.VMEM((3, markers), F32),
            pltpu.SMEM((2, 6), F32),
            pltpu.VMEM((2, 3, 2, span_y, extent_z), F32),
            pltpu.VMEM((2, 3, 2 * span_x, extent_z), F32),
            pltpu.VMEM((4, 16, extent_z), F32),
            pltpu.VMEM((4, 16, extent_z), F32),
            pltpu.VMEM((2, 3, 2 * span_x, extent_z), F32),
            pltpu.VMEM((32, markers), F32),
            pltpu.VMEM((96, markers), BF16),
            pltpu.VMEM((8, TILE), F32),
            pltpu.VMEM((8, 24, TILE), F32),
            pltpu.VMEM((8, 24, TILE), F32),
            pltpu.VMEM((planes, 3, ROWS, extent_z), F32),
            dma((8,)),
            dma((8,)),
            dma((8,)),
            dma((8,)),
            dma((8,)),
        ],
        compiler_params=pltpu.CompilerParams(
            collective_id=0, has_side_effects=True, vmem_limit_bytes=24 << 20
        ),
        name="requests",
    )(
        *(
            pltpu.with_memory_space_constraint(array, pltpu.HBM)
            for array in (
                velocity,
                owner_block.reshape(1, markers),
                base_x.reshape(1, markers),
                base_y.reshape(1, markers),
                base_z.reshape(1, markers),
                delta_weights,
                marker_offset,
                motion,
            )
        )
    )
    rhs, acted = pl.pallas_call(
        marker_kernel,
        out_shape=(
            jax.ShapeDtypeStruct(grown, F32),
            jax.ShapeDtypeStruct((8, 128), F32),
        ),
        in_specs=[vmem] * 4,
        out_specs=(vmem,) * 2,
        scratch_shapes=[
            pltpu.VMEM((every, 96, TILE), BF16),
            pltpu.VMEM((every * BINS, TILE), F32),
            pltpu.VMEM((every * BINS, TILE), F32),
            pltpu.VMEM((every, TILE), F32),
            pltpu.VMEM((2, extent_z, TILE), BF16),
            pltpu.VMEM((2, 32, TILE), F32),
            pltpu.VMEM((8, 128), I32),
            pltpu.SMEM((8, 128), I32),
            dma,
        ],
        compiler_params=pltpu.CompilerParams(vmem_limit_bytes=24 << 20),
        name="markers",
    )(fhl, started, home, arrived)
    plane = (3, ROWS, extent_z)
    new_motion, *strips = pl.pallas_call(
        functools.partial(strip_kernel, n_gx, n_gy, markers // 2),
        out_shape=(
            jax.ShapeDtypeStruct(motion.shape, F32),
            jax.ShapeDtypeStruct((2, 6, 3, ROWS, extent_z), F32),
        )
        + (jax.ShapeDtypeStruct((planes + 4,) + plane, F32),) * 4
        + (jax.ShapeDtypeStruct((3, span_x - 2, span_y, extent_z), F32),),
        in_specs=[vmem] * 2 + [smem] * 3,
        out_specs=(vmem,) * 7,
        scratch_shapes=[
            pltpu.VMEM((2, planes, 3, 8, extent_z), F32),
            pltpu.VMEM((8, 8, 128), F32),
            pltpu.VMEM((8, 8, 128), F32),
            pltpu.VMEM((n_gx, 1, 128), F32),
            pltpu.VMEM((n_gy, 1, 128), F32),
            pltpu.VMEM((2, 1, 128), F32),
            pltpu.VMEM((8, 128), F32),
            pltpu.VMEM((2, 6, 3, ROWS, extent_z), F32),
            dma((8,)),
            dma((8,)),
            dma((n_gx,)),
            dma((n_gx,)),
            dma((n_gy,)),
            dma((n_gy,)),
            dma((4 * len(RUNS),)),
            dma((4 * len(RUNS),)),
            dma((2 * X_RUNS,)),
            dma((2 * X_RUNS,)),
        ],
        compiler_params=pltpu.CompilerParams(
            collective_id=1, has_side_effects=True, vmem_limit_bytes=24 << 20
        ),
        name="strips",
    )(rhs, acted, motion, contact_sphere, contact_partner)
    velocity_star, new_motion = pl.pallas_call(
        functools.partial(relax_kernel, n_gy),
        out_shape=(
            jax.ShapeDtypeStruct(velocity.shape, F32),
            jax.ShapeDtypeStruct(motion.shape, F32),
        ),
        in_specs=[vmem] * 8,
        out_specs=(hbm, hbm),
        scratch_shapes=[
            pltpu.VMEM((2, 3, 1, span_y, extent_z), F32),
            dma((4,)),
        ],
        compiler_params=pltpu.CompilerParams(vmem_limit_bytes=24 << 20),
        name="relax",
    )(rhs, *strips, new_motion)
    return velocity_star, new_motion.T


def solution(mesh):
    placed = (
        P(None, "gx", "gy", None),
        P(("gx", "gy"), None),
        P(("gx", "gy")),
        P(("gx", "gy")),
        P(("gx", "gy")),
        P(None, ("gx", "gy")),
        P(None, ("gx", "gy")),
        P(None, ("gx", "gy")),
        P(("gx", "gy")),
        P(("gx", "gy")),
    )
    return jax.shard_map(
        functools.partial(on_device, mesh.shape["gx"], mesh.shape["gy"]),
        mesh=mesh,
        in_specs=placed,
        out_specs=(P(None, "gx", "gy", None), P(None, ("gx", "gy"))),
        check_vma=False,
    )
```

```python
import functools

import jax
import jax.numpy as jnp
from jax import lax
from jax.experimental import pallas as pl
from jax.experimental.pallas import tpu as pltpu
from jax.sharding import PartitionSpec as P

F32 = jnp.float32
BF16 = jnp.bfloat16
I32 = jnp.int32
MESH = pl.DeviceIdType.MESH

ITERS = 4
DIFFUSION = 1.0
RESPONSE = 0.5
DASHPOT = 0.1

TILE = 256
BINS = 32
WINDOW = 6
ROWS = 40
HALO = 4
LANES = [(dx, dy) for dx in (-1, 0, 1) for dy in (-1, 0, 1) if (dx, dy) != (0, 0)]
DIAGONALS = [(dx, dy) for dx, dy in LANES if dx * dy != 0]
RUNS = [
    ((0, 1), (19, 1)),
    ((1, 2), (17, 2)),
    ((3, 2), (15, 2)),
    ((5, 1), (14, 1)),
    ((6, 8),),
]
X_RUNS = len(RUNS) - 1


def split(values):
    high = values.astype(BF16)
    low = (values - high.astype(F32)).astype(BF16)
    return high, low


def pick(distance, weights):
    result = jnp.where(distance == 3, weights[3], 0.0)
    for k in (2, 1, 0):
        result = jnp.where(distance == k, weights[k], result)
    return result


def cross(a, b):
    return (
        a[1] * b[2] - a[2] * b[1],
        a[2] * b[0] - a[0] * b[2],
        a[0] * b[1] - a[1] * b[0],
    )


def remote(src, dst, send, recv, peer):
    return pltpu.make_async_remote_copy(
        src_ref=src,
        dst_ref=dst,
        send_sem=send,
        recv_sem=recv,
        device_id=peer,
        device_id_type=MESH,
    )


def greet(peers):
    barrier = pltpu.get_barrier_semaphore()
    for peer in peers:
        pl.semaphore_signal(barrier, inc=1, device_id=peer, device_id_type=MESH)
    return barrier


def neighbours(n_gx, n_gy):
    gx = lax.axis_index("gx")
    gy = lax.axis_index("gy")

    def at(dx, dy):
        return (lax.rem(gx + (dx + n_gx), n_gx), lax.rem(gy + (dy + n_gy), n_gy))

    return gx, gy, at


def terms(values):
    parts = []
    rest = values
    for _ in range(3):
        part = rest.astype(BF16)
        parts.append(part)
        rest = rest - part.astype(F32)
    return jnp.concatenate(parts, axis=0)


def chosen_columns(parts, slots, first):
    wanted = lax.broadcasted_iota(I32, (TILE, TILE), 0).astype(F32) + first
    hit = jnp.where(wanted == slots, 1.0, 0.0).astype(BF16)
    return lax.dot_general(parts, hit, (((1,), (1,)), ((), ())), preferred_element_type=F32)


def ranks(hits, above):
    return jnp.dot(hits.astype(BF16), above, preferred_element_type=F32)


def strictly_above(size):
    return (
        lax.broadcasted_iota(I32, (size, size), 0) < lax.broadcasted_iota(I32, (size, size), 1)
    ).astype(BF16)


def request_kernel(
    n_gx,
    n_gy,
    v_hbm,
    own_hbm,
    bx_hbm,
    by_hbm,
    bz_hbm,
    dw_hbm,
    off_hbm,
    mot_hbm,
    fhl,
    rhs,
    home,
    arrived,
    v_ref,
    own_ref,
    bx_ref,
    by_ref,
    bz_ref,
    dw_ref,
    off_ref,
    mot_ref,
    hx,
    hy,
    hc,
    corner,
    edges,
    pay,
    pay3,
    slot_s,
    snd,
    inbox,
    frame,
    in_sem,
    halo_send,
    halo_recv,
    pay_send,
    pay_recv,
):
    gx, gy, at = neighbours(n_gx, n_gy)
    here = gx * n_gy + gy
    barrier = greet([at(dx, dy) for dx, dy in LANES])
    loads = [
        pltpu.make_async_copy(src, dst, in_sem.at[i])
        for i, (src, dst) in enumerate(
            (
                (v_hbm, v_ref),
                (own_hbm, own_ref),
                (bx_hbm, bx_ref),
                (by_hbm, by_ref),
                (bz_hbm, bz_ref),
                (dw_hbm, dw_ref),
                (off_hbm, off_ref),
                (mot_hbm, mot_ref),
            )
        )
    ]
    for copy in loads:
        copy.start()
    markers = dw_ref.shape[1]
    chunks = markers // TILE
    span_x = v_ref.shape[1]
    span_y = v_ref.shape[2]
    extent_z = v_ref.shape[3]
    planes = span_x + 4
    for copy in loads:
        copy.wait()

    last = span_x - 2
    pl.semaphore_wait(barrier, len(LANES))
    halo = []
    halo.append(remote(v_ref.at[:, 0:2], hx.at[1], halo_send.at[0], halo_recv.at[0], at(-1, 0)))
    halo.append(
        remote(v_ref.at[:, last:span_x], hx.at[0], halo_send.at[1], halo_recv.at[1], at(1, 0))
    )
    halo.append(remote(edges.at[0], hy.at[1], halo_send.at[2], halo_recv.at[2], at(0, -1)))
    halo.append(remote(edges.at[1], hy.at[0], halo_send.at[3], halo_recv.at[3], at(0, 1)))
    for k, (dx, dy) in enumerate(DIAGONALS):
        slot = (1 if dx < 0 else 0) * 2 + (1 if dy < 0 else 0)
        halo.append(
            remote(
                corner.at[k], hc.at[slot], halo_send.at[4 + k], halo_recv.at[4 + k], at(dx, dy)
            )
        )
    corner[...] = jnp.zeros_like(corner)
    for k, (dx, dy) in enumerate(DIAGONALS):
        x0 = 0 if dx < 0 else last
        y0 = 0 if dy < 0 else span_y - 2
        for c in range(3):
            for i in range(2):
                row = 4 * c + 2 * i
                corner[k, row : row + 2, :] = v_ref[c, x0 + i, y0 : y0 + 2, :]
    for copy in halo[4:] + halo[0:2]:
        copy.start()
    for side, y0 in enumerate((0, span_y - 2)):
        for c in range(3):
            for x in range(span_x):
                edges[side, c, 2 * x : 2 * x + 2, :] = v_ref[c, x, y0 : y0 + 2, :]
    for copy in halo[2:4]:
        copy.start()

    pay[0:12, :] = dw_ref[...]
    pay[12:13, :] = bx_ref[...].astype(F32)
    pay[13:14, :] = by_ref[...].astype(F32)
    pay[14:15, :] = bz_ref[...].astype(F32)
    per_sphere = markers // 2
    second = (lax.broadcasted_iota(I32, (1, markers), 1) >= per_sphere).astype(F32)
    pay[15:16, :] = second
    motion = [mot_ref[0, c] * (1.0 - second) + mot_ref[1, c] * second for c in range(6)]
    offset = [off_ref[c : c + 1, :] for c in range(3)]
    swing = cross(motion[3:6], offset)
    for c in range(3):
        pay[16 + c : 17 + c, :] = motion[c] + swing[c]
        pay[19 + c : 20 + c, :] = offset[c]
    pay[22:23, :] = jnp.ones((1, markers), F32)
    pay[23:32, :] = jnp.zeros((9, markers), F32)
    whole = pay[...]
    pay3[...] = terms(whole)
    home[...] = whole
    home[22:23, :] = (own_ref[...] == here).astype(F32)

    above = strictly_above(TILE)
    bins = lax.broadcasted_iota(I32, (8, TILE), 0)
    carry = jnp.zeros((8, 1), F32)
    for q in range(chunks):
        owner = own_ref[:, q * TILE : (q + 1) * TILE]
        owner_x = lax.shift_right_logical(owner, n_gy.bit_length() - 1)
        owner_y = owner & (n_gy - 1)
        step_x = (owner_x - gx + 1) & (n_gx - 1)
        lane = step_x * 3 + (owner_y - gy + 1)
        lane = jnp.where(owner == here, -1, jnp.where(lane > 4, lane - 1, lane))
        hits = jnp.where(bins == lane, 1.0, 0.0)
        ranked = ranks(hits, above) + carry + bins.astype(F32) * TILE
        carry = carry + jnp.sum(hits, axis=1, keepdims=True)
        slot = jnp.sum(hits * ranked, axis=0, keepdims=True)
        slot_s[q : q + 1, :] = jnp.where(lane < 0, -1.0, slot)

    def compact(n, _):
        first = (n * TILE).astype(F32)
        moved = None
        for q in range(chunks):
            part = chosen_columns(
                pay3[:, q * TILE : (q + 1) * TILE], slot_s[q : q + 1, :], first
            )
            moved = part if moved is None else moved + part
        snd[n] = moved[0:24] + moved[32:56] + moved[64:88]
        return 0

    lax.fori_loop(0, 8, compact, 0)

    requests = [
        remote(snd.at[n], inbox.at[n], pay_send.at[n], pay_recv.at[n], at(dx, dy))
        for n, (dx, dy) in enumerate(LANES)
    ]
    for copy in requests:
        copy.start()

    inner_low = jnp.where(gy > 0, 1.0, 0.0).astype(F32)
    inner_high = jnp.where(gy < n_gy - 1, 1.0, 0.0).astype(F32)

    def clear(p, _):
        rhs[p] = jnp.zeros((3, ROWS, extent_z), F32)
        return 0

    lax.fori_loop(0, rhs.shape[0], clear, 0)

    def clear_frame(p, _):
        frame[p] = jnp.zeros((3, ROWS, extent_z), F32)
        return 0

    lax.fori_loop(0, planes, clear_frame, 0)

    def clear_beyond(p, _):
        fhl[p] = jnp.zeros((3 * ROWS, 2 * extent_z), BF16)
        return 0

    lax.fori_loop(planes, fhl.shape[0], clear_beyond, 0)

    def place(x, _):
        for c in range(3):
            plane = v_ref[c, x]
            frame[x + 2, c, 4 : 4 + span_y, :] = plane
            rhs[x + 4, c, 4 : 4 + span_y, :] = plane
        return 0

    lax.fori_loop(0, span_x, place, 0)
    for copy in halo:
        copy.wait()

    for x in range(span_x):
        for c in range(3):
            frame[x + 2, c, 2:4, :] = hy[0, c, 2 * x : 2 * x + 2, :] * inner_low
            frame[x + 2, c, 36:38, :] = hy[1, c, 2 * x : 2 * x + 2, :] * inner_high
    for side in range(2):
        for i in range(2):
            p = (0 if side == 0 else planes - 2) + i
            for c in range(3):
                frame[p, c, 4 : 4 + span_y, :] = hx[side, c, i]
                frame[p, c, 2:4, :] = hc[side * 2, 4 * c + 2 * i : 4 * c + 2 * i + 2, :] * inner_low
                frame[p, c, 36:38, :] = (
                    hc[side * 2 + 1, 4 * c + 2 * i : 4 * c + 2 * i + 2, :] * inner_high
                )

    def halve(p, _):
        high, low = split(frame[p].reshape(3 * ROWS, extent_z))
        fhl[p, :, 0:extent_z] = high
        fhl[p, :, extent_z : 2 * extent_z] = low
        return 0

    lax.fori_loop(0, planes, halve, 0)
    for copy in requests:
        copy.wait()
    arrived[...] = inbox[...]


def marker_kernel(
    fhl,
    rhs_in,
    home,
    arrived,
    rhs,
    acted,
    pay3,
    hit_s,
    rank_s,
    slot_s,
    tz,
    held,
    edge_v,
    edge,
    edge_sem,
):
    chunks = home.shape[1] // TILE
    every = chunks + 8
    extent_z = rhs.shape[3]
    bins = lax.broadcasted_iota(I32, (BINS, TILE), 0).astype(F32)

    def chunk(q):
        return home[0:24, q * TILE : (q + 1) * TILE] if q < chunks else arrived[q - chunks]

    totals = []
    for q in range(every):
        m = chunk(q)
        hits = jnp.where((bins == m[12:13]) & (m[22:23] > 0.5), 1.0, 0.0)
        hit_s[q * BINS : (q + 1) * BINS, :] = hits
        totals.append(jnp.sum(hits, axis=1, keepdims=True))
    rank_s[...] = ranks(hit_s[...], strictly_above(TILE))
    carries = []
    count = jnp.zeros((BINS, 1), F32)
    for q in range(every):
        carries.append(count)
        count = count + totals[q]
    count = jnp.broadcast_to(count, (BINS, 128))
    high, low = split(count)
    below = (
        lax.broadcasted_iota(I32, (BINS, BINS), 0) > lax.broadcasted_iota(I32, (BINS, BINS), 1)
    ).astype(BF16)
    start = jnp.dot(below, high, preferred_element_type=F32)
    start = start + jnp.dot(below, low, preferred_element_type=F32)
    opening = lax.broadcasted_iota(I32, (BINS, 128), 1).astype(F32) * TILE
    present = jnp.sum(count, axis=0, keepdims=True)
    closing = jnp.minimum(opening + TILE, present)
    first_bin = jnp.sum(jnp.where(start + count <= opening, 1.0, 0.0), axis=0, keepdims=True)
    last_bin = jnp.sum(jnp.where(start < closing, 1.0, 0.0), axis=0, keepdims=True) - 1.0
    edge_v[...] = jnp.concatenate(
        [first_bin, last_bin, present, jnp.zeros((5, 128), F32)], axis=0
    ).astype(I32)
    to_scalars = pltpu.make_async_copy(edge_v, edge, edge_sem)
    to_scalars.start()
    start = start[:, 0:1]
    for q in range(every):
        hits = hit_s[q * BINS : (q + 1) * BINS, :]
        ranked = rank_s[q * BINS : (q + 1) * BINS, :] + (carries[q] + start)
        slot = jnp.sum(hits * ranked, axis=0, keepdims=True)
        there = jnp.sum(hits, axis=0, keepdims=True)
        slot_s[q : q + 1, :] = jnp.where(there > 0.5, slot, -1.0)
        m = chunk(q)
        if q < chunks:
            source = jnp.zeros((1, TILE), F32)
        else:
            source = jnp.full((1, TILE), float(q - chunks + 1), F32)
        filled = jnp.concatenate([m[0:23], source, jnp.zeros((8, TILE), F32)], axis=0)
        pay3[q] = terms(filled)
    acted[...] = jnp.zeros_like(acted)

    def start_from(p, _):
        rhs[p] = rhs_in[p]
        return 0

    lax.fori_loop(0, rhs.shape[0], start_from, 0)
    slot_id = lax.broadcasted_iota(I32, (TILE, TILE), 0).astype(F32)

    def gather(n):
        wanted = slot_id + (n * TILE).astype(F32)
        moved = None
        for q in range(every):
            hit = jnp.where(wanted == slot_s[q : q + 1, :], 1.0, 0.0).astype(BF16)
            part = lax.dot_general(
                hit, pay3[q], (((1,), (1,)), ((), ())), preferred_element_type=F32
            )
            moved = part if moved is None else moved + part
        moved = jnp.concatenate([moved, jnp.zeros((TILE, 32), F32)], axis=1).T
        return moved[0:32] + moved[32:64] + moved[64:96]

    def prepare(m):
        cell_y = m[13:14].astype(I32)
        cell_z = m[14:15].astype(I32)
        z = lax.broadcasted_iota(I32, (extent_z, TILE), 0)
        table = pick((z - cell_z) & (extent_z - 1), [m[8 + i : 9 + i] for i in range(4)])
        high, low = split(table)
        y = lax.broadcasted_iota(I32, (ROWS, TILE), 0) - 2
        table_y = pick(y - cell_y, [m[4 + i : 5 + i] for i in range(4)])
        return high, low, table_y

    def x_table(m, plane):
        x = lax.broadcasted_iota(I32, (8, TILE), 0)
        return pick(x + plane - m[12:13].astype(I32), [m[i : i + 1] for i in range(4)])

    def sample(m, plane, high, low, table_y, totals):
        table_x = x_table(m, plane)
        folded_y = table_y.reshape(ROWS // 8, 8, TILE)
        both = fhl[pl.ds(plane, WINDOW)].reshape(WINDOW * 3 * ROWS, 2 * extent_z)
        left = jnp.concatenate([both, both[:, 0:extent_z]], axis=1)
        right = jnp.concatenate([high, high, low], axis=0)
        part = jnp.dot(left, right, preferred_element_type=F32)
        part = part.reshape(WINDOW, 3, ROWS // 8, 8, TILE)
        result = []
        for c in range(3):
            total = totals[c]
            for p in range(WINDOW):
                total = total + jnp.sum(part[p, c] * folded_y, axis=0) * table_x[p : p + 1]
            result.append(total)
        return tuple(result)

    def act(m, totals):
        totals = [jnp.sum(total, axis=0, keepdims=True) for total in totals]
        force = [m[16 + c : 17 + c] - totals[c] for c in range(3)]
        torque = cross([m[19 + c : 20 + c] for c in range(3)], force)
        acting = jnp.concatenate(force + list(torque) + [jnp.zeros((2, TILE), F32)], axis=0)
        group = m[23:24] * 2.0 + m[15:16]
        member = (
            (lax.broadcasted_iota(I32, (128, TILE), 0).astype(F32) == group)
            & (m[22:23] > 0.5)
        ).astype(F32)
        summed = lax.dot_general(
            terms(acting),
            member.astype(BF16),
            (((1,), (1,)), ((), ())),
            preferred_element_type=F32,
        )
        acted[...] += summed[0:8] + summed[8:16] + summed[16:24]
        return force

    def deposit(m, plane, force, z_high, z_low, table_y):
        table_x = x_table(m, plane)
        rows = []
        for p in range(WINDOW):
            for c in range(3):
                rows.append((force[c] * table_x[p : p + 1]) * table_y)
        high, low = split(jnp.concatenate(rows, axis=0))
        left = jnp.concatenate([high, low, high], axis=1)
        right = jnp.concatenate([z_high, z_high, z_low], axis=1)
        added = lax.dot_general(
            left, right, (((1,), (1,)), ((), ())), preferred_element_type=F32
        )
        rhs[pl.ds(plane + 2, WINDOW)] += added.reshape(WINDOW, 3, ROWS, extent_z)

    held[0] = gather(jnp.int32(0))
    to_scalars.wait()
    tiles = lax.shift_right_logical(edge[2, 0] + (TILE - 1), TILE.bit_length() - 1)
    nothing = (jnp.zeros((8, TILE), F32),) * 3

    def work(n, _):
        low_plane = edge[0, n]
        spans = (edge[1, n] + 3 - low_plane + WINDOW) // WINDOW
        slot = n & 1

        @pl.when(spans <= 1)
        def _narrow():
            m = held[slot]
            high, low, table_y = prepare(m)
            totals = sample(m, low_plane, high, low, table_y, nothing)
            following = gather(n + 1)
            force = act(m, totals)
            deposit(m, low_plane, force, high, low, table_y)
            held[1 - slot] = following

        @pl.when(spans > 1)
        def _wide():
            m = held[slot]
            high, low, table_y = prepare(m)
            tz[0] = high
            tz[1] = low

            def sample_span(j, totals):
                plane = low_plane + j * WINDOW
                return sample(held[slot], plane, tz[0], tz[1], table_y, totals)

            force = act(m, lax.fori_loop(0, spans, sample_span, nothing))

            def deposit_span(j, _):
                plane = low_plane + j * WINDOW
                deposit(held[slot], plane, force, tz[0], tz[1], table_y)
                return 0

            lax.fori_loop(0, spans, deposit_span, 0)
            held[1 - slot] = gather(n + 1)

        return 0

    lax.fori_loop(0, tiles, work, 0)


def wall_masks(gy, n_gy, span_y, extent_z):
    y = lax.broadcasted_iota(I32, (ROWS, extent_z), 0)
    low_edge = jnp.where(gy > 0, 0, HALO)
    high_edge = jnp.where(gy < n_gy - 1, ROWS, HALO + span_y)
    inside = jnp.where((y >= low_edge) & (y < high_edge), 1.0, 0.0).astype(F32)
    inside = jnp.concatenate([inside] * 3, axis=0)
    return inside, inside * (1.0 / (1.0 + 6.0 * DIFFUSION))


def relaxed(rhs, before, centre, after, scale):
    shape = rhs.shape
    flat = scale.shape
    centre = centre.reshape(flat)
    total = rhs.reshape(flat) + before.reshape(flat) + after.reshape(flat)
    total = total + pltpu.roll(centre, 1, 0) + pltpu.roll(centre, flat[0] - 1, 0)
    total = total + pltpu.roll(centre, 1, 1) + pltpu.roll(centre, flat[1] - 1, 1)
    return (total * scale).reshape(shape)


def strip_kernel(
    n_gx,
    n_gy,
    per_sphere,
    rhs,
    acted,
    mot_ref,
    cs_ref,
    cp_ref,
    nm_ref,
    xbuf,
    level_0,
    level_1,
    level_2,
    level_3,
    done,
    ybuf,
    zbuf,
    sums,
    ret,
    agx,
    agy,
    ag1,
    moved_s,
    staged,
    ret_send,
    ret_recv,
    agx_send,
    agx_recv,
    agy_send,
    agy_recv,
    y_send,
    y_recv,
    x_send,
    x_recv,
    z_send,
    z_recv,
):
    gx, gy, at = neighbours(n_gx, n_gy)
    here = gx * n_gy + gy
    planes = ybuf.shape[1]
    span_y = done.shape[2]
    peers = (
        [at(k, 0) for k in range(1, n_gx)]
        + [at(0, k) for k in range(1, n_gy)]
        + [at(dx, dy) for dx in (-1, 1) for dy in (-1, 1)]
    )
    barrier = greet(peers)
    inner_low = jnp.where(gy > 0, 1.0, 0.0).astype(F32)
    inner_high = jnp.where(gy < n_gy - 1, 1.0, 0.0).astype(F32)
    replies = [
        remote(sums.at[n], ret.at[n], ret_send.at[n], ret_recv.at[n], at(-dx, -dy))
        for n, (dx, dy) in enumerate(LANES)
    ]
    lanes = lax.broadcasted_iota(I32, (8, 128), 1)
    row_id = lax.broadcasted_iota(I32, (8, 128), 0)
    pl.semaphore_wait(barrier, len(peers))

    def along_x(k):
        return remote(ag1.at[0], agx.at[k], agx_send.at[k], agx_recv.at[k], at(k, 0))

    def along_y(k):
        return remote(ag1.at[1], agy.at[k], agy_send.at[k], agy_recv.at[k], at(0, k))

    def sphere_step_one():
        for copy in replies:
            copy.wait()
        total = acted[...]
        for n in range(8):
            total = total + ret[n]
        start = jnp.zeros((8, 128), F32)
        for c in range(6):
            for s in range(2):
                start = jnp.where((row_id == c) & (lanes == s), mot_ref[s, c], start)
        moved = start - total * (RESPONSE / per_sphere)
        moved_s[...] = moved
        lane = lanes[0:1]
        message = jnp.zeros((1, 128), F32)
        for sphere in range(2):
            for c in range(3):
                message = jnp.where(
                    lane == 3 * sphere + c, moved[c : c + 1, sphere : sphere + 1], message
                )
        ag1[0] = message
        for k in range(1, n_gx):
            along_x(k).start()

    def sphere_step_two():
        for k in range(1, n_gx):
            along_x(k).wait()
        total = ag1[0]
        for k in range(1, n_gx):
            total = total + pltpu.roll(agx[k], 6 * k, 1)
        ag1[1] = total
        for k in range(1, n_gy):
            along_y(k).start()

    def sphere_step_three():
        for k in range(1, n_gy):
            along_y(k).wait()
        table = jnp.concatenate([ag1[1]] + [agy[k] for k in range(1, n_gy)], axis=0)
        moved = moved_s[...]
        pull = jnp.zeros((8, 128), F32)
        for k in range(cs_ref.shape[0]):
            partner = cp_ref[k]
            own = cs_ref[k] - 2 * here
            holder = lax.shift_right_logical(partner, 1)
            holder_x = lax.shift_right_logical(holder, n_gy.bit_length() - 1)
            row = (gy - (holder & (n_gy - 1)) + n_gy) & (n_gy - 1)
            lane = 6 * ((gx - holder_x + n_gx) & (n_gx - 1)) + 3 * (partner & 1)
            mine = jnp.where(row_id == row, table, 0.0)
            for c in range(3):
                chosen = jnp.sum(
                    jnp.where(lanes == lane + c, mine, 0.0), axis=(0, 1), keepdims=True
                )
                pull = pull + jnp.where((lanes == own) & (row_id == c), chosen - moved, 0.0)
        settled = jnp.concatenate(
            [moved + DASHPOT * pull, jnp.zeros((120, 128), F32)], axis=0
        )
        nm_ref[...] = settled.T[0:2, 0:6]

    def y_copies(g):
        copies = []
        for r, (first, count) in enumerate(RUNS[g]):
            lo = first + 2
            base = 4 * g + 2 * r
            copies.append(
                remote(
                    rhs.at[pl.ds(lo, count), :, pl.ds(0, 8)],
                    ybuf.at[1, pl.ds(first, count)],
                    y_send.at[base],
                    y_recv.at[base],
                    at(0, -1),
                )
            )
            copies.append(
                remote(
                    rhs.at[pl.ds(lo, count), :, pl.ds(ROWS - 8, 8)],
                    ybuf.at[0, pl.ds(first, count)],
                    y_send.at[base + 1],
                    y_recv.at[base + 1],
                    at(0, 1),
                )
            )
        return copies

    def x_copies(g):
        (low, count), (high, _) = RUNS[g]
        to_low, to_high = staged.at[1, pl.ds(low, count)], rhs.at[pl.ds(high + 2, count)]
        if g == 0:
            to_low = rhs.at[pl.ds(low + 2, count)]
        high = high - (planes - 6)
        if g > 0:
            to_high = staged.at[0, pl.ds(high, count)]
        return [
            remote(
                to_low,
                xbuf.at[1, pl.ds(low, count)],
                x_send.at[2 * g],
                x_recv.at[2 * g],
                at(-1, 0),
            ),
            remote(
                to_high,
                xbuf.at[0, pl.ds(high, count)],
                x_send.at[2 * g + 1],
                x_recv.at[2 * g + 1],
                at(1, 0),
            ),
        ]

    def corner_copies():
        return [
            remote(ybuf.at[:, 0], zbuf.at[1], z_send.at[0], z_recv.at[0], at(-1, 0)),
            remote(ybuf.at[:, planes - 1], zbuf.at[0], z_send.at[1], z_recv.at[1], at(1, 0)),
        ]

    def with_strips(p):
        whole = rhs[p + 2]
        low = whole[:, 0:8] + ybuf[0, p] * inner_low
        high = whole[:, ROWS - 8 : ROWS] + ybuf[1, p] * inner_high
        return jnp.concatenate([low, whole[:, 8 : ROWS - 8], high], axis=1)

    def stage(g):
        for side, base in ((1, 0), (0, planes - 6)):
            first, count = RUNS[g][1 - side]
            for p in range(first, first + count):
                staged[side, p - base] = with_strips(p)

    for copy in y_copies(0) + x_copies(0) + y_copies(1):
        copy.start()
    for n in range(8):
        sums[n] = pltpu.roll(acted[...], 128 - 2 * (n + 1), 1)
    for copy in replies:
        copy.start()
    for g in range(2, X_RUNS + 1):
        for copy in y_copies(g):
            copy.start()
    for copy in y_copies(0):
        copy.wait()
    for copy in corner_copies():
        copy.start()
    for copy in y_copies(1):
        copy.wait()
    stage(1)
    for copy in x_copies(1):
        copy.start()
    sphere_step_one()
    for g in range(2, X_RUNS):
        for copy in y_copies(g):
            copy.wait()
        stage(g)
        for copy in x_copies(g):
            copy.start()
    for copy in y_copies(X_RUNS):
        copy.wait()
    inside, scale = wall_masks(gy, n_gy, span_y, rhs.shape[3])
    plane = rhs.shape[1:]
    stages = (level_0, level_1, level_2, level_3)
    first, last = 6, planes - 3

    def begin(x, _):
        level_0[x] = (with_strips(x - 2).reshape(inside.shape) * inside).reshape(plane)
        return 0

    lax.fori_loop(first, last + 1, begin, 0)

    def swept(k, x):
        source = stages[k - 1]
        return relaxed(level_0[x], source[x - 1], source[x], source[x + 1], scale)

    def finish(x):
        result = swept(ITERS, x)
        for c in range(3):
            done[c, x - HALO - 1] = result[c, HALO : HALO + span_y, :]

    for k in range(1, ITERS):

        def step(s, _, k=k):
            for u in range(2):
                x = first + k + 2 * s + u
                stages[k][x] = swept(k, x)
            return 0

        lax.fori_loop(0, (last - first + 1 - 2 * k) // 2, step, 0)
    for x in range(first + ITERS, last - ITERS + 1):
        finish(x)

    for g in range(X_RUNS - 1):
        for copy in x_copies(g) + (corner_copies() if g == 0 else []):
            copy.wait()
        (low, count), _ = RUNS[g]
        left = list(range(5 - low - count + 1, 5 - low + 1))
        right = list(range(planes - 2 + low, planes - 2 + low + count))
        for x, beside in [(x, xbuf[0, x]) for x in left] + [
            (x, xbuf[1, x - planes + 2]) for x in right
        ]:
            if g == 0:
                side = 0 if x < planes // 2 else 1
                low_rows = beside[:, 0:8] + zbuf[side, 0] * inner_low
                high_rows = beside[:, ROWS - 8 : ROWS] + zbuf[side, 1] * inner_high
                beside = jnp.concatenate(
                    [low_rows, beside[:, 8 : ROWS - 8], high_rows], axis=1
                )
            whole = beside + (with_strips(x - 2) if 2 <= x < planes + 2 else rhs[x])
            level_0[x] = (whole.reshape(inside.shape) * inside).reshape(plane)
        for k in range(1, ITERS):
            for x in [x + k for x in left] + [x - k for x in right]:
                stages[k][x] = swept(k, x)
        for x in [x + ITERS for x in left] + [x - ITERS for x in right]:
            finish(x)
        if g == 0:
            sphere_step_two()
        if g == 1:
            sphere_step_three()
    for copy in x_copies(X_RUNS - 1):
        copy.wait()


def relax_kernel(
    n_gy, rhs, xbuf, level_0, level_1, level_2, level_3, done, nm_in, out_ref, nm_ref, staged, sems
):
    gy = lax.axis_index("gy")
    top = level_0.shape[0] - 1
    span_x = top + 1 - 2 * HALO
    span_y = out_ref.shape[2]
    copies = [
        pltpu.make_async_copy(done, out_ref.at[:, 1 : span_x - 1], sems.at[0]),
        pltpu.make_async_copy(nm_in, nm_ref, sems.at[1]),
    ]
    for copy in copies:
        copy.start()
    inside, scale = wall_masks(gy, n_gy, span_y, rhs.shape[3])
    plane = rhs.shape[1:]
    stages = (level_0, level_1, level_2, level_3)
    for side, (edge, inward) in enumerate(((0, 1), (top, -1))):
        whole = rhs[edge] + xbuf[side, 0 if side == 0 else 5]
        outer = (whole.reshape(inside.shape) * inside).reshape(plane)
        for k in range(1, ITERS + 1):
            x = edge + inward * k
            source = stages[k - 1]
            outer = relaxed(level_0[x], outer, source[x], source[x + inward], scale)
        x = 0 if side == 0 else span_x - 1
        for c in range(3):
            staged[side, c, 0] = outer[c, HALO : HALO + span_y, :]
        copies.append(
            pltpu.make_async_copy(staged.at[side], out_ref.at[:, x : x + 1], sems.at[2 + side])
        )
        copies[-1].start()
    for copy in copies:
        copy.wait()


def on_device(
    n_gx,
    n_gy,
    velocity,
    owner_block,
    base_x,
    base_y,
    base_z,
    delta_weights,
    marker_offset,
    sphere_motion,
    contact_sphere,
    contact_partner,
):
    span_x, span_y, extent_z = velocity.shape[1:]
    markers = base_x.shape[0]
    planes = span_x + 4
    every = markers // TILE + 8
    padded = planes + WINDOW - 1
    grown = (padded + 2, 3, ROWS, extent_z)
    vmem = pl.BlockSpec(memory_space=pltpu.VMEM)
    smem = pl.BlockSpec(memory_space=pltpu.SMEM)
    hbm = pl.BlockSpec(memory_space=pltpu.HBM)
    dma = pltpu.SemaphoreType.DMA
    motion = sphere_motion.T
    fhl, started, home, arrived = pl.pallas_call(
        functools.partial(request_kernel, n_gx, n_gy),
        out_shape=(
            jax.ShapeDtypeStruct((padded, 3 * ROWS, 2 * extent_z), BF16),
            jax.ShapeDtypeStruct(grown, F32),
            jax.ShapeDtypeStruct((32, markers), F32),
            jax.ShapeDtypeStruct((8, 24, TILE), F32),
        ),
        in_specs=[hbm] * 8,
        out_specs=(vmem,) * 4,
        scratch_shapes=[
            pltpu.VMEM(velocity.shape, F32),
            pltpu.VMEM((1, markers), I32),
            pltpu.VMEM((1, markers), I32),
            pltpu.VMEM((1, markers), I32),
            pltpu.VMEM((1, markers), I32),
            pltpu.VMEM((12, markers), F32),
            pltpu.VMEM((3, markers), F32),
            pltpu.SMEM((2, 6), F32),
            pltpu.VMEM((2, 3, 2, span_y, extent_z), F32),
            pltpu.VMEM((2, 3, 2 * span_x, extent_z), F32),
            pltpu.VMEM((4, 16, extent_z), F32),
            pltpu.VMEM((4, 16, extent_z), F32),
            pltpu.VMEM((2, 3, 2 * span_x, extent_z), F32),
            pltpu.VMEM((32, markers), F32),
            pltpu.VMEM((96, markers), BF16),
            pltpu.VMEM((8, TILE), F32),
            pltpu.VMEM((8, 24, TILE), F32),
            pltpu.VMEM((8, 24, TILE), F32),
            pltpu.VMEM((planes, 3, ROWS, extent_z), F32),
            dma((8,)),
            dma((8,)),
            dma((8,)),
            dma((8,)),
            dma((8,)),
        ],
        compiler_params=pltpu.CompilerParams(
            collective_id=0, has_side_effects=True, vmem_limit_bytes=24 << 20
        ),
        name="requests",
    )(
        *(
            pltpu.with_memory_space_constraint(array, pltpu.HBM)
            for array in (
                velocity,
                owner_block.reshape(1, markers),
                base_x.reshape(1, markers),
                base_y.reshape(1, markers),
                base_z.reshape(1, markers),
                delta_weights,
                marker_offset,
                motion,
            )
        )
    )
    rhs, acted = pl.pallas_call(
        marker_kernel,
        out_shape=(
            jax.ShapeDtypeStruct(grown, F32),
            jax.ShapeDtypeStruct((8, 128), F32),
        ),
        in_specs=[vmem] * 4,
        out_specs=(vmem,) * 2,
        scratch_shapes=[
            pltpu.VMEM((every, 96, TILE), BF16),
            pltpu.VMEM((every * BINS, TILE), F32),
            pltpu.VMEM((every * BINS, TILE), F32),
            pltpu.VMEM((every, TILE), F32),
            pltpu.VMEM((2, extent_z, TILE), BF16),
            pltpu.VMEM((2, 32, TILE), F32),
            pltpu.VMEM((8, 128), I32),
            pltpu.SMEM((8, 128), I32),
            dma,
        ],
        compiler_params=pltpu.CompilerParams(vmem_limit_bytes=24 << 20),
        name="markers",
    )(fhl, started, home, arrived)
    plane = (3, ROWS, extent_z)
    new_motion, *strips = pl.pallas_call(
        functools.partial(strip_kernel, n_gx, n_gy, markers // 2),
        out_shape=(
            jax.ShapeDtypeStruct(motion.shape, F32),
            jax.ShapeDtypeStruct((2, 6, 3, ROWS, extent_z), F32),
        )
        + (jax.ShapeDtypeStruct((planes + 4,) + plane, F32),) * 4
        + (jax.ShapeDtypeStruct((3, span_x - 2, span_y, extent_z), F32),),
        in_specs=[vmem] * 2 + [smem] * 3,
        out_specs=(vmem,) * 7,
        scratch_shapes=[
            pltpu.VMEM((2, planes, 3, 8, extent_z), F32),
            pltpu.VMEM((2, 2, 3, 8, extent_z), F32),
            pltpu.VMEM((8, 8, 128), F32),
            pltpu.VMEM((8, 8, 128), F32),
            pltpu.VMEM((n_gx, 1, 128), F32),
            pltpu.VMEM((n_gy, 1, 128), F32),
            pltpu.VMEM((2, 1, 128), F32),
            pltpu.VMEM((8, 128), F32),
            pltpu.VMEM((2, 6, 3, ROWS, extent_z), F32),
            dma((8,)),
            dma((8,)),
            dma((n_gx,)),
            dma((n_gx,)),
            dma((n_gy,)),
            dma((n_gy,)),
            dma((4 * len(RUNS),)),
            dma((4 * len(RUNS),)),
            dma((2 * X_RUNS,)),
            dma((2 * X_RUNS,)),
            dma((2,)),
            dma((2,)),
        ],
        compiler_params=pltpu.CompilerParams(
            collective_id=1, has_side_effects=True, vmem_limit_bytes=24 << 20
        ),
        name="strips",
    )(rhs, acted, motion, contact_sphere, contact_partner)
    velocity_star, new_motion = pl.pallas_call(
        functools.partial(relax_kernel, n_gy),
        out_shape=(
            jax.ShapeDtypeStruct(velocity.shape, F32),
            jax.ShapeDtypeStruct(motion.shape, F32),
        ),
        in_specs=[vmem] * 8,
        out_specs=(hbm, hbm),
        scratch_shapes=[
            pltpu.VMEM((2, 3, 1, span_y, extent_z), F32),
            dma((4,)),
        ],
        compiler_params=pltpu.CompilerParams(vmem_limit_bytes=24 << 20),
        name="relax",
    )(rhs, *strips, new_motion)
    return velocity_star, new_motion.T


def solution(mesh):
    placed = (
        P(None, "gx", "gy", None),
        P(("gx", "gy"), None),
        P(("gx", "gy")),
        P(("gx", "gy")),
        P(("gx", "gy")),
        P(None, ("gx", "gy")),
        P(None, ("gx", "gy")),
        P(None, ("gx", "gy")),
        P(("gx", "gy")),
        P(("gx", "gy")),
    )
    return jax.shard_map(
        functools.partial(on_device, mesh.shape["gx"], mesh.shape["gy"]),
        mesh=mesh,
        in_specs=placed,
        out_specs=(P(None, "gx", "gy", None), P(None, ("gx", "gy"))),
        check_vma=False,
    )
```

```python
import functools

import jax
import jax.numpy as jnp
from jax import lax
from jax.experimental import pallas as pl
from jax.experimental.pallas import tpu as pltpu
from jax.sharding import PartitionSpec as P

F32 = jnp.float32
BF16 = jnp.bfloat16
I32 = jnp.int32
MESH = pl.DeviceIdType.MESH

ITERS = 4
DIFFUSION = 1.0
RESPONSE = 0.5
DASHPOT = 0.1

TILE = 256
BINS = 32
WINDOW = 6
ROWS = 40
HALO = 4
LANES = [(dx, dy) for dx in (-1, 0, 1) for dy in (-1, 0, 1) if (dx, dy) != (0, 0)]
DIAGONALS = [(dx, dy) for dx, dy in LANES if dx * dy != 0]
RUNS = [
    ((0, 1), (19, 1)),
    ((1, 2), (17, 2)),
    ((3, 2), (15, 2)),
    ((5, 1), (14, 1)),
    ((6, 8),),
]
X_RUNS = len(RUNS) - 1


def split(values):
    high = values.astype(BF16)
    low = (values - high.astype(F32)).astype(BF16)
    return high, low


def pick(distance, weights):
    result = jnp.where(distance == 3, weights[3], 0.0)
    for k in (2, 1, 0):
        result = jnp.where(distance == k, weights[k], result)
    return result


def cross(a, b):
    return (
        a[1] * b[2] - a[2] * b[1],
        a[2] * b[0] - a[0] * b[2],
        a[0] * b[1] - a[1] * b[0],
    )


def remote(src, dst, send, recv, peer):
    return pltpu.make_async_remote_copy(
        src_ref=src,
        dst_ref=dst,
        send_sem=send,
        recv_sem=recv,
        device_id=peer,
        device_id_type=MESH,
    )


def wait_all(whole, send, recv, at):
    copy = remote(whole, whole, send, recv, at(1, 0))
    copy.wait()


def greet(peers):
    barrier = pltpu.get_barrier_semaphore()
    for peer in peers:
        pl.semaphore_signal(barrier, inc=1, device_id=peer, device_id_type=MESH)
    return barrier


def neighbours(n_gx, n_gy):
    gx = lax.axis_index("gx")
    gy = lax.axis_index("gy")

    def at(dx, dy):
        return (lax.rem(gx + (dx + n_gx), n_gx), lax.rem(gy + (dy + n_gy), n_gy))

    return gx, gy, at


def terms(values):
    parts = []
    rest = values
    for _ in range(3):
        part = rest.astype(BF16)
        parts.append(part)
        rest = rest - part.astype(F32)
    return jnp.concatenate(parts, axis=0)


def chosen_columns(parts, slots, first):
    wanted = lax.broadcasted_iota(I32, (TILE, TILE), 0).astype(F32) + first
    hit = jnp.where(wanted == slots, 1.0, 0.0).astype(BF16)
    return lax.dot_general(parts, hit, (((1,), (1,)), ((), ())), preferred_element_type=F32)


def ranks(hits, above):
    return jnp.dot(hits.astype(BF16), above, preferred_element_type=F32)


def strictly_above(size):
    return (
        lax.broadcasted_iota(I32, (size, size), 0) < lax.broadcasted_iota(I32, (size, size), 1)
    ).astype(BF16)


def request_kernel(
    n_gx,
    n_gy,
    v_hbm,
    own_hbm,
    bx_hbm,
    by_hbm,
    bz_hbm,
    dw_hbm,
    off_hbm,
    mot_hbm,
    fhl,
    rhs,
    home,
    arrived,
    v_ref,
    own_ref,
    bx_ref,
    by_ref,
    bz_ref,
    dw_ref,
    off_ref,
    mot_ref,
    hx,
    hy,
    hc,
    corner,
    edges,
    pay,
    pay3,
    slot_s,
    snd,
    inbox,
    frame,
    in_sem,
    halo_send,
    halo_recv,
    pay_send,
    pay_recv,
):
    gx, gy, at = neighbours(n_gx, n_gy)
    here = gx * n_gy + gy
    barrier = greet([at(dx, dy) for dx, dy in LANES])
    loads = [
        pltpu.make_async_copy(src, dst, in_sem.at[i])
        for i, (src, dst) in enumerate(
            (
                (v_hbm, v_ref),
                (own_hbm, own_ref),
                (bx_hbm, bx_ref),
                (by_hbm, by_ref),
                (bz_hbm, bz_ref),
                (dw_hbm, dw_ref),
                (off_hbm, off_ref),
                (mot_hbm, mot_ref),
            )
        )
    ]
    for copy in loads:
        copy.start()
    markers = dw_ref.shape[1]
    chunks = markers // TILE
    span_x = v_ref.shape[1]
    span_y = v_ref.shape[2]
    extent_z = v_ref.shape[3]
    planes = span_x + 4
    for copy in loads:
        copy.wait()

    last = span_x - 2
    pl.semaphore_wait(barrier, len(LANES))
    halo = []
    halo.append(remote(v_ref.at[:, 0:2], hx.at[1], halo_send.at[0], halo_recv.at[0], at(-1, 0)))
    halo.append(
        remote(v_ref.at[:, last:span_x], hx.at[0], halo_send.at[1], halo_recv.at[1], at(1, 0))
    )
    halo.append(remote(edges.at[0], hy.at[1], halo_send.at[2], halo_recv.at[2], at(0, -1)))
    halo.append(remote(edges.at[1], hy.at[0], halo_send.at[3], halo_recv.at[3], at(0, 1)))
    for k, (dx, dy) in enumerate(DIAGONALS):
        slot = (1 if dx < 0 else 0) * 2 + (1 if dy < 0 else 0)
        halo.append(
            remote(
                corner.at[k], hc.at[slot], halo_send.at[4 + k], halo_recv.at[4 + k], at(dx, dy)
            )
        )
    corner[...] = jnp.zeros_like(corner)
    for k, (dx, dy) in enumerate(DIAGONALS):
        x0 = 0 if dx < 0 else last
        y0 = 0 if dy < 0 else span_y - 2
        for c in range(3):
            for i in range(2):
                row = 4 * c + 2 * i
                corner[k, row : row + 2, :] = v_ref[c, x0 + i, y0 : y0 + 2, :]
    for copy in halo[4:] + halo[0:2]:
        copy.start()
    for side, y0 in enumerate((0, span_y - 2)):
        for c in range(3):
            for x in range(span_x):
                edges[side, c, 2 * x : 2 * x + 2, :] = v_ref[c, x, y0 : y0 + 2, :]
    for copy in halo[2:4]:
        copy.start()

    pay[0:12, :] = dw_ref[...]
    pay[12:13, :] = bx_ref[...].astype(F32)
    pay[13:14, :] = by_ref[...].astype(F32)
    pay[14:15, :] = bz_ref[...].astype(F32)
    per_sphere = markers // 2
    second = (lax.broadcasted_iota(I32, (1, markers), 1) >= per_sphere).astype(F32)
    pay[15:16, :] = second
    motion = [mot_ref[0, c] * (1.0 - second) + mot_ref[1, c] * second for c in range(6)]
    offset = [off_ref[c : c + 1, :] for c in range(3)]
    swing = cross(motion[3:6], offset)
    for c in range(3):
        pay[16 + c : 17 + c, :] = motion[c] + swing[c]
        pay[19 + c : 20 + c, :] = offset[c]
    pay[22:23, :] = jnp.ones((1, markers), F32)
    pay[23:32, :] = jnp.zeros((9, markers), F32)
    whole = pay[...]
    pay3[...] = terms(whole)
    home[...] = whole
    home[22:23, :] = (own_ref[...] == here).astype(F32)

    above = strictly_above(TILE)
    bins = lax.broadcasted_iota(I32, (8, TILE), 0)
    carry = jnp.zeros((8, 1), F32)
    for q in range(chunks):
        owner = own_ref[:, q * TILE : (q + 1) * TILE]
        owner_x = lax.shift_right_logical(owner, n_gy.bit_length() - 1)
        owner_y = owner & (n_gy - 1)
        step_x = (owner_x - gx + 1) & (n_gx - 1)
        lane = step_x * 3 + (owner_y - gy + 1)
        lane = jnp.where(owner == here, -1, jnp.where(lane > 4, lane - 1, lane))
        hits = jnp.where(bins == lane, 1.0, 0.0)
        ranked = ranks(hits, above) + carry + bins.astype(F32) * TILE
        carry = carry + jnp.sum(hits, axis=1, keepdims=True)
        slot = jnp.sum(hits * ranked, axis=0, keepdims=True)
        slot_s[q : q + 1, :] = jnp.where(lane < 0, -1.0, slot)

    def compact(n, _):
        first = (n * TILE).astype(F32)
        moved = None
        for q in range(chunks):
            part = chosen_columns(
                pay3[:, q * TILE : (q + 1) * TILE], slot_s[q : q + 1, :], first
            )
            moved = part if moved is None else moved + part
        snd[n] = moved[0:24] + moved[32:56] + moved[64:88]
        return 0

    lax.fori_loop(0, 8, compact, 0)

    requests = [
        remote(snd.at[n], inbox.at[n], pay_send.at[0], pay_recv.at[0], at(dx, dy))
        for n, (dx, dy) in enumerate(LANES)
    ]
    for copy in requests:
        copy.start()

    inner_low = jnp.where(gy > 0, 1.0, 0.0).astype(F32)
    inner_high = jnp.where(gy < n_gy - 1, 1.0, 0.0).astype(F32)

    def clear(p, _):
        rhs[p] = jnp.zeros((3, ROWS, extent_z), F32)
        return 0

    lax.fori_loop(0, rhs.shape[0], clear, 0)

    def clear_frame(p, _):
        frame[p] = jnp.zeros((3, ROWS, extent_z), F32)
        return 0

    lax.fori_loop(0, planes, clear_frame, 0)

    def clear_beyond(p, _):
        fhl[p] = jnp.zeros((3 * ROWS, 2 * extent_z), BF16)
        return 0

    lax.fori_loop(planes, fhl.shape[0], clear_beyond, 0)

    def place(x, _):
        for c in range(3):
            plane = v_ref[c, x]
            frame[x + 2, c, 4 : 4 + span_y, :] = plane
            rhs[x + 4, c, 4 : 4 + span_y, :] = plane
        return 0

    lax.fori_loop(0, span_x, place, 0)
    for copy in halo:
        copy.wait()

    for x in range(span_x):
        for c in range(3):
            frame[x + 2, c, 2:4, :] = hy[0, c, 2 * x : 2 * x + 2, :] * inner_low
            frame[x + 2, c, 36:38, :] = hy[1, c, 2 * x : 2 * x + 2, :] * inner_high
    for side in range(2):
        for i in range(2):
            p = (0 if side == 0 else planes - 2) + i
            for c in range(3):
                frame[p, c, 4 : 4 + span_y, :] = hx[side, c, i]
                frame[p, c, 2:4, :] = hc[side * 2, 4 * c + 2 * i : 4 * c + 2 * i + 2, :] * inner_low
                frame[p, c, 36:38, :] = (
                    hc[side * 2 + 1, 4 * c + 2 * i : 4 * c + 2 * i + 2, :] * inner_high
                )

    def halve(p, _):
        high, low = split(frame[p].reshape(3 * ROWS, extent_z))
        fhl[p, :, 0:extent_z] = high
        fhl[p, :, extent_z : 2 * extent_z] = low
        return 0

    lax.fori_loop(0, planes, halve, 0)
    wait_all(inbox, pay_send.at[0], pay_recv.at[0], at)
    arrived[...] = inbox[...]


def marker_kernel(
    fhl,
    rhs_in,
    home,
    arrived,
    rhs,
    acted,
    pay3,
    hit_s,
    rank_s,
    slot_s,
    tz,
    held,
    edge_v,
    edge,
    edge_sem,
):
    chunks = home.shape[1] // TILE
    every = chunks + 8
    extent_z = rhs.shape[3]
    bins = lax.broadcasted_iota(I32, (BINS, TILE), 0).astype(F32)

    def chunk(q):
        return home[0:24, q * TILE : (q + 1) * TILE] if q < chunks else arrived[q - chunks]

    totals = []
    for q in range(every):
        m = chunk(q)
        hits = jnp.where((bins == m[12:13]) & (m[22:23] > 0.5), 1.0, 0.0)
        hit_s[q * BINS : (q + 1) * BINS, :] = hits
        totals.append(jnp.sum(hits, axis=1, keepdims=True))
    rank_s[...] = ranks(hit_s[...], strictly_above(TILE))
    carries = []
    count = jnp.zeros((BINS, 1), F32)
    for q in range(every):
        carries.append(count)
        count = count + totals[q]
    count = jnp.broadcast_to(count, (BINS, 128))
    high, low = split(count)
    below = (
        lax.broadcasted_iota(I32, (BINS, BINS), 0) > lax.broadcasted_iota(I32, (BINS, BINS), 1)
    ).astype(BF16)
    start = jnp.dot(below, high, preferred_element_type=F32)
    start = start + jnp.dot(below, low, preferred_element_type=F32)
    opening = lax.broadcasted_iota(I32, (BINS, 128), 1).astype(F32) * TILE
    present = jnp.sum(count, axis=0, keepdims=True)
    closing = jnp.minimum(opening + TILE, present)
    first_bin = jnp.sum(jnp.where(start + count <= opening, 1.0, 0.0), axis=0, keepdims=True)
    last_bin = jnp.sum(jnp.where(start < closing, 1.0, 0.0), axis=0, keepdims=True) - 1.0
    edge_v[...] = jnp.concatenate(
        [first_bin, last_bin, present, jnp.zeros((5, 128), F32)], axis=0
    ).astype(I32)
    to_scalars = pltpu.make_async_copy(edge_v, edge, edge_sem)
    to_scalars.start()
    start = start[:, 0:1]
    for q in range(every):
        hits = hit_s[q * BINS : (q + 1) * BINS, :]
        ranked = rank_s[q * BINS : (q + 1) * BINS, :] + (carries[q] + start)
        slot = jnp.sum(hits * ranked, axis=0, keepdims=True)
        there = jnp.sum(hits, axis=0, keepdims=True)
        slot_s[q : q + 1, :] = jnp.where(there > 0.5, slot, -1.0)
        m = chunk(q)
        if q < chunks:
            source = jnp.zeros((1, TILE), F32)
        else:
            source = jnp.full((1, TILE), float(q - chunks + 1), F32)
        filled = jnp.concatenate([m[0:23], source, jnp.zeros((8, TILE), F32)], axis=0)
        pay3[q] = terms(filled)
    acted[...] = jnp.zeros_like(acted)

    def start_from(p, _):
        rhs[p] = rhs_in[p]
        return 0

    lax.fori_loop(0, rhs.shape[0], start_from, 0)
    slot_id = lax.broadcasted_iota(I32, (TILE, TILE), 0).astype(F32)

    def gather(n):
        wanted = slot_id + (n * TILE).astype(F32)
        moved = None
        for q in range(every):
            hit = jnp.where(wanted == slot_s[q : q + 1, :], 1.0, 0.0).astype(BF16)
            part = lax.dot_general(
                hit, pay3[q], (((1,), (1,)), ((), ())), preferred_element_type=F32
            )
            moved = part if moved is None else moved + part
        moved = jnp.concatenate([moved, jnp.zeros((TILE, 32), F32)], axis=1).T
        return moved[0:32] + moved[32:64] + moved[64:96]

    def prepare(m):
        cell_y = m[13:14].astype(I32)
        cell_z = m[14:15].astype(I32)
        z = lax.broadcasted_iota(I32, (extent_z, TILE), 0)
        table = pick((z - cell_z) & (extent_z - 1), [m[8 + i : 9 + i] for i in range(4)])
        high, low = split(table)
        y = lax.broadcasted_iota(I32, (ROWS, TILE), 0) - 2
        table_y = pick(y - cell_y, [m[4 + i : 5 + i] for i in range(4)])
        return high, low, table_y

    def x_table(m, plane):
        x = lax.broadcasted_iota(I32, (8, TILE), 0)
        return pick(x + plane - m[12:13].astype(I32), [m[i : i + 1] for i in range(4)])

    def sample(m, plane, high, low, table_y, totals):
        table_x = x_table(m, plane)
        folded_y = table_y.reshape(ROWS // 8, 8, TILE)
        both = fhl[pl.ds(plane, WINDOW)].reshape(WINDOW * 3 * ROWS, 2 * extent_z)
        left = jnp.concatenate([both, both[:, 0:extent_z]], axis=1)
        right = jnp.concatenate([high, high, low], axis=0)
        part = jnp.dot(left, right, preferred_element_type=F32)
        part = part.reshape(WINDOW, 3, ROWS // 8, 8, TILE)
        result = []
        for c in range(3):
            total = totals[c]
            for p in range(WINDOW):
                total = total + jnp.sum(part[p, c] * folded_y, axis=0) * table_x[p : p + 1]
            result.append(total)
        return tuple(result)

    def act(m, totals):
        totals = [jnp.sum(total, axis=0, keepdims=True) for total in totals]
        force = [m[16 + c : 17 + c] - totals[c] for c in range(3)]
        torque = cross([m[19 + c : 20 + c] for c in range(3)], force)
        acting = jnp.concatenate(force + list(torque) + [jnp.zeros((2, TILE), F32)], axis=0)
        group = m[23:24] * 2.0 + m[15:16]
        member = (
            (lax.broadcasted_iota(I32, (128, TILE), 0).astype(F32) == group)
            & (m[22:23] > 0.5)
        ).astype(F32)
        summed = lax.dot_general(
            terms(acting),
            member.astype(BF16),
            (((1,), (1,)), ((), ())),
            preferred_element_type=F32,
        )
        acted[...] += summed[0:8] + summed[8:16] + summed[16:24]
        return force

    def deposit(m, plane, force, z_high, z_low, table_y):
        table_x = x_table(m, plane)
        rows = []
        for p in range(WINDOW):
            for c in range(3):
                rows.append((force[c] * table_x[p : p + 1]) * table_y)
        high, low = split(jnp.concatenate(rows, axis=0))
        left = jnp.concatenate([high, low, high], axis=1)
        right = jnp.concatenate([z_high, z_high, z_low], axis=1)
        added = lax.dot_general(
            left, right, (((1,), (1,)), ((), ())), preferred_element_type=F32
        )
        rhs[pl.ds(plane + 2, WINDOW)] += added.reshape(WINDOW, 3, ROWS, extent_z)

    held[0] = gather(jnp.int32(0))
    to_scalars.wait()
    tiles = lax.shift_right_logical(edge[2, 0] + (TILE - 1), TILE.bit_length() - 1)
    nothing = (jnp.zeros((8, TILE), F32),) * 3

    def work(n, _):
        low_plane = edge[0, n]
        spans = (edge[1, n] + 3 - low_plane + WINDOW) // WINDOW
        slot = n & 1

        @pl.when(spans <= 1)
        def _narrow():
            m = held[slot]
            high, low, table_y = prepare(m)
            totals = sample(m, low_plane, high, low, table_y, nothing)
            following = gather(n + 1)
            force = act(m, totals)
            deposit(m, low_plane, force, high, low, table_y)
            held[1 - slot] = following

        @pl.when(spans > 1)
        def _wide():
            m = held[slot]
            high, low, table_y = prepare(m)
            tz[0] = high
            tz[1] = low

            def sample_span(j, totals):
                plane = low_plane + j * WINDOW
                return sample(held[slot], plane, tz[0], tz[1], table_y, totals)

            force = act(m, lax.fori_loop(0, spans, sample_span, nothing))

            def deposit_span(j, _):
                plane = low_plane + j * WINDOW
                deposit(held[slot], plane, force, tz[0], tz[1], table_y)
                return 0

            lax.fori_loop(0, spans, deposit_span, 0)
            held[1 - slot] = gather(n + 1)

        return 0

    lax.fori_loop(0, tiles, work, 0)


def wall_masks(gy, n_gy, span_y, extent_z):
    y = lax.broadcasted_iota(I32, (ROWS, extent_z), 0)
    low_edge = jnp.where(gy > 0, 0, HALO)
    high_edge = jnp.where(gy < n_gy - 1, ROWS, HALO + span_y)
    inside = jnp.where((y >= low_edge) & (y < high_edge), 1.0, 0.0).astype(F32)
    inside = jnp.concatenate([inside] * 3, axis=0)
    return inside, inside * (1.0 / (1.0 + 6.0 * DIFFUSION))


def relaxed(rhs, before, centre, after, scale):
    shape = rhs.shape
    flat = scale.shape
    centre = centre.reshape(flat)
    total = rhs.reshape(flat) + before.reshape(flat) + after.reshape(flat)
    total = total + pltpu.roll(centre, 1, 0) + pltpu.roll(centre, flat[0] - 1, 0)
    total = total + pltpu.roll(centre, 1, 1) + pltpu.roll(centre, flat[1] - 1, 1)
    return (total * scale).reshape(shape)


def strip_kernel(
    n_gx,
    n_gy,
    per_sphere,
    rhs,
    acted,
    mot_ref,
    cs_ref,
    cp_ref,
    nm_ref,
    xbuf,
    level_0,
    level_1,
    level_2,
    level_3,
    done,
    ybuf,
    zbuf,
    sums,
    ret,
    agx,
    agy,
    ag1,
    moved_s,
    staged,
    ret_send,
    ret_recv,
    agx_send,
    agx_recv,
    agy_send,
    agy_recv,
    y_send,
    y_recv,
    x_send,
    x_recv,
    z_send,
    z_recv,
):
    gx, gy, at = neighbours(n_gx, n_gy)
    here = gx * n_gy + gy
    planes = ybuf.shape[1]
    span_y = done.shape[2]
    peers = (
        [at(k, 0) for k in range(1, n_gx)]
        + [at(0, k) for k in range(1, n_gy)]
        + [at(dx, dy) for dx in (-1, 1) for dy in (-1, 1)]
    )
    barrier = greet(peers)
    inner_low = jnp.where(gy > 0, 1.0, 0.0).astype(F32)
    inner_high = jnp.where(gy < n_gy - 1, 1.0, 0.0).astype(F32)
    replies = [
        remote(sums.at[n], ret.at[n], ret_send.at[0], ret_recv.at[0], at(-dx, -dy))
        for n, (dx, dy) in enumerate(LANES)
    ]
    lanes = lax.broadcasted_iota(I32, (8, 128), 1)
    row_id = lax.broadcasted_iota(I32, (8, 128), 0)
    pl.semaphore_wait(barrier, len(peers))

    def along_x(k):
        return remote(ag1.at[0], agx.at[k], agx_send.at[0], agx_recv.at[0], at(k, 0))

    def along_y(k):
        return remote(ag1.at[1], agy.at[k], agy_send.at[0], agy_recv.at[0], at(0, k))

    def sphere_step_one():
        wait_all(ret, ret_send.at[0], ret_recv.at[0], at)
        total = acted[...]
        for n in range(8):
            total = total + ret[n]
        start = jnp.zeros((8, 128), F32)
        for c in range(6):
            for s in range(2):
                start = jnp.where((row_id == c) & (lanes == s), mot_ref[s, c], start)
        moved = start - total * (RESPONSE / per_sphere)
        moved_s[...] = moved
        lane = lanes[0:1]
        message = jnp.zeros((1, 128), F32)
        for sphere in range(2):
            for c in range(3):
                message = jnp.where(
                    lane == 3 * sphere + c, moved[c : c + 1, sphere : sphere + 1], message
                )
        ag1[0] = message
        for k in range(1, n_gx):
            along_x(k).start()

    def sphere_step_two():
        wait_all(agx.at[pl.ds(1, n_gx - 1)], agx_send.at[0], agx_recv.at[0], at)
        total = ag1[0]
        for k in range(1, n_gx):
            total = total + pltpu.roll(agx[k], 6 * k, 1)
        ag1[1] = total
        for k in range(1, n_gy):
            along_y(k).start()

    def sphere_step_three():
        wait_all(agy.at[pl.ds(1, n_gy - 1)], agy_send.at[0], agy_recv.at[0], at)
        table = jnp.concatenate([ag1[1]] + [agy[k] for k in range(1, n_gy)], axis=0)
        moved = moved_s[...]
        pull = jnp.zeros((8, 128), F32)
        for k in range(cs_ref.shape[0]):
            partner = cp_ref[k]
            own = cs_ref[k] - 2 * here
            holder = lax.shift_right_logical(partner, 1)
            holder_x = lax.shift_right_logical(holder, n_gy.bit_length() - 1)
            row = (gy - (holder & (n_gy - 1)) + n_gy) & (n_gy - 1)
            lane = 6 * ((gx - holder_x + n_gx) & (n_gx - 1)) + 3 * (partner & 1)
            mine = jnp.where(row_id == row, table, 0.0)
            for c in range(3):
                chosen = jnp.sum(
                    jnp.where(lanes == lane + c, mine, 0.0), axis=(0, 1), keepdims=True
                )
                pull = pull + jnp.where((lanes == own) & (row_id == c), chosen - moved, 0.0)
        settled = jnp.concatenate(
            [moved + DASHPOT * pull, jnp.zeros((120, 128), F32)], axis=0
        )
        nm_ref[...] = settled.T[0:2, 0:6]

    def y_copies(g):
        copies = []
        for first, count in RUNS[g]:
            lo = first + 2
            copies.append(
                remote(
                    rhs.at[pl.ds(lo, count), :, pl.ds(0, 8)],
                    ybuf.at[1, pl.ds(first, count)],
                    y_send.at[g],
                    y_recv.at[g],
                    at(0, -1),
                )
            )
            copies.append(
                remote(
                    rhs.at[pl.ds(lo, count), :, pl.ds(ROWS - 8, 8)],
                    ybuf.at[0, pl.ds(first, count)],
                    y_send.at[g],
                    y_recv.at[g],
                    at(0, 1),
                )
            )
        return copies

    def wait_y(g):
        planes_in = sum(count for _, count in RUNS[g])
        wait_all(ybuf.at[:, pl.ds(0, planes_in)], y_send.at[g], y_recv.at[g], at)

    def x_copies(g):
        (low, count), (high, _) = RUNS[g]
        to_low, to_high = staged.at[1, pl.ds(low, count)], rhs.at[pl.ds(high + 2, count)]
        if g == 0:
            to_low = rhs.at[pl.ds(low + 2, count)]
        high = high - (planes - 6)
        if g > 0:
            to_high = staged.at[0, pl.ds(high, count)]
        return [
            remote(
                to_low,
                xbuf.at[1, pl.ds(low, count)],
                x_send.at[2 * g],
                x_recv.at[2 * g],
                at(-1, 0),
            ),
            remote(
                to_high,
                xbuf.at[0, pl.ds(high, count)],
                x_send.at[2 * g + 1],
                x_recv.at[2 * g + 1],
                at(1, 0),
            ),
        ]

    def corner_copies():
        return [
            remote(ybuf.at[:, 0], zbuf.at[1], z_send.at[0], z_recv.at[0], at(-1, 0)),
            remote(ybuf.at[:, planes - 1], zbuf.at[0], z_send.at[1], z_recv.at[1], at(1, 0)),
        ]

    def with_strips(p):
        whole = rhs[p + 2]
        low = whole[:, 0:8] + ybuf[0, p] * inner_low
        high = whole[:, ROWS - 8 : ROWS] + ybuf[1, p] * inner_high
        return jnp.concatenate([low, whole[:, 8 : ROWS - 8], high], axis=1)

    def stage(g):
        for side, base in ((1, 0), (0, planes - 6)):
            first, count = RUNS[g][1 - side]
            for p in range(first, first + count):
                staged[side, p - base] = with_strips(p)

    for copy in y_copies(0) + x_copies(0) + y_copies(1):
        copy.start()
    for n in range(8):
        sums[n] = pltpu.roll(acted[...], 128 - 2 * (n + 1), 1)
    for copy in replies:
        copy.start()
    for g in range(2, X_RUNS + 1):
        for copy in y_copies(g):
            copy.start()
    wait_y(0)
    for copy in corner_copies():
        copy.start()
    wait_y(1)
    stage(1)
    for copy in x_copies(1):
        copy.start()
    sphere_step_one()
    for g in range(2, X_RUNS):
        wait_y(g)
        stage(g)
        for copy in x_copies(g):
            copy.start()
    wait_y(X_RUNS)
    inside, scale = wall_masks(gy, n_gy, span_y, rhs.shape[3])
    plane = rhs.shape[1:]
    stages = (level_0, level_1, level_2, level_3)
    first, last = 6, planes - 3

    def begin(x, _):
        level_0[x] = (with_strips(x - 2).reshape(inside.shape) * inside).reshape(plane)
        return 0

    lax.fori_loop(first, last + 1, begin, 0)

    def swept(k, x):
        source = stages[k - 1]
        return relaxed(level_0[x], source[x - 1], source[x], source[x + 1], scale)

    def finish(x):
        result = swept(ITERS, x)
        for c in range(3):
            done[c, x - HALO - 1] = result[c, HALO : HALO + span_y, :]

    for k in range(1, ITERS):

        def step(s, _, k=k):
            for u in range(2):
                x = first + k + 2 * s + u
                stages[k][x] = swept(k, x)
            return 0

        lax.fori_loop(0, (last - first + 1 - 2 * k) // 2, step, 0)
    for x in range(first + ITERS, last - ITERS + 1):
        finish(x)

    for g in range(X_RUNS - 1):
        for copy in x_copies(g) + (corner_copies() if g == 0 else []):
            copy.wait()
        (low, count), _ = RUNS[g]
        left = list(range(5 - low - count + 1, 5 - low + 1))
        right = list(range(planes - 2 + low, planes - 2 + low + count))
        for x, beside in [(x, xbuf[0, x]) for x in left] + [
            (x, xbuf[1, x - planes + 2]) for x in right
        ]:
            if g == 0:
                side = 0 if x < planes // 2 else 1
                low_rows = beside[:, 0:8] + zbuf[side, 0] * inner_low
                high_rows = beside[:, ROWS - 8 : ROWS] + zbuf[side, 1] * inner_high
                beside = jnp.concatenate(
                    [low_rows, beside[:, 8 : ROWS - 8], high_rows], axis=1
                )
            whole = beside + (with_strips(x - 2) if 2 <= x < planes + 2 else rhs[x])
            level_0[x] = (whole.reshape(inside.shape) * inside).reshape(plane)
        for k in range(1, ITERS):
            for x in [x + k for x in left] + [x - k for x in right]:
                stages[k][x] = swept(k, x)
        for x in [x + ITERS for x in left] + [x - ITERS for x in right]:
            finish(x)
        if g == 0:
            sphere_step_two()
        if g == 1:
            sphere_step_three()
    for copy in x_copies(X_RUNS - 1):
        copy.wait()


def relax_kernel(
    n_gy, rhs, xbuf, level_0, level_1, level_2, level_3, done, nm_in, out_ref, nm_ref, staged, sems
):
    gy = lax.axis_index("gy")
    top = level_0.shape[0] - 1
    span_x = top + 1 - 2 * HALO
    span_y = out_ref.shape[2]
    copies = [
        pltpu.make_async_copy(done, out_ref.at[:, 1 : span_x - 1], sems.at[0]),
        pltpu.make_async_copy(nm_in, nm_ref, sems.at[1]),
    ]
    for copy in copies:
        copy.start()
    inside, scale = wall_masks(gy, n_gy, span_y, rhs.shape[3])
    plane = rhs.shape[1:]
    stages = (level_0, level_1, level_2, level_3)
    for side, (edge, inward) in enumerate(((0, 1), (top, -1))):
        whole = rhs[edge] + xbuf[side, 0 if side == 0 else 5]
        outer = (whole.reshape(inside.shape) * inside).reshape(plane)
        for k in range(1, ITERS + 1):
            x = edge + inward * k
            source = stages[k - 1]
            outer = relaxed(level_0[x], outer, source[x], source[x + inward], scale)
        x = 0 if side == 0 else span_x - 1
        for c in range(3):
            staged[side, c, 0] = outer[c, HALO : HALO + span_y, :]
        copies.append(
            pltpu.make_async_copy(staged.at[side], out_ref.at[:, x : x + 1], sems.at[2 + side])
        )
        copies[-1].start()
    for copy in copies:
        copy.wait()


def on_device(
    n_gx,
    n_gy,
    velocity,
    owner_block,
    base_x,
    base_y,
    base_z,
    delta_weights,
    marker_offset,
    sphere_motion,
    contact_sphere,
    contact_partner,
):
    span_x, span_y, extent_z = velocity.shape[1:]
    markers = base_x.shape[0]
    planes = span_x + 4
    every = markers // TILE + 8
    padded = planes + WINDOW - 1
    grown = (padded + 2, 3, ROWS, extent_z)
    vmem = pl.BlockSpec(memory_space=pltpu.VMEM)
    smem = pl.BlockSpec(memory_space=pltpu.SMEM)
    hbm = pl.BlockSpec(memory_space=pltpu.HBM)
    dma = pltpu.SemaphoreType.DMA
    motion = sphere_motion.T
    fhl, started, home, arrived = pl.pallas_call(
        functools.partial(request_kernel, n_gx, n_gy),
        out_shape=(
            jax.ShapeDtypeStruct((padded, 3 * ROWS, 2 * extent_z), BF16),
            jax.ShapeDtypeStruct(grown, F32),
            jax.ShapeDtypeStruct((32, markers), F32),
            jax.ShapeDtypeStruct((8, 24, TILE), F32),
        ),
        in_specs=[hbm] * 8,
        out_specs=(vmem,) * 4,
        scratch_shapes=[
            pltpu.VMEM(velocity.shape, F32),
            pltpu.VMEM((1, markers), I32),
            pltpu.VMEM((1, markers), I32),
            pltpu.VMEM((1, markers), I32),
            pltpu.VMEM((1, markers), I32),
            pltpu.VMEM((12, markers), F32),
            pltpu.VMEM((3, markers), F32),
            pltpu.SMEM((2, 6), F32),
            pltpu.VMEM((2, 3, 2, span_y, extent_z), F32),
            pltpu.VMEM((2, 3, 2 * span_x, extent_z), F32),
            pltpu.VMEM((4, 16, extent_z), F32),
            pltpu.VMEM((4, 16, extent_z), F32),
            pltpu.VMEM((2, 3, 2 * span_x, extent_z), F32),
            pltpu.VMEM((32, markers), F32),
            pltpu.VMEM((96, markers), BF16),
            pltpu.VMEM((8, TILE), F32),
            pltpu.VMEM((8, 24, TILE), F32),
            pltpu.VMEM((8, 24, TILE), F32),
            pltpu.VMEM((planes, 3, ROWS, extent_z), F32),
            dma((8,)),
            dma((8,)),
            dma((8,)),
            dma((1,)),
            dma((1,)),
        ],
        compiler_params=pltpu.CompilerParams(
            collective_id=0, has_side_effects=True, vmem_limit_bytes=24 << 20
        ),
        name="requests",
    )(
        *(
            pltpu.with_memory_space_constraint(array, pltpu.HBM)
            for array in (
                velocity,
                owner_block.reshape(1, markers),
                base_x.reshape(1, markers),
                base_y.reshape(1, markers),
                base_z.reshape(1, markers),
                delta_weights,
                marker_offset,
                motion,
            )
        )
    )
    rhs, acted = pl.pallas_call(
        marker_kernel,
        out_shape=(
            jax.ShapeDtypeStruct(grown, F32),
            jax.ShapeDtypeStruct((8, 128), F32),
        ),
        in_specs=[vmem] * 4,
        out_specs=(vmem,) * 2,
        scratch_shapes=[
            pltpu.VMEM((every, 96, TILE), BF16),
            pltpu.VMEM((every * BINS, TILE), F32),
            pltpu.VMEM((every * BINS, TILE), F32),
            pltpu.VMEM((every, TILE), F32),
            pltpu.VMEM((2, extent_z, TILE), BF16),
            pltpu.VMEM((2, 32, TILE), F32),
            pltpu.VMEM((8, 128), I32),
            pltpu.SMEM((8, 128), I32),
            dma,
        ],
        compiler_params=pltpu.CompilerParams(vmem_limit_bytes=24 << 20),
        name="markers",
    )(fhl, started, home, arrived)
    plane = (3, ROWS, extent_z)
    new_motion, *strips = pl.pallas_call(
        functools.partial(strip_kernel, n_gx, n_gy, markers // 2),
        out_shape=(
            jax.ShapeDtypeStruct(motion.shape, F32),
            jax.ShapeDtypeStruct((2, 6, 3, ROWS, extent_z), F32),
        )
        + (jax.ShapeDtypeStruct((planes + 4,) + plane, F32),) * 4
        + (jax.ShapeDtypeStruct((3, span_x - 2, span_y, extent_z), F32),),
        in_specs=[vmem] * 2 + [smem] * 3,
        out_specs=(vmem,) * 7,
        scratch_shapes=[
            pltpu.VMEM((2, planes, 3, 8, extent_z), F32),
            pltpu.VMEM((2, 2, 3, 8, extent_z), F32),
            pltpu.VMEM((8, 8, 128), F32),
            pltpu.VMEM((8, 8, 128), F32),
            pltpu.VMEM((n_gx, 1, 128), F32),
            pltpu.VMEM((n_gy, 1, 128), F32),
            pltpu.VMEM((2, 1, 128), F32),
            pltpu.VMEM((8, 128), F32),
            pltpu.VMEM((2, 6, 3, ROWS, extent_z), F32),
            dma((1,)),
            dma((1,)),
            dma((1,)),
            dma((1,)),
            dma((1,)),
            dma((1,)),
            dma((len(RUNS),)),
            dma((len(RUNS),)),
            dma((2 * X_RUNS,)),
            dma((2 * X_RUNS,)),
            dma((2,)),
            dma((2,)),
        ],
        compiler_params=pltpu.CompilerParams(
            collective_id=1, has_side_effects=True, vmem_limit_bytes=24 << 20
        ),
        name="strips",
    )(rhs, acted, motion, contact_sphere, contact_partner)
    velocity_star, new_motion = pl.pallas_call(
        functools.partial(relax_kernel, n_gy),
        out_shape=(
            jax.ShapeDtypeStruct(velocity.shape, F32),
            jax.ShapeDtypeStruct(motion.shape, F32),
        ),
        in_specs=[vmem] * 8,
        out_specs=(hbm, hbm),
        scratch_shapes=[
            pltpu.VMEM((2, 3, 1, span_y, extent_z), F32),
            dma((4,)),
        ],
        compiler_params=pltpu.CompilerParams(vmem_limit_bytes=24 << 20),
        name="relax",
    )(rhs, *strips, new_motion)
    return velocity_star, new_motion.T


def solution(mesh):
    placed = (
        P(None, "gx", "gy", None),
        P(("gx", "gy"), None),
        P(("gx", "gy")),
        P(("gx", "gy")),
        P(("gx", "gy")),
        P(None, ("gx", "gy")),
        P(None, ("gx", "gy")),
        P(None, ("gx", "gy")),
        P(("gx", "gy")),
        P(("gx", "gy")),
    )
    return jax.shard_map(
        functools.partial(on_device, mesh.shape["gx"], mesh.shape["gy"]),
        mesh=mesh,
        in_specs=placed,
        out_specs=(P(None, "gx", "gy", None), P(None, ("gx", "gy"))),
        check_vma=False,
    )
```

```python
import functools

import jax
import jax.numpy as jnp
from jax import lax
from jax.experimental import pallas as pl
from jax.experimental.pallas import tpu as pltpu
from jax.sharding import PartitionSpec as P

F32 = jnp.float32
BF16 = jnp.bfloat16
I32 = jnp.int32
MESH = pl.DeviceIdType.MESH

ITERS = 4
DIFFUSION = 1.0
RESPONSE = 0.5
DASHPOT = 0.1

TILE = 256
BINS = 32
WINDOW = 6
ROWS = 40
HALO = 4
LANES = [(dx, dy) for dx in (-1, 0, 1) for dy in (-1, 0, 1) if (dx, dy) != (0, 0)]
DIAGONALS = [(dx, dy) for dx, dy in LANES if dx * dy != 0]
RUNS = [
    ((0, 1), (19, 1)),
    ((1, 2), (17, 2)),
    ((3, 2), (15, 2)),
    ((5, 1), (14, 1)),
    ((6, 8),),
]
X_RUNS = len(RUNS) - 1


def split(values):
    high = values.astype(BF16)
    low = (values - high.astype(F32)).astype(BF16)
    return high, low


def pick(distance, weights):
    result = jnp.where(distance == 3, weights[3], 0.0)
    for k in (2, 1, 0):
        result = jnp.where(distance == k, weights[k], result)
    return result


def cross(a, b):
    return (
        a[1] * b[2] - a[2] * b[1],
        a[2] * b[0] - a[0] * b[2],
        a[0] * b[1] - a[1] * b[0],
    )


def remote(src, dst, send, recv, peer):
    return pltpu.make_async_remote_copy(
        src_ref=src,
        dst_ref=dst,
        send_sem=send,
        recv_sem=recv,
        device_id=peer,
        device_id_type=MESH,
    )


def wait_all(whole, send, recv, at):
    copy = remote(whole, whole, send, recv, at(1, 0))
    copy.wait()


def greet(peers):
    barrier = pltpu.get_barrier_semaphore()
    for peer in peers:
        pl.semaphore_signal(barrier, inc=1, device_id=peer, device_id_type=MESH)
    return barrier


def neighbours(n_gx, n_gy):
    gx = lax.axis_index("gx")
    gy = lax.axis_index("gy")

    def at(dx, dy):
        return (lax.rem(gx + (dx + n_gx), n_gx), lax.rem(gy + (dy + n_gy), n_gy))

    return gx, gy, at


def terms(values):
    parts = []
    rest = values
    for _ in range(3):
        part = rest.astype(BF16)
        parts.append(part)
        rest = rest - part.astype(F32)
    return jnp.concatenate(parts, axis=0)


def chosen_columns(parts, slots, first):
    wanted = lax.broadcasted_iota(I32, (TILE, TILE), 0).astype(F32) + first
    hit = jnp.where(wanted == slots, 1.0, 0.0).astype(BF16)
    return lax.dot_general(parts, hit, (((1,), (1,)), ((), ())), preferred_element_type=F32)


def ranks(hits, above):
    return jnp.dot(hits.astype(BF16), above, preferred_element_type=F32)


def strictly_above(size):
    return (
        lax.broadcasted_iota(I32, (size, size), 0) < lax.broadcasted_iota(I32, (size, size), 1)
    ).astype(BF16)


def request_kernel(
    n_gx,
    n_gy,
    v_hbm,
    own_hbm,
    bx_hbm,
    by_hbm,
    bz_hbm,
    dw_hbm,
    off_hbm,
    mot_hbm,
    fhl,
    rhs,
    home,
    arrived,
    v_ref,
    own_ref,
    bx_ref,
    by_ref,
    bz_ref,
    dw_ref,
    off_ref,
    mot_ref,
    hx,
    hy,
    hc,
    corner,
    edges,
    pay,
    pay3,
    slot_s,
    snd,
    inbox,
    frame,
    in_sem,
    halo_send,
    halo_recv,
    pay_send,
    pay_recv,
):
    gx, gy, at = neighbours(n_gx, n_gy)
    here = gx * n_gy + gy
    barrier = greet([at(dx, dy) for dx, dy in LANES])
    loads = [
        pltpu.make_async_copy(src, dst, in_sem.at[i])
        for i, (src, dst) in enumerate(
            (
                (v_hbm, v_ref),
                (own_hbm, own_ref),
                (bx_hbm, bx_ref),
                (by_hbm, by_ref),
                (bz_hbm, bz_ref),
                (dw_hbm, dw_ref),
                (off_hbm, off_ref),
                (mot_hbm, mot_ref),
            )
        )
    ]
    for copy in loads:
        copy.start()
    markers = dw_ref.shape[1]
    chunks = markers // TILE
    span_x = v_ref.shape[1]
    span_y = v_ref.shape[2]
    extent_z = v_ref.shape[3]
    planes = span_x + 4
    for copy in loads:
        copy.wait()

    last = span_x - 2
    pl.semaphore_wait(barrier, len(LANES))
    halo = []
    halo.append(remote(v_ref.at[:, 0:2], hx.at[1], halo_send.at[0], halo_recv.at[0], at(-1, 0)))
    halo.append(
        remote(v_ref.at[:, last:span_x], hx.at[0], halo_send.at[1], halo_recv.at[1], at(1, 0))
    )
    halo.append(remote(edges.at[0], hy.at[1], halo_send.at[2], halo_recv.at[2], at(0, -1)))
    halo.append(remote(edges.at[1], hy.at[0], halo_send.at[3], halo_recv.at[3], at(0, 1)))
    for k, (dx, dy) in enumerate(DIAGONALS):
        slot = (1 if dx < 0 else 0) * 2 + (1 if dy < 0 else 0)
        halo.append(
            remote(
                corner.at[k], hc.at[slot], halo_send.at[4 + k], halo_recv.at[4 + k], at(dx, dy)
            )
        )
    corner[...] = jnp.zeros_like(corner)
    for k, (dx, dy) in enumerate(DIAGONALS):
        x0 = 0 if dx < 0 else last
        y0 = 0 if dy < 0 else span_y - 2
        for c in range(3):
            for i in range(2):
                row = 4 * c + 2 * i
                corner[k, row : row + 2, :] = v_ref[c, x0 + i, y0 : y0 + 2, :]
    for copy in halo[4:] + halo[0:2]:
        copy.start()
    for side, y0 in enumerate((0, span_y - 2)):
        for c in range(3):
            for x in range(span_x):
                edges[side, c, 2 * x : 2 * x + 2, :] = v_ref[c, x, y0 : y0 + 2, :]
    for copy in halo[2:4]:
        copy.start()

    pay[0:12, :] = dw_ref[...]
    pay[12:13, :] = bx_ref[...].astype(F32)
    pay[13:14, :] = by_ref[...].astype(F32)
    pay[14:15, :] = bz_ref[...].astype(F32)
    per_sphere = markers // 2
    second = (lax.broadcasted_iota(I32, (1, markers), 1) >= per_sphere).astype(F32)
    pay[15:16, :] = second
    motion = [mot_ref[0, c] * (1.0 - second) + mot_ref[1, c] * second for c in range(6)]
    offset = [off_ref[c : c + 1, :] for c in range(3)]
    swing = cross(motion[3:6], offset)
    for c in range(3):
        pay[16 + c : 17 + c, :] = motion[c] + swing[c]
        pay[19 + c : 20 + c, :] = offset[c]
    pay[22:23, :] = jnp.ones((1, markers), F32)
    pay[23:32, :] = jnp.zeros((9, markers), F32)
    whole = pay[...]
    pay3[...] = terms(whole)
    home[...] = whole
    home[22:23, :] = (own_ref[...] == here).astype(F32)

    above = strictly_above(TILE)
    bins = lax.broadcasted_iota(I32, (8, TILE), 0)
    carry = jnp.zeros((8, 1), F32)
    for q in range(chunks):
        owner = own_ref[:, q * TILE : (q + 1) * TILE]
        owner_x = lax.shift_right_logical(owner, n_gy.bit_length() - 1)
        owner_y = owner & (n_gy - 1)
        step_x = (owner_x - gx + 1) & (n_gx - 1)
        lane = step_x * 3 + (owner_y - gy + 1)
        lane = jnp.where(owner == here, -1, jnp.where(lane > 4, lane - 1, lane))
        hits = jnp.where(bins == lane, 1.0, 0.0)
        ranked = ranks(hits, above) + carry + bins.astype(F32) * TILE
        carry = carry + jnp.sum(hits, axis=1, keepdims=True)
        slot = jnp.sum(hits * ranked, axis=0, keepdims=True)
        slot_s[q : q + 1, :] = jnp.where(lane < 0, -1.0, slot)

    def compact(n, _):
        first = (n * TILE).astype(F32)
        moved = None
        for q in range(chunks):
            part = chosen_columns(
                pay3[:, q * TILE : (q + 1) * TILE], slot_s[q : q + 1, :], first
            )
            moved = part if moved is None else moved + part
        snd[n] = moved[0:24] + moved[32:56] + moved[64:88]
        return 0

    lax.fori_loop(0, 8, compact, 0)

    requests = [
        remote(snd.at[n], inbox.at[n], pay_send.at[0], pay_recv.at[0], at(dx, dy))
        for n, (dx, dy) in enumerate(LANES)
    ]
    for copy in requests:
        copy.start()

    inner_low = jnp.where(gy > 0, 1.0, 0.0).astype(F32)
    inner_high = jnp.where(gy < n_gy - 1, 1.0, 0.0).astype(F32)

    def clear(p, _):
        rhs[p] = jnp.zeros((3, ROWS, extent_z), F32)
        return 0

    lax.fori_loop(0, rhs.shape[0], clear, 0)

    def clear_frame(p, _):
        frame[p] = jnp.zeros((3, ROWS, extent_z), F32)
        return 0

    lax.fori_loop(0, planes, clear_frame, 0)

    def clear_beyond(p, _):
        fhl[p] = jnp.zeros((3 * ROWS, 2 * extent_z), BF16)
        return 0

    lax.fori_loop(planes, fhl.shape[0], clear_beyond, 0)

    def place(x, _):
        for c in range(3):
            plane = v_ref[c, x]
            frame[x + 2, c, 4 : 4 + span_y, :] = plane
            rhs[x + 4, c, 4 : 4 + span_y, :] = plane
        return 0

    lax.fori_loop(0, span_x, place, 0)
    for copy in halo:
        copy.wait()

    for x in range(span_x):
        for c in range(3):
            frame[x + 2, c, 2:4, :] = hy[0, c, 2 * x : 2 * x + 2, :] * inner_low
            frame[x + 2, c, 36:38, :] = hy[1, c, 2 * x : 2 * x + 2, :] * inner_high
    for side in range(2):
        for i in range(2):
            p = (0 if side == 0 else planes - 2) + i
            for c in range(3):
                frame[p, c, 4 : 4 + span_y, :] = hx[side, c, i]
                frame[p, c, 2:4, :] = hc[side * 2, 4 * c + 2 * i : 4 * c + 2 * i + 2, :] * inner_low
                frame[p, c, 36:38, :] = (
                    hc[side * 2 + 1, 4 * c + 2 * i : 4 * c + 2 * i + 2, :] * inner_high
                )

    def halve(p, _):
        high, low = split(frame[p].reshape(3 * ROWS, extent_z))
        fhl[p, :, 0:extent_z] = high
        fhl[p, :, extent_z : 2 * extent_z] = low
        return 0

    lax.fori_loop(0, planes, halve, 0)
    wait_all(inbox, pay_send.at[0], pay_recv.at[0], at)
    arrived[...] = inbox[...]


def marker_kernel(
    fhl,
    rhs_in,
    home,
    arrived,
    rhs,
    acted,
    pay3,
    hit_s,
    rank_s,
    slot_s,
    tz,
    held,
    edge_v,
    edge,
    edge_sem,
):
    chunks = home.shape[1] // TILE
    every = chunks + 8
    extent_z = rhs.shape[3]
    bins = lax.broadcasted_iota(I32, (BINS, TILE), 0).astype(F32)

    def chunk(q):
        return home[0:24, q * TILE : (q + 1) * TILE] if q < chunks else arrived[q - chunks]

    totals = []
    for q in range(every):
        m = chunk(q)
        hits = jnp.where((bins == m[12:13]) & (m[22:23] > 0.5), 1.0, 0.0)
        hit_s[q * BINS : (q + 1) * BINS, :] = hits
        totals.append(jnp.sum(hits, axis=1, keepdims=True))
    rank_s[...] = ranks(hit_s[...], strictly_above(TILE))
    carries = []
    count = jnp.zeros((BINS, 1), F32)
    for q in range(every):
        carries.append(count)
        count = count + totals[q]
    count = jnp.broadcast_to(count, (BINS, 128))
    high, low = split(count)
    below = (
        lax.broadcasted_iota(I32, (BINS, BINS), 0) > lax.broadcasted_iota(I32, (BINS, BINS), 1)
    ).astype(BF16)
    start = jnp.dot(below, high, preferred_element_type=F32)
    start = start + jnp.dot(below, low, preferred_element_type=F32)
    opening = lax.broadcasted_iota(I32, (BINS, 128), 1).astype(F32) * TILE
    present = jnp.sum(count, axis=0, keepdims=True)
    closing = jnp.minimum(opening + TILE, present)
    first_bin = jnp.sum(jnp.where(start + count <= opening, 1.0, 0.0), axis=0, keepdims=True)
    last_bin = jnp.sum(jnp.where(start < closing, 1.0, 0.0), axis=0, keepdims=True) - 1.0
    edge_v[...] = jnp.concatenate(
        [first_bin, last_bin, present, jnp.zeros((5, 128), F32)], axis=0
    ).astype(I32)
    to_scalars = pltpu.make_async_copy(edge_v, edge, edge_sem)
    to_scalars.start()
    start = start[:, 0:1]
    for q in range(every):
        hits = hit_s[q * BINS : (q + 1) * BINS, :]
        ranked = rank_s[q * BINS : (q + 1) * BINS, :] + (carries[q] + start)
        slot = jnp.sum(hits * ranked, axis=0, keepdims=True)
        there = jnp.sum(hits, axis=0, keepdims=True)
        slot_s[q : q + 1, :] = jnp.where(there > 0.5, slot, -1.0)
        m = chunk(q)
        if q < chunks:
            source = jnp.zeros((1, TILE), F32)
        else:
            source = jnp.full((1, TILE), float(q - chunks + 1), F32)
        filled = jnp.concatenate([m[0:23], source, jnp.zeros((8, TILE), F32)], axis=0)
        pay3[q] = terms(filled)
    acted[...] = jnp.zeros_like(acted)

    for p in range(rhs.shape[0]):
        rhs[p] = rhs_in[p]
    slot_id = lax.broadcasted_iota(I32, (TILE, TILE), 0).astype(F32)

    def gather(n):
        wanted = slot_id + (n * TILE).astype(F32)
        moved = None
        for q in range(every):
            hit = jnp.where(wanted == slot_s[q : q + 1, :], 1.0, 0.0).astype(BF16)
            part = lax.dot_general(
                hit, pay3[q], (((1,), (1,)), ((), ())), preferred_element_type=F32
            )
            moved = part if moved is None else moved + part
        moved = jnp.concatenate([moved, jnp.zeros((TILE, 32), F32)], axis=1).T
        return moved[0:32] + moved[32:64] + moved[64:96]

    def prepare(m):
        cell_y = m[13:14].astype(I32)
        cell_z = m[14:15].astype(I32)
        z = lax.broadcasted_iota(I32, (extent_z, TILE), 0)
        table = pick((z - cell_z) & (extent_z - 1), [m[8 + i : 9 + i] for i in range(4)])
        high, low = split(table)
        y = lax.broadcasted_iota(I32, (ROWS, TILE), 0) - 2
        table_y = pick(y - cell_y, [m[4 + i : 5 + i] for i in range(4)])
        return high, low, table_y

    def x_table(m, plane):
        x = lax.broadcasted_iota(I32, (8, TILE), 0)
        return pick(x + plane - m[12:13].astype(I32), [m[i : i + 1] for i in range(4)])

    def sample(m, plane, high, low, table_y, totals):
        table_x = x_table(m, plane)
        folded_y = table_y.reshape(ROWS // 8, 8, TILE)
        both = fhl[pl.ds(plane, WINDOW)].reshape(WINDOW * 3 * ROWS, 2 * extent_z)
        left = jnp.concatenate([both, both[:, 0:extent_z]], axis=1)
        right = jnp.concatenate([high, high, low], axis=0)
        part = jnp.dot(left, right, preferred_element_type=F32)
        part = part.reshape(WINDOW, 3, ROWS // 8, 8, TILE)
        result = []
        for c in range(3):
            total = totals[c]
            for p in range(WINDOW):
                total = total + jnp.sum(part[p, c] * folded_y, axis=0) * table_x[p : p + 1]
            result.append(total)
        return tuple(result)

    def act(m, totals):
        totals = [jnp.sum(total, axis=0, keepdims=True) for total in totals]
        force = [m[16 + c : 17 + c] - totals[c] for c in range(3)]
        torque = cross([m[19 + c : 20 + c] for c in range(3)], force)
        acting = jnp.concatenate(force + list(torque) + [jnp.zeros((2, TILE), F32)], axis=0)
        group = m[23:24] * 2.0 + m[15:16]
        member = (
            (lax.broadcasted_iota(I32, (128, TILE), 0).astype(F32) == group)
            & (m[22:23] > 0.5)
        ).astype(F32)
        summed = lax.dot_general(
            terms(acting),
            member.astype(BF16),
            (((1,), (1,)), ((), ())),
            preferred_element_type=F32,
        )
        acted[...] += summed[0:8] + summed[8:16] + summed[16:24]
        return force

    def deposit(m, plane, force, z_high, z_low, table_y):
        table_x = x_table(m, plane)
        rows = []
        for p in range(WINDOW):
            for c in range(3):
                rows.append((force[c] * table_x[p : p + 1]) * table_y)
        high, low = split(jnp.concatenate(rows, axis=0))
        left = jnp.concatenate([high, low, high], axis=1)
        right = jnp.concatenate([z_high, z_high, z_low], axis=1)
        added = lax.dot_general(
            left, right, (((1,), (1,)), ((), ())), preferred_element_type=F32
        )
        rhs[pl.ds(plane + 2, WINDOW)] += added.reshape(WINDOW, 3, ROWS, extent_z)

    held[0] = gather(jnp.int32(0))
    to_scalars.wait()
    tiles = lax.shift_right_logical(edge[2, 0] + (TILE - 1), TILE.bit_length() - 1)
    nothing = (jnp.zeros((8, TILE), F32),) * 3

    def work(n, _):
        low_plane = edge[0, n]
        spans = (edge[1, n] + 3 - low_plane + WINDOW) // WINDOW
        slot = n & 1

        @pl.when(spans <= 1)
        def _narrow():
            m = held[slot]
            high, low, table_y = prepare(m)
            totals = sample(m, low_plane, high, low, table_y, nothing)
            following = gather(n + 1)
            force = act(m, totals)
            deposit(m, low_plane, force, high, low, table_y)
            held[1 - slot] = following

        @pl.when(spans > 1)
        def _wide():
            m = held[slot]
            high, low, table_y = prepare(m)
            tz[0] = high
            tz[1] = low

            def sample_span(j, totals):
                plane = low_plane + j * WINDOW
                return sample(held[slot], plane, tz[0], tz[1], table_y, totals)

            force = act(m, lax.fori_loop(0, spans, sample_span, nothing))

            def deposit_span(j, _):
                plane = low_plane + j * WINDOW
                deposit(held[slot], plane, force, tz[0], tz[1], table_y)
                return 0

            lax.fori_loop(0, spans, deposit_span, 0)
            held[1 - slot] = gather(n + 1)

        return 0

    lax.fori_loop(0, tiles, work, 0)


def wall_masks(gy, n_gy, span_y, extent_z):
    y = lax.broadcasted_iota(I32, (ROWS, extent_z), 0)
    low_edge = jnp.where(gy > 0, 0, HALO)
    high_edge = jnp.where(gy < n_gy - 1, ROWS, HALO + span_y)
    inside = jnp.where((y >= low_edge) & (y < high_edge), 1.0, 0.0).astype(F32)
    inside = jnp.concatenate([inside] * 3, axis=0)
    return inside, inside * (1.0 / (1.0 + 6.0 * DIFFUSION))


def relaxed(rhs, before, centre, after, scale):
    shape = rhs.shape
    flat = scale.shape
    centre = centre.reshape(flat)
    total = rhs.reshape(flat) + before.reshape(flat) + after.reshape(flat)
    total = total + pltpu.roll(centre, 1, 0) + pltpu.roll(centre, flat[0] - 1, 0)
    total = total + pltpu.roll(centre, 1, 1) + pltpu.roll(centre, flat[1] - 1, 1)
    return (total * scale).reshape(shape)


def strip_kernel(
    n_gx,
    n_gy,
    per_sphere,
    rhs,
    acted,
    mot_ref,
    cs_ref,
    cp_ref,
    nm_ref,
    xbuf,
    level_0,
    level_1,
    level_2,
    level_3,
    done,
    ybuf,
    zbuf,
    sums,
    ret,
    agx,
    agy,
    ag1,
    moved_s,
    staged,
    ret_send,
    ret_recv,
    agx_send,
    agx_recv,
    agy_send,
    agy_recv,
    y_send,
    y_recv,
    x_send,
    x_recv,
    z_send,
    z_recv,
):
    gx, gy, at = neighbours(n_gx, n_gy)
    here = gx * n_gy + gy
    planes = ybuf.shape[1]
    span_y = done.shape[2]
    peers = (
        [at(k, 0) for k in range(1, n_gx)]
        + [at(0, k) for k in range(1, n_gy)]
        + [at(dx, dy) for dx in (-1, 1) for dy in (-1, 1)]
    )
    barrier = greet(peers)
    inner_low = jnp.where(gy > 0, 1.0, 0.0).astype(F32)
    inner_high = jnp.where(gy < n_gy - 1, 1.0, 0.0).astype(F32)
    replies = [
        remote(sums.at[n], ret.at[n], ret_send.at[0], ret_recv.at[0], at(-dx, -dy))
        for n, (dx, dy) in enumerate(LANES)
    ]
    lanes = lax.broadcasted_iota(I32, (8, 128), 1)
    row_id = lax.broadcasted_iota(I32, (8, 128), 0)
    pl.semaphore_wait(barrier, len(peers))

    def along_x(k):
        return remote(ag1.at[0], agx.at[k], agx_send.at[0], agx_recv.at[0], at(k, 0))

    def along_y(k):
        return remote(ag1.at[1], agy.at[k], agy_send.at[0], agy_recv.at[0], at(0, k))

    def sphere_step_one():
        wait_all(ret, ret_send.at[0], ret_recv.at[0], at)
        total = acted[...]
        for n in range(8):
            total = total + ret[n]
        start = jnp.zeros((8, 128), F32)
        for c in range(6):
            for s in range(2):
                start = jnp.where((row_id == c) & (lanes == s), mot_ref[s, c], start)
        moved = start - total * (RESPONSE / per_sphere)
        moved_s[...] = moved
        lane = lanes[0:1]
        message = jnp.zeros((1, 128), F32)
        for sphere in range(2):
            for c in range(3):
                message = jnp.where(
                    lane == 3 * sphere + c, moved[c : c + 1, sphere : sphere + 1], message
                )
        ag1[0] = message
        for k in range(1, n_gx):
            along_x(k).start()

    def sphere_step_two():
        wait_all(agx.at[pl.ds(1, n_gx - 1)], agx_send.at[0], agx_recv.at[0], at)
        total = ag1[0]
        for k in range(1, n_gx):
            total = total + pltpu.roll(agx[k], 6 * k, 1)
        ag1[1] = total
        for k in range(1, n_gy):
            along_y(k).start()

    def sphere_step_three():
        wait_all(agy.at[pl.ds(1, n_gy - 1)], agy_send.at[0], agy_recv.at[0], at)
        table = jnp.concatenate([ag1[1]] + [agy[k] for k in range(1, n_gy)], axis=0)
        moved = moved_s[...]
        pull = jnp.zeros((8, 128), F32)
        for k in range(cs_ref.shape[0]):
            partner = cp_ref[k]
            own = cs_ref[k] - 2 * here
            holder = lax.shift_right_logical(partner, 1)
            holder_x = lax.shift_right_logical(holder, n_gy.bit_length() - 1)
            row = (gy - (holder & (n_gy - 1)) + n_gy) & (n_gy - 1)
            lane = 6 * ((gx - holder_x + n_gx) & (n_gx - 1)) + 3 * (partner & 1)
            mine = jnp.where(row_id == row, table, 0.0)
            for c in range(3):
                chosen = jnp.sum(
                    jnp.where(lanes == lane + c, mine, 0.0), axis=(0, 1), keepdims=True
                )
                pull = pull + jnp.where((lanes == own) & (row_id == c), chosen - moved, 0.0)
        settled = jnp.concatenate(
            [moved + DASHPOT * pull, jnp.zeros((120, 128), F32)], axis=0
        )
        nm_ref[...] = settled.T[0:2, 0:6]

    def y_copies(g):
        copies = []
        for first, count in RUNS[g]:
            lo = first + 2
            copies.append(
                remote(
                    rhs.at[pl.ds(lo, count), :, pl.ds(0, 8)],
                    ybuf.at[1, pl.ds(first, count)],
                    y_send.at[g],
                    y_recv.at[g],
                    at(0, -1),
                )
            )
            copies.append(
                remote(
                    rhs.at[pl.ds(lo, count), :, pl.ds(ROWS - 8, 8)],
                    ybuf.at[0, pl.ds(first, count)],
                    y_send.at[g],
                    y_recv.at[g],
                    at(0, 1),
                )
            )
        return copies

    def wait_y(g):
        planes_in = sum(count for _, count in RUNS[g])
        wait_all(ybuf.at[:, pl.ds(0, planes_in)], y_send.at[g], y_recv.at[g], at)

    def x_copies(g):
        (low, count), (high, _) = RUNS[g]
        to_low, to_high = staged.at[1, pl.ds(low, count)], rhs.at[pl.ds(high + 2, count)]
        if g == 0:
            to_low = rhs.at[pl.ds(low + 2, count)]
        high = high - (planes - 6)
        if g > 0:
            to_high = staged.at[0, pl.ds(high, count)]
        return [
            remote(
                to_low,
                xbuf.at[1, pl.ds(low, count)],
                x_send.at[2 * g],
                x_recv.at[2 * g],
                at(-1, 0),
            ),
            remote(
                to_high,
                xbuf.at[0, pl.ds(high, count)],
                x_send.at[2 * g + 1],
                x_recv.at[2 * g + 1],
                at(1, 0),
            ),
        ]

    def corner_copies():
        return [
            remote(ybuf.at[:, 0], zbuf.at[1], z_send.at[0], z_recv.at[0], at(-1, 0)),
            remote(ybuf.at[:, planes - 1], zbuf.at[0], z_send.at[1], z_recv.at[1], at(1, 0)),
        ]

    def with_strips(p):
        whole = rhs[p + 2]
        low = whole[:, 0:8] + ybuf[0, p] * inner_low
        high = whole[:, ROWS - 8 : ROWS] + ybuf[1, p] * inner_high
        return jnp.concatenate([low, whole[:, 8 : ROWS - 8], high], axis=1)

    def stage(g):
        for side, base in ((1, 0), (0, planes - 6)):
            first, count = RUNS[g][1 - side]
            for p in range(first, first + count):
                staged[side, p - base] = with_strips(p)

    for copy in y_copies(0) + x_copies(0) + y_copies(1):
        copy.start()
    for n in range(8):
        sums[n] = pltpu.roll(acted[...], 128 - 2 * (n + 1), 1)
    for copy in replies:
        copy.start()
    for g in range(2, X_RUNS + 1):
        for copy in y_copies(g):
            copy.start()
    wait_y(0)
    for copy in corner_copies():
        copy.start()
    wait_y(1)
    stage(1)
    for copy in x_copies(1):
        copy.start()
    sphere_step_one()
    for g in range(2, X_RUNS):
        wait_y(g)
        stage(g)
        for copy in x_copies(g):
            copy.start()
    wait_y(X_RUNS)
    inside, scale = wall_masks(gy, n_gy, span_y, rhs.shape[3])
    plane = rhs.shape[1:]
    stages = (level_0, level_1, level_2, level_3)
    first, last = 6, planes - 3

    def begin(x, _):
        level_0[x] = (with_strips(x - 2).reshape(inside.shape) * inside).reshape(plane)
        return 0

    lax.fori_loop(first, last + 1, begin, 0)

    def swept(k, x):
        source = stages[k - 1]
        return relaxed(level_0[x], source[x - 1], source[x], source[x + 1], scale)

    def finish(x):
        result = swept(ITERS, x)
        for c in range(3):
            done[c, x - HALO - 1] = result[c, HALO : HALO + span_y, :]

    for k in range(1, ITERS):

        def step(s, _, k=k):
            for u in range(2):
                x = first + k + 2 * s + u
                stages[k][x] = swept(k, x)
            return 0

        lax.fori_loop(0, (last - first + 1 - 2 * k) // 2, step, 0)
    for x in range(first + ITERS, last - ITERS + 1):
        finish(x)

    for g in range(X_RUNS - 1):
        for copy in x_copies(g) + (corner_copies() if g == 0 else []):
            copy.wait()
        (low, count), _ = RUNS[g]
        left = list(range(5 - low - count + 1, 5 - low + 1))
        right = list(range(planes - 2 + low, planes - 2 + low + count))
        for x, beside in [(x, xbuf[0, x]) for x in left] + [
            (x, xbuf[1, x - planes + 2]) for x in right
        ]:
            if g == 0:
                side = 0 if x < planes // 2 else 1
                low_rows = beside[:, 0:8] + zbuf[side, 0] * inner_low
                high_rows = beside[:, ROWS - 8 : ROWS] + zbuf[side, 1] * inner_high
                beside = jnp.concatenate(
                    [low_rows, beside[:, 8 : ROWS - 8], high_rows], axis=1
                )
            whole = beside + (with_strips(x - 2) if 2 <= x < planes + 2 else rhs[x])
            level_0[x] = (whole.reshape(inside.shape) * inside).reshape(plane)
        for k in range(1, ITERS):
            for x in [x + k for x in left] + [x - k for x in right]:
                stages[k][x] = swept(k, x)
        for x in [x + ITERS for x in left] + [x - ITERS for x in right]:
            finish(x)
        if g == 0:
            sphere_step_two()
        if g == 1:
            sphere_step_three()
    for copy in x_copies(X_RUNS - 1):
        copy.wait()


def relax_kernel(
    n_gy, rhs, xbuf, level_0, level_1, level_2, level_3, done, nm_in, out_ref, nm_ref, staged, sems
):
    gy = lax.axis_index("gy")
    top = level_0.shape[0] - 1
    span_x = top + 1 - 2 * HALO
    span_y = out_ref.shape[2]
    copies = [
        pltpu.make_async_copy(done, out_ref.at[:, 1 : span_x - 1], sems.at[0]),
        pltpu.make_async_copy(nm_in, nm_ref, sems.at[1]),
    ]
    for copy in copies:
        copy.start()
    inside, scale = wall_masks(gy, n_gy, span_y, rhs.shape[3])
    plane = rhs.shape[1:]
    stages = (level_0, level_1, level_2, level_3)
    for side, (edge, inward) in enumerate(((0, 1), (top, -1))):
        whole = rhs[edge] + xbuf[side, 0 if side == 0 else 5]
        outer = (whole.reshape(inside.shape) * inside).reshape(plane)
        for k in range(1, ITERS + 1):
            x = edge + inward * k
            source = stages[k - 1]
            outer = relaxed(level_0[x], outer, source[x], source[x + inward], scale)
        x = 0 if side == 0 else span_x - 1
        for c in range(3):
            staged[side, c, 0] = outer[c, HALO : HALO + span_y, :]
        copies.append(
            pltpu.make_async_copy(staged.at[side], out_ref.at[:, x : x + 1], sems.at[2 + side])
        )
        copies[-1].start()
    for copy in copies:
        copy.wait()


def on_device(
    n_gx,
    n_gy,
    velocity,
    owner_block,
    base_x,
    base_y,
    base_z,
    delta_weights,
    marker_offset,
    sphere_motion,
    contact_sphere,
    contact_partner,
):
    span_x, span_y, extent_z = velocity.shape[1:]
    markers = base_x.shape[0]
    planes = span_x + 4
    every = markers // TILE + 8
    padded = planes + WINDOW - 1
    grown = (padded + 2, 3, ROWS, extent_z)
    vmem = pl.BlockSpec(memory_space=pltpu.VMEM)
    smem = pl.BlockSpec(memory_space=pltpu.SMEM)
    hbm = pl.BlockSpec(memory_space=pltpu.HBM)
    dma = pltpu.SemaphoreType.DMA
    motion = sphere_motion.T
    fhl, started, home, arrived = pl.pallas_call(
        functools.partial(request_kernel, n_gx, n_gy),
        out_shape=(
            jax.ShapeDtypeStruct((padded, 3 * ROWS, 2 * extent_z), BF16),
            jax.ShapeDtypeStruct(grown, F32),
            jax.ShapeDtypeStruct((32, markers), F32),
            jax.ShapeDtypeStruct((8, 24, TILE), F32),
        ),
        in_specs=[hbm] * 8,
        out_specs=(vmem,) * 4,
        scratch_shapes=[
            pltpu.VMEM(velocity.shape, F32),
            pltpu.VMEM((1, markers), I32),
            pltpu.VMEM((1, markers), I32),
            pltpu.VMEM((1, markers), I32),
            pltpu.VMEM((1, markers), I32),
            pltpu.VMEM((12, markers), F32),
            pltpu.VMEM((3, markers), F32),
            pltpu.SMEM((2, 6), F32),
            pltpu.VMEM((2, 3, 2, span_y, extent_z), F32),
            pltpu.VMEM((2, 3, 2 * span_x, extent_z), F32),
            pltpu.VMEM((4, 16, extent_z), F32),
            pltpu.VMEM((4, 16, extent_z), F32),
            pltpu.VMEM((2, 3, 2 * span_x, extent_z), F32),
            pltpu.VMEM((32, markers), F32),
            pltpu.VMEM((96, markers), BF16),
            pltpu.VMEM((8, TILE), F32),
            pltpu.VMEM((8, 24, TILE), F32),
            pltpu.VMEM((8, 24, TILE), F32),
            pltpu.VMEM((planes, 3, ROWS, extent_z), F32),
            dma((8,)),
            dma((8,)),
            dma((8,)),
            dma((1,)),
            dma((1,)),
        ],
        compiler_params=pltpu.CompilerParams(
            collective_id=0, has_side_effects=True, vmem_limit_bytes=24 << 20
        ),
        name="requests",
    )(
        *(
            pltpu.with_memory_space_constraint(array, pltpu.HBM)
            for array in (
                velocity,
                owner_block.reshape(1, markers),
                base_x.reshape(1, markers),
                base_y.reshape(1, markers),
                base_z.reshape(1, markers),
                delta_weights,
                marker_offset,
                motion,
            )
        )
    )
    rhs, acted = pl.pallas_call(
        marker_kernel,
        out_shape=(
            jax.ShapeDtypeStruct(grown, F32),
            jax.ShapeDtypeStruct((8, 128), F32),
        ),
        in_specs=[vmem] * 4,
        out_specs=(vmem,) * 2,
        scratch_shapes=[
            pltpu.VMEM((every, 96, TILE), BF16),
            pltpu.VMEM((every * BINS, TILE), F32),
            pltpu.VMEM((every * BINS, TILE), F32),
            pltpu.VMEM((every, TILE), F32),
            pltpu.VMEM((2, extent_z, TILE), BF16),
            pltpu.VMEM((2, 32, TILE), F32),
            pltpu.VMEM((8, 128), I32),
            pltpu.SMEM((8, 128), I32),
            dma,
        ],
        compiler_params=pltpu.CompilerParams(vmem_limit_bytes=24 << 20),
        name="markers",
    )(fhl, started, home, arrived)
    plane = (3, ROWS, extent_z)
    new_motion, *strips = pl.pallas_call(
        functools.partial(strip_kernel, n_gx, n_gy, markers // 2),
        out_shape=(
            jax.ShapeDtypeStruct(motion.shape, F32),
            jax.ShapeDtypeStruct((2, 6, 3, ROWS, extent_z), F32),
        )
        + (jax.ShapeDtypeStruct((planes + 4,) + plane, F32),) * 4
        + (jax.ShapeDtypeStruct((3, span_x - 2, span_y, extent_z), F32),),
        in_specs=[vmem] * 2 + [smem] * 3,
        out_specs=(vmem,) * 7,
        scratch_shapes=[
            pltpu.VMEM((2, planes, 3, 8, extent_z), F32),
            pltpu.VMEM((2, 2, 3, 8, extent_z), F32),
            pltpu.VMEM((8, 8, 128), F32),
            pltpu.VMEM((8, 8, 128), F32),
            pltpu.VMEM((n_gx, 1, 128), F32),
            pltpu.VMEM((n_gy, 1, 128), F32),
            pltpu.VMEM((2, 1, 128), F32),
            pltpu.VMEM((8, 128), F32),
            pltpu.VMEM((2, 6, 3, ROWS, extent_z), F32),
            dma((1,)),
            dma((1,)),
            dma((1,)),
            dma((1,)),
            dma((1,)),
            dma((1,)),
            dma((len(RUNS),)),
            dma((len(RUNS),)),
            dma((2 * X_RUNS,)),
            dma((2 * X_RUNS,)),
            dma((2,)),
            dma((2,)),
        ],
        compiler_params=pltpu.CompilerParams(
            collective_id=1, has_side_effects=True, vmem_limit_bytes=24 << 20
        ),
        name="strips",
    )(rhs, acted, motion, contact_sphere, contact_partner)
    velocity_star, new_motion = pl.pallas_call(
        functools.partial(relax_kernel, n_gy),
        out_shape=(
            jax.ShapeDtypeStruct(velocity.shape, F32),
            jax.ShapeDtypeStruct(motion.shape, F32),
        ),
        in_specs=[vmem] * 8,
        out_specs=(hbm, hbm),
        scratch_shapes=[
            pltpu.VMEM((2, 3, 1, span_y, extent_z), F32),
            dma((4,)),
        ],
        compiler_params=pltpu.CompilerParams(vmem_limit_bytes=24 << 20),
        name="relax",
    )(rhs, *strips, new_motion)
    return velocity_star, new_motion.T


def solution(mesh):
    placed = (
        P(None, "gx", "gy", None),
        P(("gx", "gy"), None),
        P(("gx", "gy")),
        P(("gx", "gy")),
        P(("gx", "gy")),
        P(None, ("gx", "gy")),
        P(None, ("gx", "gy")),
        P(None, ("gx", "gy")),
        P(("gx", "gy")),
        P(("gx", "gy")),
    )
    return jax.shard_map(
        functools.partial(on_device, mesh.shape["gx"], mesh.shape["gy"]),
        mesh=mesh,
        in_specs=placed,
        out_specs=(P(None, "gx", "gy", None), P(None, ("gx", "gy"))),
        check_vma=False,
    )
```
